32 devices in a mesh: dp: 32 (over z, y, x, core).
Axes of the slice: x: 2, y: 2, z: 4, core: 2. Of those that a mesh axis runs over, the one named last changes fastest.
Arguments:
- w_in0: float32 [128, 64], replicated
- w_short: float32 [128, 256], replicated
- w_in: float32 [17, 256, 64], replicated
- w_mid: float32 [18, 3, 3, 64, 64], replicated
- w_out: float32 [18, 64, 256], replicated
- w_fc: float32 [256, 100], replicated
- w_bn: float32 [14336], replicated
- w_bias: float32 [100], replicated
- g_in0: float32 [32, 128, 64], P('dp')
- g_short: float32 [32, 128, 256], P('dp')
- g_in: float32 [32, 17, 256, 64], P('dp')
- g_mid: float32 [32, 18, 3, 3, 64, 64], P('dp')
- g_out: float32 [32, 18, 64, 256], P('dp')
- g_bn: float32 [32, 14336], P('dp')
- pooled: bfloat16 [32768, 256], P('dp')
- dlogits: bfloat16 [32768, 100], P('dp')
- v_in0: float32 [8192], P('dp')
- v_short: float32 [32768], P('dp')
- v_in: float32 [17, 16384], P(None, 'dp')
- v_mid: float32 [18, 36864], P(None, 'dp')
- v_out: float32 [18, 16384], P(None, 'dp')
- v_fc: float32 [25600], P('dp')
- v_bn: float32 [14336], P('dp')
- v_bias: float32 [128], P('dp')
- learn_rate: float32 [], replicated
Outputs:
- output 1: float32 [128, 64], replicated
- output 2: float32 [128, 256], replicated
- output 3: float32 [17, 256, 64], replicated
- output 4: float32 [18, 3, 3, 64, 64], replicated
- output 5: float32 [18, 64, 256], replicated
- output 6: float32 [256, 100], replicated
- output 7: float32 [14336], replicated
- output 8: float32 [100], replicated
- output 9: bfloat16 [128, 64], replicated
- output 10: bfloat16 [128, 256], replicated
- output 11: bfloat16 [17, 256, 64], replicated
- output 12: bfloat16 [18, 3, 3, 64, 64], replicated
- output 13: bfloat16 [18, 64, 256], replicated
- output 14: bfloat16 [256, 100], replicated
- output 15: float32 [8192], P('dp')
- output 16: float32 [32768], P('dp')
- output 17: float32 [17, 16384], P(None, 'dp')
- output 18: float32 [18, 36864], P(None, 'dp')
- output 19: float32 [18, 16384], P(None, 'dp')
- output 20: float32 [25600], P('dp')
- output 21: float32 [14336], P('dp')
- output 22: float32 [128], P('dp')
All inputs are finite; a program needn't handle non-finite values.
Results may differ from the reference program's by a relative error of at most 0.001.
Values sent between devices are 32-bit elements.
A program may use at most 1 GiB of HBM per device.

```python
import math
import jax
import jax.numpy as jnp

C_IN = 128
C_MID = 64
C_OUT = 256
BLOCKS = 18
CLASSES = 100
LOCAL_BATCH = 1024
DEVICES = 32
BN_LEN = 14336
BIAS_PAD = 128

ROWS = DEVICES * LOCAL_BATCH
MOMENTUM = 0.9
TRUST_COEF = 0.001
DECAY = 0.0001


def draw_stack(key, count, shape, fan_in):
    keys = jax.random.split(key, 6)
    scale = fan_in ** -0.5
    ones = (1,) * len(shape)
    size = math.prod(shape)
    weight = scale * jax.random.normal(keys[0], (count,) + shape, jnp.float32)
    ratio = 1e-4 * 2.0 ** jax.random.uniform(keys[1], (1, count) + ones, jnp.float32, 0.0, 4.0)
    slope = jax.random.uniform(keys[5], (1, count) + ones, jnp.float32, 1.5, 3.0)
    place = (jnp.arange(size, dtype=jnp.float32) / size - 0.5).reshape((1, 1) + shape)
    ramp = 2.0 ** (slope * place)
    noise = jax.random.normal(keys[2], (DEVICES, count) + shape, jnp.float32)
    dev_mean = jax.random.normal(keys[3], (DEVICES, count) + ones, jnp.float32)
    gradient = scale * ratio * ramp * (math.sqrt(DEVICES) * noise + dev_mean)
    moment = 0.03 * scale * jax.random.normal(keys[4], (count, size), jnp.float32)
    return weight, gradient, moment


def setup_inputs(seed: int = 0) -> dict:
    keys = jax.random.split(jax.random.key(seed), 17)
    w_in0, g_in0, v_in0 = draw_stack(keys[0], 1, (C_IN, C_MID), C_IN)
    w_short, g_short, v_short = draw_stack(keys[1], 1, (C_IN, C_OUT), C_IN)
    w_in, g_in, v_in = draw_stack(keys[2], BLOCKS - 1, (C_OUT, C_MID), C_OUT)
    w_mid, g_mid, v_mid = draw_stack(keys[3], BLOCKS, (3, 3, C_MID, C_MID), 9 * C_MID)
    w_out, g_out, v_out = draw_stack(keys[4], BLOCKS, (C_MID, C_OUT), C_MID)
    fc_scale = C_OUT ** -0.5
    w_fc = fc_scale * jax.random.normal(keys[5], (C_OUT, CLASSES), jnp.float32)
    v_fc = 0.03 * fc_scale * jax.random.normal(keys[6], (C_OUT * CLASSES,), jnp.float32)
    pooled = jnp.abs(jax.random.normal(keys[7], (ROWS, C_OUT), jnp.float32))
    dev_shift = 0.2 * jax.random.normal(keys[8], (DEVICES, 1, CLASSES), jnp.float32)
    dlogits = 0.1 * (jax.random.normal(keys[9], (DEVICES, LOCAL_BATCH, CLASSES), jnp.float32) + dev_shift)
    bias_scale = 0.1 * (ROWS ** -0.5 + 0.2 * DEVICES ** -0.5)
    w_bias = 300.0 * bias_scale * jax.random.normal(keys[10], (CLASSES,), jnp.float32)
    v_bias = 20.0 * bias_scale * jax.random.normal(keys[11], (BIAS_PAD,), jnp.float32)
    w_bn = 0.5 + 0.5 * jax.random.normal(keys[12], (BN_LEN,), jnp.float32)
    bn_noise = jax.random.normal(keys[13], (DEVICES, BN_LEN), jnp.float32)
    bn_shift = jax.random.normal(keys[14], (DEVICES, 1), jnp.float32)
    g_bn = 0.001 * (math.sqrt(DEVICES) * bn_noise + bn_shift)
    v_bn = 0.03 * jax.random.normal(keys[15], (BN_LEN,), jnp.float32)
    learn_rate = jax.random.uniform(keys[16], (), jnp.float32, 10.0, 30.0)
    return {
        'w_in0': w_in0[0], 'w_short': w_short[0], 'w_in': w_in, 'w_mid': w_mid, 'w_out': w_out,
        'w_fc': w_fc, 'w_bn': w_bn, 'w_bias': w_bias,
        'g_in0': g_in0[:, 0], 'g_short': g_short[:, 0], 'g_in': g_in, 'g_mid': g_mid, 'g_out': g_out,
        'g_bn': g_bn,
        'pooled': pooled.astype(jnp.bfloat16),
        'dlogits': dlogits.reshape(ROWS, CLASSES).astype(jnp.bfloat16),
        'v_in0': v_in0[0], 'v_short': v_short[0], 'v_in': v_in, 'v_mid': v_mid, 'v_out': v_out,
        'v_fc': v_fc, 'v_bn': v_bn, 'v_bias': v_bias,
        'learn_rate': learn_rate,
    }


def lars_step(weight, gradient, moment, learn_rate):
    count = moment.shape[0]
    w_flat = weight.reshape(count, -1)
    g_flat = gradient.reshape(count, -1)
    w_norm = jnp.sqrt(jnp.sum(w_flat * w_flat, axis=1, keepdims=True))
    g_norm = jnp.sqrt(jnp.sum(g_flat * g_flat, axis=1, keepdims=True))
    trust = jnp.where((w_norm > 0) & (g_norm > 0), TRUST_COEF * w_norm / (g_norm + DECAY * w_norm), 1.0)
    moment_new = MOMENTUM * moment + learn_rate * trust * (g_flat + DECAY * w_flat)
    return (w_flat - moment_new).reshape(weight.shape), moment_new


def reference(w_in0, w_short, w_in, w_mid, w_out, w_fc, w_bn, w_bias,
              g_in0, g_short, g_in, g_mid, g_out, g_bn, pooled, dlogits,
              v_in0, v_short, v_in, v_mid, v_out, v_fc, v_bn, v_bias, learn_rate):
    fc_grad = jnp.dot(pooled.T, dlogits, preferred_element_type=jnp.float32) / ROWS
    bias_grad = jnp.sum(dlogits.astype(jnp.float32), axis=0) / ROWS
    kernels = [
        (w_in0, jnp.mean(g_in0, axis=0), v_in0),
        (w_short, jnp.mean(g_short, axis=0), v_short),
        (w_in, jnp.mean(g_in, axis=0), v_in),
        (w_mid, jnp.mean(g_mid, axis=0), v_mid),
        (w_out, jnp.mean(g_out, axis=0), v_out),
        (w_fc, fc_grad, v_fc),
    ]
    new_w = []
    new_v = []
    for weight, gradient, moment in kernels:
        w_next, moment_next = lars_step(weight, gradient, moment.reshape(-1, moment.shape[-1]), learn_rate)
        new_w.append(w_next)
        new_v.append(moment_next.reshape(moment.shape))
    bn_moment = MOMENTUM * v_bn + learn_rate * jnp.mean(g_bn, axis=0)
    bias_moment = MOMENTUM * v_bias + learn_rate * jnp.pad(bias_grad, (0, BIAS_PAD - CLASSES))
    w_bn_new = w_bn - bn_moment
    w_bias_new = w_bias - bias_moment[:CLASSES]
    return (new_w[0], new_w[1], new_w[2], new_w[3], new_w[4], new_w[5], w_bn_new, w_bias_new,
            new_w[0].astype(jnp.bfloat16), new_w[1].astype(jnp.bfloat16), new_w[2].astype(jnp.bfloat16),
            new_w[3].astype(jnp.bfloat16), new_w[4].astype(jnp.bfloat16), new_w[5].astype(jnp.bfloat16),
            new_v[0], new_v[1], new_v[2], new_v[3], new_v[4], new_v[5], bn_moment, bias_moment)
```

```python
import functools
import jax
import jax.numpy as jnp
from jax import lax
from jax.experimental import pallas as pl
from jax.experimental.pallas import tpu as pltpu
from jax.sharding import PartitionSpec as P

MOMENTUM = 0.9
TRUST_COEF = 0.001
DECAY = 0.0001
N_DEV = 32
LANES = 128
MID, IN0, IN, OUT, SHORT, FC, BN, BIAS, ROWS = 0, 162, 164, 232, 304, 312, 320, 324, 328
N_MID, N_IN, N_OUT = 18, 17, 18
CLASSES = 100
ID_IN0, ID_IN, ID_OUT, ID_SHORT, ID_FC, ID_PLAIN = 18, 19, 36, 54, 55, 56
F32 = jnp.float32
VMEM = pltpu.VMEM


def tensor_of_row(row):
    out = jnp.where(row < IN0, row // 9, ID_IN0)
    out = jnp.where(row >= IN, ID_IN + (row - IN) // 4, out)
    out = jnp.where(row >= OUT, ID_OUT + (row - OUT) // 4, out)
    out = jnp.where(row >= SHORT, ID_SHORT + (row - SHORT) // 8, out)
    return jnp.where(row >= BN, ID_PLAIN, out)


def left(a, b):
    return jnp.concatenate([a[:, :64], b[:, :64]], axis=1)


def right(a, b):
    return jnp.concatenate([a[:, 64:], b[:, 64:]], axis=1)


def across(piece8, row):
    return pl.ds(piece8 * 8 * ROWS + row, 8, stride=ROWS)


def pack_kernel(g_mid, g_in, g_in0, g_out, g_short, g_bn, pooled, dlog_t,
                w_mid, w_in, w_in0, w_out, w_short, w_fc, w_bn, w_bias, v_mid, v_in, v_out, v_small,
                packed, w_own, v_own,
                s_mid, s_in, s_in0, s_out, s_short, s_bn, s_x, s_d, xt, fct,
                o_mid, o_in, o_in0, o_out, o_short, o_fc, o_bn, ot, sems):
    rank = lax.axis_index('dp')
    copies = []

    def fetch(src, dst):
        copy = pltpu.make_async_copy(src, dst, sems.at[len(copies)])
        copy.start()
        copies.append(copy)
        return copy

    c_mid = fetch(g_mid, s_mid)
    c_in = fetch(g_in, s_in)
    c_in0 = fetch(g_in0, s_in0)
    c_out = [fetch(g_out.at[:, :, pl.ds(128 * h, 128)], s_out.at[h]) for h in range(2)]
    c_short = [fetch(g_short.at[:, pl.ds(128 * h, 128)], s_short.at[h]) for h in range(2)]
    c_bn = fetch(g_bn, s_bn)
    c_fc = [fetch(pooled, s_x), fetch(dlog_t, s_d)]
    mid_at = pl.multiple_of((18 * rank) // 8 * 8, 8)
    mid_off = 18 * rank - mid_at
    out_at = pl.multiple_of((2 * rank) // 8 * 8, 8)
    out_off = 2 * lax.rem(rank, 4)
    short_at = pl.multiple_of((4 * rank) // 8 * 8, 8)
    short_off = 4 * lax.rem(rank, 2)
    col_at = pl.multiple_of((rank // 16) * 128, 128)
    col_off = pl.multiple_of(lax.rem(rank, 16) * 8, 8)
    c_own = [
        fetch(w_mid.at[:, pl.ds(mid_at, 24), :], o_mid),
        fetch(w_in.at[:, :, pl.ds(col_at, 128)], o_in),
        fetch(w_in0, o_in0),
        fetch(w_out.at[:, pl.ds(out_at, 8), pl.ds(0, 128)], o_out.at[0]),
        fetch(w_out.at[:, pl.ds(out_at, 8), pl.ds(128, 128)], o_out.at[1]),
        fetch(w_short.at[pl.ds(short_at, 8), pl.ds(0, 128)], o_short.at[0]),
        fetch(w_short.at[pl.ds(short_at, 8), pl.ds(128, 128)], o_short.at[1]),
        fetch(w_fc.at[:, pl.ds(col_at, 128)], o_fc),
        fetch(w_bn, o_bn),
    ]

    for ref, base, tiles, count in ((v_mid, MID, 9, N_MID), (v_in, IN, 4, N_IN), (v_out, OUT, 4, N_OUT)):
        for m in range(tiles):
            for t in range(0, count, 8):
                size = min(8, count - t)
                v_own[pl.ds(base + tiles * t + m, size, stride=tiles), :] = ref[t:t + size, 128 * m:128 * m + 128]
    v_own[IN0:IN0 + 2, :] = v_small[0:2, :]
    v_own[SHORT:SHORT + 24, :] = v_small[8:32, :]

    c_mid.wait()

    def mid_body(t, carry):
        for a in range(4):
            for k in range(9):
                even = s_mid[t, pl.ds(144 * a + 2 * k, 8, stride=18), :]
                odd = s_mid[t, pl.ds(144 * a + 2 * k + 1, 8, stride=18), :]
                packed[across(a, MID + 9 * t + k), :] = jnp.concatenate([even, odd], axis=1)
        return carry

    lax.fori_loop(0, N_MID, mid_body, 0)
    c_in.wait()
    c_in0.wait()

    def in_rows(t, other):
        for a in range(4):
            for k in range(4):
                even = xt[pl.ds(64 * a + 2 * k, 8, stride=8), :]
                odd = xt[pl.ds(64 * a + 2 * k + 1, 8, stride=8), :]
                packed[across(a, IN + 4 * t + k), :] = left(even, odd)
                if other is not None:
                    packed[across(a, IN + 4 * other + k), :] = right(even, odd)

    def in_body(t, carry):
        both = jnp.concatenate([s_in[t], s_in[t + 8]], axis=0)
        for h in range(2):
            xt[128 * h:128 * h + 128, :] = both[:, 128 * h:128 * h + 128].T
        in_rows(t, t + 8)
        return carry

    lax.fori_loop(0, 8, in_body, 0)
    last = jnp.concatenate([s_in[16], jnp.concatenate([s_in0[...], s_in0[...]], axis=1)], axis=0)
    for h in range(2):
        xt[128 * h:128 * h + 128, :] = last[:, 128 * h:128 * h + 128].T
    in_rows(16, None)
    for a in range(4):
        for k in range(2):
            even = xt[pl.ds(32 * a + 2 * k, 8, stride=4), :]
            odd = xt[pl.ds(32 * a + 2 * k + 1, 8, stride=4), :]
            packed[across(a, IN0 + k), :] = right(even, odd)
    for copy in c_out + c_short:
        copy.wait()

    def out_body(t, carry):
        for a in range(4):
            for p in range(2):
                for h in range(2):
                    packed[across(a, OUT + 4 * t + 2 * p + h), :] = s_out[h, t, pl.ds(16 * a + p, 8, stride=2), :]
        return carry

    lax.fori_loop(0, N_OUT, out_body, 0)
    for a in range(4):
        for p in range(4):
            for h in range(2):
                packed[across(a, SHORT + 2 * p + h), :] = s_short[h, pl.ds(32 * a + p, 8, stride=4), :]
    for i in range(N_DEV):
        packed[i * ROWS + BN:i * ROWS + ROWS, :] = jnp.zeros((8, LANES), F32)
    c_bn.wait()
    for b in range(2):
        for k in range(4):
            for half in range(2):
                packed[pl.ds((16 * b + half) * ROWS + BN + k, 8, stride=2 * ROWS), :] = (
                    s_bn[pl.ds(56 * b + 3 * half + k, 8, stride=7), :])
    for copy in c_fc:
        copy.wait()
    scale = 1.0 / s_x.shape[0]
    fct[...] = jnp.zeros_like(fct)
    fct[0:CLASSES, :] = jnp.dot(s_d[...], s_x[...], preferred_element_type=F32) * scale
    bias = lax.dot_general(jnp.ones((8, s_d.shape[1]), jnp.bfloat16), s_d[...], (((1,), (1,)), ((), ())),
                           preferred_element_type=F32) * scale
    bias = jnp.concatenate([bias, jnp.zeros((8, LANES - CLASSES), F32)], axis=1)
    for a in range(4):
        packed[across(a, BIAS), :] = bias
    for h in range(2):
        cols = fct[:, 128 * h:128 * h + 128].T
        for j in range(16):
            at = (16 * h + j) * ROWS + FC
            packed[at:at + 8, :] = cols[8 * j:8 * j + 8, :]

    for copy in c_own:
        copy.wait()
    for t in range(N_MID):
        even = o_mid[t, pl.ds(mid_off, 9, stride=2), :]
        odd = o_mid[t, pl.ds(mid_off + 1, 9, stride=2), :]
        w_own[MID + 9 * t:MID + 9 * t + 9, :] = jnp.concatenate([even, odd], axis=1)
    for t in range(9):
        other = o_in[t + 8] if t < 8 else o_in0[...]
        ot[...] = jnp.concatenate([o_in[2 * 8 if t == 8 else t], other], axis=0).T
        even = ot[pl.ds(col_off, 4, stride=2), :]
        odd = ot[pl.ds(col_off + 1, 4, stride=2), :]
        here = 16 if t == 8 else t
        w_own[IN + 4 * here:IN + 4 * here + 4, :] = left(even, odd)
        if t < 8:
            w_own[IN + 4 * (t + 8):IN + 4 * (t + 8) + 4, :] = right(even, odd)
    even = ot[pl.ds(4 * rank, 2, stride=2), :]
    odd = ot[pl.ds(4 * rank + 1, 2, stride=2), :]
    w_own[IN0:IN0 + 2, :] = right(even, odd)
    for p in range(2):
        for h in range(2):
            for t in range(N_OUT):
                w_own[OUT + 4 * t + 2 * p + h:OUT + 4 * t + 2 * p + h + 1, :] = o_out[h, t, pl.ds(out_off + p, 1), :]
    for p in range(4):
        for h in range(2):
            w_own[SHORT + 2 * p + h:SHORT + 2 * p + h + 1, :] = o_short[h, pl.ds(short_off + p, 1), :]
    fct[0:CLASSES, 0:LANES] = o_fc[...]
    ot[...] = fct[:, 0:LANES].T
    w_own[FC:FC + 8, :] = jnp.where(lax.broadcasted_iota(jnp.int32, (8, LANES), 1) < CLASSES,
                                    ot[pl.ds(col_off, 8), :], 0.0)
    w_own[BN:ROWS, :] = jnp.zeros((8, LANES), F32)
    bn_at = 7 * (rank // 2) + 3 * lax.rem(rank, 2)
    for k in range(4):
        w_own[BN + k:BN + k + 1, :] = o_bn[pl.ds(bn_at + k, 1), :]
    lane = lax.broadcasted_iota(jnp.int32, (1, LANES), 1)
    w_own[BIAS:BIAS + 1, :] = jnp.where((lane >= 4 * rank) & (lane < 4 * rank + 4), w_bias[...], 0.0)


def pack_grads(ops):
    any_ = pl.BlockSpec(memory_space=pl.ANY)
    vm = pl.BlockSpec(memory_space=VMEM)
    return pl.pallas_call(
        pack_kernel,
        out_shape=(jax.ShapeDtypeStruct((N_DEV * ROWS, LANES), F32), jax.ShapeDtypeStruct((ROWS, LANES), F32),
                   jax.ShapeDtypeStruct((ROWS, LANES), F32)),
        in_specs=[any_] * 15 + [vm] * 5,
        out_specs=(vm, vm, vm),
        scratch_shapes=[
            VMEM((N_MID, 576, 64), F32), VMEM((N_IN, 64, 256), F32), VMEM((64, 128), F32),
            VMEM((2, N_OUT, 64, 128), F32), VMEM((2, 128, 128), F32), VMEM((112, 128), F32),
            VMEM((1024, 256), jnp.bfloat16), VMEM((CLASSES, 1024), jnp.bfloat16),
            VMEM((256, 128), F32), VMEM((128, 256), F32),
            VMEM((N_MID, 24, 64), F32), VMEM((N_IN, 64, 128), F32), VMEM((64, 128), F32),
            VMEM((2, N_OUT, 8, 128), F32), VMEM((2, 8, 128), F32), VMEM((CLASSES, 128), F32),
            VMEM((112, 128), F32), VMEM((128, 128), F32),
            pltpu.SemaphoreType.DMA((24,)),
        ],
        compiler_params=pltpu.CompilerParams(vmem_limit_bytes=40 * 2**20),
    )(*ops)


def unpack_kernel(packed, v_own, n_mid, n_in, n_in0, n_out, n_short, n_fc, n_bn, n_bias,
                  b_mid, b_in, b_in0, b_out, b_short, b_fc, v_mid, v_in, v_out, v_small,
                  s_mid, s_in, s_out, s_short, s_in0, s_fc, t_mid, t_in, t_out, t_short, t_in0, t_fc, xt, sems):
    bf = jnp.bfloat16

    def put(src, dst, k):
        pltpu.make_async_copy(src, dst, sems.at[k]).start()

    def mid_body(t, carry):
        for a in range(4):
            for k in range(9):
                x = packed[across(a, MID + 9 * t + k), :]
                s_mid[t, pl.ds(144 * a + 2 * k, 8, stride=18), :] = x[:, :64]
                s_mid[t, pl.ds(144 * a + 2 * k + 1, 8, stride=18), :] = x[:, 64:]
        put(s_mid.at[t], n_mid.at[t], 0)
        t_mid[t] = s_mid[t].astype(bf)
        put(t_mid.at[t], b_mid.at[t], 1)
        return carry

    lax.fori_loop(0, N_MID, mid_body, 0)

    def in_rows(t, other):
        for a in range(4):
            for k in range(4):
                x = packed[across(a, IN + 4 * t + k), :]
                y = packed[across(a, IN + 4 * other + k), :] if other is not None else x
                xt[pl.ds(64 * a + 2 * k, 8, stride=8), :] = left(x, y)
                xt[pl.ds(64 * a + 2 * k + 1, 8, stride=8), :] = right(x, y)

    def in_body(t, carry):
        in_rows(t, t + 8)
        for h in range(2):
            cols = xt[128 * h:128 * h + 128, :].T
            s_in[t, :, 128 * h:128 * h + 128] = cols[:64]
            s_in[t + 8, :, 128 * h:128 * h + 128] = cols[64:]
            t_in[t, :, 128 * h:128 * h + 128] = cols[:64].astype(bf)
            t_in[t + 8, :, 128 * h:128 * h + 128] = cols[64:].astype(bf)
        for u in (t, t + 8):
            put(s_in.at[u], n_in.at[u], 2)
            put(t_in.at[u], b_in.at[u], 3)
        return carry

    lax.fori_loop(0, 8, in_body, 0)
    in_rows(16, None)
    for h in range(2):
        cols = xt[128 * h:128 * h + 128, :].T
        s_in[16, :, 128 * h:128 * h + 128] = cols[:64]
        t_in[16, :, 128 * h:128 * h + 128] = cols[:64].astype(bf)
    put(s_in.at[16], n_in.at[16], 2)
    put(t_in.at[16], b_in.at[16], 3)
    for a in range(4):
        for k in range(2):
            x = packed[across(a, IN0 + k), :]
            xt[pl.ds(32 * a + 2 * k, 8, stride=4), :] = x
            xt[pl.ds(32 * a + 2 * k + 1, 8, stride=4), :] = right(x, x)
    cols = xt[0:128, :].T
    s_in0[...] = cols[:64]
    t_in0[...] = cols[:64].astype(bf)
    put(s_in0, n_in0, 4)
    put(t_in0, b_in0, 5)

    def out_body(t, carry):
        for a in range(4):
            for p in range(2):
                for h in range(2):
                    s_out[h, t, pl.ds(16 * a + p, 8, stride=2), :] = packed[across(a, OUT + 4 * t + 2 * p + h), :]
        for h in range(2):
            t_out[h, t] = s_out[h, t].astype(bf)
            put(s_out.at[h, t], n_out.at[t, :, pl.ds(128 * h, 128)], 6)
            put(t_out.at[h, t], b_out.at[t, :, pl.ds(128 * h, 128)], 7)
        return carry

    lax.fori_loop(0, N_OUT, out_body, 0)
    for h in range(2):
        for a in range(4):
            for p in range(4):
                s_short[h, pl.ds(32 * a + p, 8, stride=4), :] = packed[across(a, SHORT + 2 * p + h), :]
        t_short[h] = s_short[h].astype(bf)
        put(s_short.at[h], n_short.at[:, pl.ds(128 * h, 128)], 8)
        put(t_short.at[h], b_short.at[:, pl.ds(128 * h, 128)], 9)
    for i in range(N_DEV):
        xt[8 * i:8 * i + 8, :] = packed[i * ROWS + FC:i * ROWS + FC + 8, :]
    for h in range(2):
        cols = xt[128 * h:128 * h + 128, :].T
        s_fc[:, 128 * h:128 * h + 128] = cols[:CLASSES]
        t_fc[:, 128 * h:128 * h + 128] = cols[:CLASSES].astype(bf)
    put(s_fc, n_fc, 10)
    put(t_fc, b_fc, 11)

    lane = lax.broadcasted_iota(jnp.int32, (8, LANES), 1)
    for b in range(2):
        def even(k):
            return packed[pl.ds(16 * b * ROWS + BN + k, 8, stride=2 * ROWS), :]

        def odd(k):
            return packed[pl.ds((16 * b + 1) * ROWS + BN + k, 8, stride=2 * ROWS), :]

        for k in range(3):
            n_bn[pl.ds(56 * b + k, 8, stride=7), :] = even(k)
            n_bn[pl.ds(56 * b + 4 + k, 8, stride=7), :] = odd(1 + k)
        n_bn[pl.ds(56 * b + 3, 8, stride=7), :] = jnp.where(lane < 64, even(3), odd(0))
    total = packed[across(0, BIAS), :]
    for a in range(1, 4):
        total = total + packed[across(a, BIAS), :]
    n_bias[...] = jnp.sum(total, axis=0, keepdims=True)

    for ref, base, tiles, count in ((v_mid, MID, 9, N_MID), (v_in, IN, 4, N_IN), (v_out, OUT, 4, N_OUT)):
        for m in range(tiles):
            for t in range(0, count, 8):
                size = min(8, count - t)
                ref[t:t + size, 128 * m:128 * m + 128] = v_own[pl.ds(base + tiles * t + m, size, stride=tiles), :]
    v_small[0:2, :] = v_own[IN0:IN0 + 2, :]
    v_small[8:32, :] = v_own[SHORT:SHORT + 24, :]

    for k, (src, dst) in enumerate(((s_mid, n_mid), (t_mid, b_mid), (s_in, n_in), (t_in, b_in), (s_in0, n_in0),
                                    (t_in0, b_in0))):
        pltpu.make_async_copy(src, dst, sems.at[k]).wait()
    for h in range(2):
        half = pl.ds(128 * h, 128)
        for k, (src, dst) in enumerate(((s_out, n_out.at[:, :, half]), (t_out, b_out.at[:, :, half]),
                                        (s_short, n_short.at[:, half]), (t_short, b_short.at[:, half]))):
            pltpu.make_async_copy(src.at[h], dst, sems.at[6 + k]).wait()
    pltpu.make_async_copy(s_fc, n_fc, sems.at[10]).wait()
    pltpu.make_async_copy(t_fc, b_fc, sems.at[11]).wait()


def unpack_weights(packed, v_own):
    any_ = pl.BlockSpec(memory_space=pl.ANY)
    vm = pl.BlockSpec(memory_space=VMEM)
    bf = jnp.bfloat16
    kernels = ((N_MID, 576, 64), (N_IN, 64, 256), (64, 128), (N_OUT, 64, 256), (128, 256), (CLASSES, 256))
    shapes = [(s, F32) for s in kernels] + [((112, 128), F32), ((1, 128), F32)] + [(s, bf) for s in kernels]
    shapes += [((N_MID, 1152), F32), ((N_IN, 512), F32), ((N_OUT, 512), F32), ((32, LANES), F32)]
    scratch = ((N_MID, 576, 64), (N_IN, 64, 256), (2, N_OUT, 64, 128), (2, 128, 128), (64, 128), (CLASSES, 256))
    return pl.pallas_call(
        unpack_kernel,
        out_shape=[jax.ShapeDtypeStruct(s, d) for s, d in shapes],
        in_specs=[vm, vm],
        out_specs=[any_] * 6 + [vm] * 2 + [any_] * 6 + [vm] * 4,
        scratch_shapes=[VMEM(s, F32) for s in scratch] + [VMEM(s, bf) for s in scratch]
        + [VMEM((256, 128), F32), pltpu.SemaphoreType.DMA((12,))],
        compiler_params=pltpu.CompilerParams(vmem_limit_bytes=40 * 2**20),
    )(packed, v_own)


def exchange(packed, w_own, v_own, learn_rate):
    rank = lax.axis_index('dp')
    grad = lax.psum_scatter(packed.reshape(N_DEV, ROWS, LANES), 'dp', scatter_dimension=0, tiled=True)[0] / N_DEV
    ids = tensor_of_row(jnp.arange(ROWS))
    member = ids[:, None] == jnp.arange(64)[None, :]
    sums = jnp.stack([jnp.sum(grad * grad, axis=1), jnp.sum(w_own * w_own, axis=1)])
    partial = jnp.sum(jnp.where(member[None], sums[:, :, None], 0.0), axis=1)
    total = lax.psum(partial, 'dp')
    g_norm = jnp.sqrt(total[0])
    w_norm = jnp.sqrt(total[1])
    trust = jnp.where((w_norm > 0) & (g_norm > 0), TRUST_COEF * w_norm / (g_norm + DECAY * w_norm), 1.0)
    trust = jnp.sum(jnp.where(member, trust[None], 0.0), axis=1)
    plain = ids == ID_PLAIN
    trust = jnp.where(plain, 1.0, trust)[:, None]
    decay = jnp.where(plain, 0.0, DECAY)[:, None]
    v_next = MOMENTUM * v_own + learn_rate * trust * (grad + decay * w_own)
    lane = jnp.arange(LANES)
    mine = (jnp.arange(ROWS)[:, None] != BIAS) | ((lane >= 4 * rank) & (lane < 4 * rank + 4))[None]
    w_next = jnp.where(mine, w_own - v_next, 0.0)
    gathered = lax.all_gather(w_next, 'dp', axis=0, tiled=True)
    return gathered, v_next


def solution(mesh):
    spec_full = P()
    spec_lead = P('dp')
    spec_cols = P(None, 'dp')
    moment_specs = (spec_lead, spec_lead, spec_cols, spec_cols, spec_cols, spec_lead, spec_lead, spec_lead)
    in_specs = (spec_full,) * 8 + (spec_lead,) * 8 + moment_specs + (spec_full,)
    out_specs = (spec_full,) * 14 + moment_specs

    def body(w_in0, w_short, w_in, w_mid, w_out, w_fc, w_bn, w_bias,
             g_in0, g_short, g_in, g_mid, g_out, g_bn, pooled, dlogits,
             v_in0, v_short, v_in, v_mid, v_out, v_fc, v_bn, v_bias, learn_rate):
        rank = lax.axis_index('dp')
        odd = rank % 2 == 1
        lane = jnp.arange(LANES)
        v_bn_rows = jnp.where(odd, jnp.pad(v_bn, (64, 0)), jnp.pad(v_bn, (0, 64))).reshape(4, LANES)
        v_bias_row = lax.dynamic_update_slice(jnp.zeros((1, LANES), F32), v_bias[None], (0, 4 * rank))
        v_small = jnp.concatenate([
            jnp.pad(v_in0.reshape(2, LANES), ((0, 6), (0, 0))), v_short.reshape(8, LANES),
            jnp.pad(v_fc.reshape(8, CLASSES), ((0, 0), (0, LANES - CLASSES))),
            v_bn_rows, v_bias_row, jnp.zeros((3, LANES), F32)])
        packed, w_own, v_own = pack_grads((
            g_mid.reshape(N_MID, 576, 64), jnp.swapaxes(g_in[0], 1, 2), g_in0[0].T, g_out[0], g_short[0],
            g_bn.reshape(112, LANES), pooled, dlogits.T,
            w_mid.reshape(N_MID, 576, 64), jnp.swapaxes(w_in, 1, 2), w_in0.T, w_out, w_short, w_fc.T,
            w_bn.reshape(112, LANES), jnp.pad(w_bias, (0, LANES - CLASSES))[None], v_mid, v_in, v_out, v_small))
        gathered, v_next = exchange(packed, w_own, v_own, learn_rate)
        (n_mid, n_in, n_in0, n_out, n_short, n_fc, n_bn, n_bias, b_mid, b_in, b_in0, b_out, b_short, b_fc,
         m_mid, m_in, m_out, m_small) = unpack_weights(gathered, v_next)
        m_bn = m_small[24:28].reshape(-1)
        m_bn = jnp.where(odd, m_bn[64:], m_bn[:448])
        m_bias = lax.dynamic_slice(m_small, (28, 4 * rank), (1, 4))[0]
        return (n_in0.T, n_short, jnp.swapaxes(n_in, 1, 2), n_mid.reshape(w_mid.shape), n_out, n_fc.T,
                n_bn.reshape(-1), n_bias[0, :CLASSES],
                b_in0.T, b_short, jnp.swapaxes(b_in, 1, 2), b_mid.reshape(w_mid.shape), b_out, b_fc.T,
                m_small[0:2].reshape(-1), m_small[8:16].reshape(-1), m_in, m_mid, m_out,
                m_small[16:24, :CLASSES].reshape(-1), m_bn, m_bias)

    return jax.shard_map(body, mesh=mesh, in_specs=in_specs, out_specs=out_specs, check_vma=False)
```

```python
import functools
import jax
import jax.numpy as jnp
from jax import lax
from jax.experimental import pallas as pl
from jax.experimental.pallas import tpu as pltpu
from jax.sharding import PartitionSpec as P

MOMENTUM = 0.9
TRUST_COEF = 0.001
DECAY = 0.0001
N_DEV = 32
LANES = 128
MID, IN0, IN, OUT, SHORT, FC, BN, BIAS, ROWS = 0, 162, 164, 232, 304, 312, 320, 324, 328
N_MID, N_IN, N_OUT = 18, 17, 18
CLASSES = 100
ID_IN0, ID_IN, ID_OUT, ID_SHORT, ID_FC, ID_PLAIN = 18, 19, 36, 54, 55, 56
F32 = jnp.float32
VMEM = pltpu.VMEM


def left(a, b):
    return jnp.concatenate([a[:, :64], b[:, :64]], axis=1)


def right(a, b):
    return jnp.concatenate([a[:, 64:], b[:, 64:]], axis=1)


def across(piece8, row):
    return pl.ds(piece8 * 8 * ROWS + row, 8, stride=ROWS)


def pack_kernel(g_mid, g_in, g_in0, g_out, g_short, g_bn, pooled, dlog_t,
                w_mid, w_in, w_in0, w_out, w_short, w_fc, w_bn, w_bias, v_mid, v_in, v_out, v_small,
                packed, w_own, v_own,
                s_mid, s_in, s_in0, s_out, s_short, s_bn, s_x, s_d, xt, fct,
                o_mid, o_in, o_in0, o_out, o_short, o_fc, o_bn, ot, sems):
    rank = lax.axis_index('dp')
    copies = []

    def fetch(src, dst):
        copy = pltpu.make_async_copy(src, dst, sems.at[len(copies)])
        copy.start()
        copies.append(copy)
        return copy

    c_mid = fetch(g_mid, s_mid)
    c_in = fetch(g_in, s_in)
    c_in0 = fetch(g_in0, s_in0)
    c_out = [fetch(g_out.at[:, :, pl.ds(128 * h, 128)], s_out.at[h]) for h in range(2)]
    c_short = [fetch(g_short.at[:, pl.ds(128 * h, 128)], s_short.at[h]) for h in range(2)]
    c_bn = fetch(g_bn, s_bn)
    c_fc = [fetch(pooled, s_x), fetch(dlog_t, s_d)]
    mid_at = pl.multiple_of((18 * rank) // 8 * 8, 8)
    mid_off = 18 * rank - mid_at
    out_at = pl.multiple_of((2 * rank) // 8 * 8, 8)
    out_off = 2 * lax.rem(rank, 4)
    short_at = pl.multiple_of((4 * rank) // 8 * 8, 8)
    short_off = 4 * lax.rem(rank, 2)
    col_at = pl.multiple_of((rank // 16) * 128, 128)
    col_off = pl.multiple_of(lax.rem(rank, 16) * 8, 8)
    c_own = [
        fetch(w_mid.at[:, pl.ds(mid_at, 24), :], o_mid),
        fetch(w_in.at[:, :, pl.ds(col_at, 128)], o_in),
        fetch(w_in0, o_in0),
        fetch(w_out.at[:, pl.ds(out_at, 8), pl.ds(0, 128)], o_out.at[0]),
        fetch(w_out.at[:, pl.ds(out_at, 8), pl.ds(128, 128)], o_out.at[1]),
        fetch(w_short.at[pl.ds(short_at, 8), pl.ds(0, 128)], o_short.at[0]),
        fetch(w_short.at[pl.ds(short_at, 8), pl.ds(128, 128)], o_short.at[1]),
        fetch(w_fc.at[:, pl.ds(col_at, 128)], o_fc),
        fetch(w_bn, o_bn),
    ]

    for ref, base, tiles, count in ((v_mid, MID, 9, N_MID), (v_in, IN, 4, N_IN), (v_out, OUT, 4, N_OUT)):
        for m in range(tiles):
            for t in range(0, count, 8):
                size = min(8, count - t)
                v_own[pl.ds(base + tiles * t + m, size, stride=tiles), :] = ref[t:t + size, 128 * m:128 * m + 128]
    v_own[IN0:IN0 + 2, :] = v_small[0:2, :]
    v_own[SHORT:SHORT + 24, :] = v_small[8:32, :]

    c_mid.wait()

    def mid_body(t, carry):
        for a in range(4):
            for k in range(9):
                even = s_mid[t, pl.ds(144 * a + 2 * k, 8, stride=18), :]
                odd = s_mid[t, pl.ds(144 * a + 2 * k + 1, 8, stride=18), :]
                packed[across(a, MID + 9 * t + k), :] = jnp.concatenate([even, odd], axis=1)
        return carry

    lax.fori_loop(0, N_MID, mid_body, 0)
    c_in.wait()
    c_in0.wait()

    def in_rows(t, other):
        for a in range(4):
            for k in range(4):
                even = xt[pl.ds(64 * a + 2 * k, 8, stride=8), :]
                odd = xt[pl.ds(64 * a + 2 * k + 1, 8, stride=8), :]
                packed[across(a, IN + 4 * t + k), :] = left(even, odd)
                if other is not None:
                    packed[across(a, IN + 4 * other + k), :] = right(even, odd)

    def in_body(t, carry):
        both = jnp.concatenate([s_in[t], s_in[t + 8]], axis=0)
        for h in range(2):
            xt[128 * h:128 * h + 128, :] = both[:, 128 * h:128 * h + 128].T
        in_rows(t, t + 8)
        return carry

    lax.fori_loop(0, 8, in_body, 0)
    last = jnp.concatenate([s_in[16], jnp.concatenate([s_in0[...], s_in0[...]], axis=1)], axis=0)
    for h in range(2):
        xt[128 * h:128 * h + 128, :] = last[:, 128 * h:128 * h + 128].T
    in_rows(16, None)
    for a in range(4):
        for k in range(2):
            even = xt[pl.ds(32 * a + 2 * k, 8, stride=4), :]
            odd = xt[pl.ds(32 * a + 2 * k + 1, 8, stride=4), :]
            packed[across(a, IN0 + k), :] = right(even, odd)
    for copy in c_out + c_short:
        copy.wait()

    def out_body(t, carry):
        for a in range(4):
            for p in range(2):
                for h in range(2):
                    packed[across(a, OUT + 4 * t + 2 * p + h), :] = s_out[h, t, pl.ds(16 * a + p, 8, stride=2), :]
        return carry

    lax.fori_loop(0, N_OUT, out_body, 0)
    for a in range(4):
        for p in range(4):
            for h in range(2):
                packed[across(a, SHORT + 2 * p + h), :] = s_short[h, pl.ds(32 * a + p, 8, stride=4), :]
    for i in range(N_DEV):
        packed[i * ROWS + BN:i * ROWS + ROWS, :] = jnp.zeros((8, LANES), F32)
    c_bn.wait()
    for b in range(2):
        for k in range(4):
            for half in range(2):
                packed[pl.ds((16 * b + half) * ROWS + BN + k, 8, stride=2 * ROWS), :] = (
                    s_bn[pl.ds(56 * b + 3 * half + k, 8, stride=7), :])
    for copy in c_fc:
        copy.wait()
    scale = 1.0 / s_x.shape[0]
    fct[...] = jnp.zeros_like(fct)
    fct[0:CLASSES, :] = jnp.dot(s_d[...], s_x[...], preferred_element_type=F32) * scale
    bias = lax.dot_general(jnp.ones((8, s_d.shape[1]), jnp.bfloat16), s_d[...], (((1,), (1,)), ((), ())),
                           preferred_element_type=F32) * scale
    bias = jnp.concatenate([bias, jnp.zeros((8, LANES - CLASSES), F32)], axis=1)
    for a in range(4):
        packed[across(a, BIAS), :] = bias
    for h in range(2):
        cols = fct[:, 128 * h:128 * h + 128].T
        for j in range(16):
            at = (16 * h + j) * ROWS + FC
            packed[at:at + 8, :] = cols[8 * j:8 * j + 8, :]

    for copy in c_own:
        copy.wait()
    for t in range(N_MID):
        even = o_mid[t, pl.ds(mid_off, 9, stride=2), :]
        odd = o_mid[t, pl.ds(mid_off + 1, 9, stride=2), :]
        w_own[MID + 9 * t:MID + 9 * t + 9, :] = jnp.concatenate([even, odd], axis=1)
    for t in range(9):
        other = o_in[t + 8] if t < 8 else o_in0[...]
        ot[...] = jnp.concatenate([o_in[2 * 8 if t == 8 else t], other], axis=0).T
        even = ot[pl.ds(col_off, 4, stride=2), :]
        odd = ot[pl.ds(col_off + 1, 4, stride=2), :]
        here = 16 if t == 8 else t
        w_own[IN + 4 * here:IN + 4 * here + 4, :] = left(even, odd)
        if t < 8:
            w_own[IN + 4 * (t + 8):IN + 4 * (t + 8) + 4, :] = right(even, odd)
    even = ot[pl.ds(4 * rank, 2, stride=2), :]
    odd = ot[pl.ds(4 * rank + 1, 2, stride=2), :]
    w_own[IN0:IN0 + 2, :] = right(even, odd)
    for p in range(2):
        for h in range(2):
            for t in range(N_OUT):
                w_own[OUT + 4 * t + 2 * p + h:OUT + 4 * t + 2 * p + h + 1, :] = o_out[h, t, pl.ds(out_off + p, 1), :]
    for p in range(4):
        for h in range(2):
            w_own[SHORT + 2 * p + h:SHORT + 2 * p + h + 1, :] = o_short[h, pl.ds(short_off + p, 1), :]
    fct[0:CLASSES, 0:LANES] = o_fc[...]
    ot[...] = fct[:, 0:LANES].T
    w_own[FC:FC + 8, :] = jnp.where(lax.broadcasted_iota(jnp.int32, (8, LANES), 1) < CLASSES,
                                    ot[pl.ds(col_off, 8), :], 0.0)
    w_own[BN:ROWS, :] = jnp.zeros((8, LANES), F32)
    bn_at = 7 * (rank // 2) + 3 * lax.rem(rank, 2)
    for k in range(4):
        w_own[BN + k:BN + k + 1, :] = o_bn[pl.ds(bn_at + k, 1), :]
    lane = lax.broadcasted_iota(jnp.int32, (1, LANES), 1)
    w_own[BIAS:BIAS + 1, :] = jnp.where((lane >= 4 * rank) & (lane < 4 * rank + 4), w_bias[...], 0.0)


def pack_grads(ops):
    any_ = pl.BlockSpec(memory_space=pl.ANY)
    vm = pl.BlockSpec(memory_space=VMEM)
    return pl.pallas_call(
        pack_kernel,
        out_shape=(jax.ShapeDtypeStruct((N_DEV * ROWS, LANES), F32), jax.ShapeDtypeStruct((ROWS, LANES), F32),
                   jax.ShapeDtypeStruct((ROWS, LANES), F32)),
        in_specs=[any_] * 15 + [vm] * 5,
        out_specs=(vm, vm, vm),
        scratch_shapes=[
            VMEM((N_MID, 576, 64), F32), VMEM((N_IN, 64, 256), F32), VMEM((64, 128), F32),
            VMEM((2, N_OUT, 64, 128), F32), VMEM((2, 128, 128), F32), VMEM((112, 128), F32),
            VMEM((1024, 256), jnp.bfloat16), VMEM((CLASSES, 1024), jnp.bfloat16),
            VMEM((256, 128), F32), VMEM((128, 256), F32),
            VMEM((N_MID, 24, 64), F32), VMEM((N_IN, 64, 128), F32), VMEM((64, 128), F32),
            VMEM((2, N_OUT, 8, 128), F32), VMEM((2, 8, 128), F32), VMEM((CLASSES, 128), F32),
            VMEM((112, 128), F32), VMEM((128, 128), F32),
            pltpu.SemaphoreType.DMA((24,)),
        ],
        compiler_params=pltpu.CompilerParams(vmem_limit_bytes=60 * 2**20),
    )(*ops)


def unpack_kernel(packed, v_own, n_mid, n_in, n_in0, n_out, n_short, n_fc, n_bn, n_bias,
                  b_mid, b_in, b_in0, b_out, b_short, b_fc, v_mid, v_in, v_out, v_small,
                  s_mid, s_in, s_out, s_short, s_in0, s_fc, t_mid, t_in, t_out, t_short, t_in0, t_fc, xt, sems):
    bf = jnp.bfloat16

    def put(src, dst, k):
        pltpu.make_async_copy(src, dst, sems.at[k]).start()

    def mid_body(t, carry):
        for a in range(4):
            for k in range(9):
                x = packed[across(a, MID + 9 * t + k), :]
                s_mid[t, pl.ds(144 * a + 2 * k, 8, stride=18), :] = x[:, :64]
                s_mid[t, pl.ds(144 * a + 2 * k + 1, 8, stride=18), :] = x[:, 64:]
        put(s_mid.at[t], n_mid.at[t], 0)
        t_mid[t] = s_mid[t].astype(bf)
        put(t_mid.at[t], b_mid.at[t], 1)
        return carry

    lax.fori_loop(0, N_MID, mid_body, 0)

    def in_rows(t, other):
        for a in range(4):
            for k in range(4):
                x = packed[across(a, IN + 4 * t + k), :]
                y = packed[across(a, IN + 4 * other + k), :] if other is not None else x
                xt[pl.ds(64 * a + 2 * k, 8, stride=8), :] = left(x, y)
                xt[pl.ds(64 * a + 2 * k + 1, 8, stride=8), :] = right(x, y)

    def in_body(t, carry):
        in_rows(t, t + 8)
        for h in range(2):
            cols = xt[128 * h:128 * h + 128, :].T
            s_in[t, :, 128 * h:128 * h + 128] = cols[:64]
            s_in[t + 8, :, 128 * h:128 * h + 128] = cols[64:]
            t_in[t, :, 128 * h:128 * h + 128] = cols[:64].astype(bf)
            t_in[t + 8, :, 128 * h:128 * h + 128] = cols[64:].astype(bf)
        for u in (t, t + 8):
            put(s_in.at[u], n_in.at[u], 2)
            put(t_in.at[u], b_in.at[u], 3)
        return carry

    lax.fori_loop(0, 8, in_body, 0)
    in_rows(16, None)
    for h in range(2):
        cols = xt[128 * h:128 * h + 128, :].T
        s_in[16, :, 128 * h:128 * h + 128] = cols[:64]
        t_in[16, :, 128 * h:128 * h + 128] = cols[:64].astype(bf)
    put(s_in.at[16], n_in.at[16], 2)
    put(t_in.at[16], b_in.at[16], 3)
    for a in range(4):
        for k in range(2):
            x = packed[across(a, IN0 + k), :]
            xt[pl.ds(32 * a + 2 * k, 8, stride=4), :] = x
            xt[pl.ds(32 * a + 2 * k + 1, 8, stride=4), :] = right(x, x)
    cols = xt[0:128, :].T
    s_in0[...] = cols[:64]
    t_in0[...] = cols[:64].astype(bf)
    put(s_in0, n_in0, 4)
    put(t_in0, b_in0, 5)

    def out_body(t, carry):
        for a in range(4):
            for p in range(2):
                for h in range(2):
                    s_out[h, t, pl.ds(16 * a + p, 8, stride=2), :] = packed[across(a, OUT + 4 * t + 2 * p + h), :]
        for h in range(2):
            t_out[h, t] = s_out[h, t].astype(bf)
            put(s_out.at[h, t], n_out.at[t, :, pl.ds(128 * h, 128)], 6)
            put(t_out.at[h, t], b_out.at[t, :, pl.ds(128 * h, 128)], 7)
        return carry

    lax.fori_loop(0, N_OUT, out_body, 0)
    for h in range(2):
        for a in range(4):
            for p in range(4):
                s_short[h, pl.ds(32 * a + p, 8, stride=4), :] = packed[across(a, SHORT + 2 * p + h), :]
        t_short[h] = s_short[h].astype(bf)
        put(s_short.at[h], n_short.at[:, pl.ds(128 * h, 128)], 8)
        put(t_short.at[h], b_short.at[:, pl.ds(128 * h, 128)], 9)
    for i in range(N_DEV):
        xt[8 * i:8 * i + 8, :] = packed[i * ROWS + FC:i * ROWS + FC + 8, :]
    for h in range(2):
        cols = xt[128 * h:128 * h + 128, :].T
        s_fc[:, 128 * h:128 * h + 128] = cols[:CLASSES]
        t_fc[:, 128 * h:128 * h + 128] = cols[:CLASSES].astype(bf)
    put(s_fc, n_fc, 10)
    put(t_fc, b_fc, 11)

    lane = lax.broadcasted_iota(jnp.int32, (8, LANES), 1)
    for b in range(2):
        def even(k):
            return packed[pl.ds(16 * b * ROWS + BN + k, 8, stride=2 * ROWS), :]

        def odd(k):
            return packed[pl.ds((16 * b + 1) * ROWS + BN + k, 8, stride=2 * ROWS), :]

        for k in range(3):
            n_bn[pl.ds(56 * b + k, 8, stride=7), :] = even(k)
            n_bn[pl.ds(56 * b + 4 + k, 8, stride=7), :] = odd(1 + k)
        n_bn[pl.ds(56 * b + 3, 8, stride=7), :] = jnp.where(lane < 64, even(3), odd(0))
    total = packed[across(0, BIAS), :]
    for a in range(1, 4):
        total = total + packed[across(a, BIAS), :]
    n_bias[...] = jnp.sum(total, axis=0, keepdims=True)

    for ref, base, tiles, count in ((v_mid, MID, 9, N_MID), (v_in, IN, 4, N_IN), (v_out, OUT, 4, N_OUT)):
        for m in range(tiles):
            for t in range(0, count, 8):
                size = min(8, count - t)
                ref[t:t + size, 128 * m:128 * m + 128] = v_own[pl.ds(base + tiles * t + m, size, stride=tiles), :]
    v_small[0:2, :] = v_own[IN0:IN0 + 2, :]
    v_small[8:32, :] = v_own[SHORT:SHORT + 24, :]

    for k, (src, dst) in enumerate(((s_mid, n_mid), (t_mid, b_mid), (s_in, n_in), (t_in, b_in), (s_in0, n_in0),
                                    (t_in0, b_in0))):
        pltpu.make_async_copy(src, dst, sems.at[k]).wait()
    for h in range(2):
        half = pl.ds(128 * h, 128)
        for k, (src, dst) in enumerate(((s_out, n_out.at[:, :, half]), (t_out, b_out.at[:, :, half]),
                                        (s_short, n_short.at[:, half]), (t_short, b_short.at[:, half]))):
            pltpu.make_async_copy(src.at[h], dst, sems.at[6 + k]).wait()
    pltpu.make_async_copy(s_fc, n_fc, sems.at[10]).wait()
    pltpu.make_async_copy(t_fc, b_fc, sems.at[11]).wait()


def unpack_weights(packed, v_own):
    any_ = pl.BlockSpec(memory_space=pl.ANY)
    vm = pl.BlockSpec(memory_space=VMEM)
    bf = jnp.bfloat16
    kernels = ((N_MID, 576, 64), (N_IN, 64, 256), (64, 128), (N_OUT, 64, 256), (128, 256), (CLASSES, 256))
    shapes = [(s, F32) for s in kernels] + [((112, 128), F32), ((1, 128), F32)] + [(s, bf) for s in kernels]
    shapes += [((N_MID, 1152), F32), ((N_IN, 512), F32), ((N_OUT, 512), F32), ((32, LANES), F32)]
    scratch = ((N_MID, 576, 64), (N_IN, 64, 256), (2, N_OUT, 64, 128), (2, 128, 128), (64, 128), (CLASSES, 256))
    return pl.pallas_call(
        unpack_kernel,
        out_shape=[jax.ShapeDtypeStruct(s, d) for s, d in shapes],
        in_specs=[vm, vm],
        out_specs=[any_] * 6 + [vm] * 2 + [any_] * 6 + [vm] * 4,
        scratch_shapes=[VMEM(s, F32) for s in scratch] + [VMEM(s, bf) for s in scratch]
        + [VMEM((256, 128), F32), pltpu.SemaphoreType.DMA((12,))],
        compiler_params=pltpu.CompilerParams(vmem_limit_bytes=60 * 2**20),
    )(packed, v_own)

CHUNKS = ((0, 72, 'x'), (72, 72, 'y'), (144, 48, 'x'), (192, 48, 'y'), (240, 48, 'x'), (288, 40, 'y'))
STEPS = (
    (0, 0), (1, 0), (0, 1), (4, 0), (2, 0), (3, 0), (4, 1), (1, 1), (0, 2), (3, 1), (1, 2), (0, 3), (2, 1), (4, 2),
    (5, 0), (1, 3), (5, 1), (3, 2), (4, 3), (2, 2), (3, 3), (1, 4), (5, 2), (2, 3), (0, 4), (4, 4), (5, 3), (1, 5),
    (3, 4), (0, 5), (2, 4), (5, 4), (3, 5), (1, 6), (5, 5), (0, 6), (2, 5), (1, 7), (3, 6), (0, 7), (4, 5), (2, 6),
    (4, 6), (1, 8), (5, 6), (3, 7), (2, 7), (4, 7), (5, 7), (2, 8), (1, 9), (0, 8), (2, 9), (3, 8), (5, 8), (0, 9),
    (3, 9), (4, 8), (5, 9), (4, 9),
)
STAGES = 10
S_CORE, S_ONE, S_TWO, S_Z, A_Z, A_TWO, A_ONE, A_CORE, N_SEMS = 0, 1, 2, 2, 5, 9, 10, 11, 12
MESH = pl.DeviceIdType.MESH


def first_row(t):
    out = jnp.where(t < N_MID, 9 * t, IN0)
    out = jnp.where(t >= ID_IN, IN + 4 * (t - ID_IN), out)
    out = jnp.where(t >= ID_OUT, OUT + 4 * (t - ID_OUT), out)
    return jnp.where(t >= ID_SHORT, SHORT + 8 * (t - ID_SHORT), out)


def exchange_kernel(lr, packed, w_own, v_own, full, v_new,
                    got_core, acc, got_one, got_two, got_z, grad, norms, send, recv, n_send, n_recv):
    rank = lax.axis_index('dp')
    core = lax.rem(rank, 2)
    x = lax.rem(rank // 2, 2)
    y = lax.rem(rank // 4, 2)
    z = rank // 8

    def device(zz, yy, xx, cc):
        return (((zz * 2 + yy) * 2 + xx) * 2 + cc,)

    core_peer = device(z, y, x, 1 - core)
    x_peer = device(z, y, 1 - x, core)
    y_peer = device(z, 1 - y, x, core)

    barrier = pltpu.get_barrier_semaphore()

    def greet(d, carry):
        pl.semaphore_signal(barrier, inc=1, device_id=(lax.rem(rank + d, N_DEV),), device_id_type=MESH)
        return carry

    lax.fori_loop(1, N_DEV, greet, 0)
    pl.semaphore_wait(barrier, N_DEV - 1)

    copies = {}

    def start(c, k, src, dst, peer):
        copy = pltpu.make_async_remote_copy(src_ref=src, dst_ref=dst, send_sem=send.at[c * N_SEMS + k],
                                            recv_sem=recv.at[c * N_SEMS + k], device_id=peer, device_id_type=MESH)
        copy.start()
        copies[c, k] = copy

    def arrived(c, k):
        copies[c, k].wait_recv()

    def step(c, stage):
        at, size, first = CHUNKS[c]
        rows = pl.ds(at, size)
        x_first = first == 'x'
        one_peer, two_peer = (x_peer, y_peer) if x_first else (y_peer, x_peer)

        def half(zz, yx, mine):
            return (zz, yx, x if mine else 1 - x) if x_first else (zz, y if mine else 1 - y, yx)

        if stage == 0:
            start(c, S_CORE, packed.at[:, :, :, 1 - core, rows, :], got_core.at[:, :, :, rows, :], core_peer)
        elif stage == 1:
            arrived(c, S_CORE)

            def add(mine):
                def body(m, carry):
                    zz, yx = m // 2, lax.rem(m, 2)
                    a, b, d = half(zz, yx, mine)
                    acc[a, b, d, rows, :] = packed[a, b, d, core, rows, :] + got_core[a, b, d, rows, :]
                    return carry

                lax.fori_loop(0, 8, body, 0)

            add(False)
            src = acc.at[:, :, 1 - x, rows, :] if x_first else acc.at[:, 1 - y, :, rows, :]
            start(c, S_ONE, src, got_one.at[:, :, rows, :], one_peer)
            add(True)
        elif stage == 2:
            arrived(c, S_ONE)

            def add(other):
                def body(zz, carry):
                    a, b, d = half(zz, other, True)
                    acc[a, b, d, rows, :] = acc[a, b, d, rows, :] + got_one[zz, other, rows, :]
                    return carry

                lax.fori_loop(0, 4, body, 0)

            here = y if x_first else x
            add(1 - here)
            src = acc.at[:, 1 - y, x, rows, :] if x_first else acc.at[:, y, 1 - x, rows, :]
            start(c, S_TWO, src, got_two.at[:, rows, :], two_peer)
            add(here)
        elif stage == 3:
            arrived(c, S_TWO)
            for d in (1, 2, 3, 0):
                zz = lax.rem(z + d, 4)
                acc[zz, y, x, rows, :] = acc[zz, y, x, rows, :] + got_two[zz, rows, :]
                if d:
                    start(c, S_Z + d, acc.at[zz, y, x, rows, :], got_z.at[d - 1, rows, :], device(zz, y, x, core))
        elif stage == 4:
            for d in (1, 2, 3):
                arrived(c, S_Z + d)
            mean = (acc[z, y, x, rows, :] + got_z[0, rows, :] + got_z[1, rows, :] + got_z[2, rows, :]) * (1.0 / N_DEV)
            grad[rows, :] = mean
            own = w_own[rows, :]
            g_sum = jnp.sum(mean * mean, axis=1, keepdims=True)
            w_sum = jnp.sum(own * own, axis=1, keepdims=True)
            row = lax.broadcasted_iota(jnp.int32, (size, LANES), 0) + at
            lane = lax.broadcasted_iota(jnp.int32, (size, LANES), 1)
            tensor = jnp.where(lane < 64, lane, lane - 64)
            member = (row >= first_row(tensor)) & (row < first_row(tensor + 1))
            part = jnp.where(member, jnp.where(lane < 64, g_sum, w_sum), 0.0)
            norms[c, rank] = jnp.sum(part, axis=0, keepdims=True)

            def tell(d, carry):
                pltpu.make_async_remote_copy(
                    src_ref=norms.at[c, rank], dst_ref=norms.at[c, rank], send_sem=n_send.at[c],
                    recv_sem=n_recv.at[c], device_id=(lax.rem(rank + d, N_DEV),), device_id_type=MESH).start()
                return carry

            lax.fori_loop(1, N_DEV, tell, 0)
        elif stage == 5:
            others = norms.at[c, pl.ds(0, N_DEV - 1)]
            pltpu.make_async_copy(others, others, n_recv.at[c]).wait()
            total = jnp.sum(norms[c], axis=0)
            g_norm = jnp.sqrt(total)
            w_norm = pltpu.roll(g_norm, 64, 1)
            trust = jnp.where((w_norm > 0) & (g_norm > 0), TRUST_COEF * w_norm / (g_norm + DECAY * w_norm), 1.0)
            row = lax.broadcasted_iota(jnp.int32, (size, LANES), 0) + at
            lane = lax.broadcasted_iota(jnp.int32, (size, LANES), 1)
            trust = jnp.where(lane == ID_PLAIN, 1.0, trust)
            member = (row >= first_row(lane)) & (row < first_row(lane + 1)) & (lane <= ID_PLAIN)
            rate = lr[0] * jnp.sum(jnp.where(member, trust, 0.0), axis=1, keepdims=True)
            decay = jnp.where(row < BN, DECAY, 0.0)
            own = w_own[rows, :]
            moment = MOMENTUM * v_own[rows, :] + rate * (grad[rows, :] + decay * own)
            v_new[rows, :] = moment
            mine = (row != BIAS) | ((lane >= 4 * rank) & (lane < 4 * rank + 4))
            full[z, y, x, core, rows, :] = jnp.where(mine, own - moment, 0.0)
            for d in (1, 2, 3):
                piece = full.at[z, y, x, core, rows, :]
                start(c, A_Z + d, piece, piece, device(lax.rem(z + d, 4), y, x, core))
        elif stage == 6:
            for d in (1, 2, 3):
                arrived(c, A_Z + d)
            pieces = full.at[:, y, x, core, rows, :]
            start(c, A_TWO, pieces, pieces, two_peer)
        elif stage == 7:
            arrived(c, A_TWO)
            pieces = full.at[:, :, x, core, rows, :] if x_first else full.at[:, y, :, core, rows, :]
            start(c, A_ONE, pieces, pieces, one_peer)
        elif stage == 8:
            arrived(c, A_ONE)
            pieces = full.at[:, :, :, core, rows, :]
            start(c, A_CORE, pieces, pieces, core_peer)
        else:
            arrived(c, A_CORE)

    for c, stage in STEPS:
        step(c, stage)
    for copy in copies.values():
        copy.wait_send()
    for c in range(len(CHUNKS)):
        others = norms.at[c, pl.ds(0, N_DEV - 1)]
        pltpu.make_async_copy(others, others, n_send.at[c]).wait()


def exchange(packed, w_own, v_own, learn_rate):
    vm = pl.BlockSpec(memory_space=VMEM)
    count = len(CHUNKS)
    full, v_new = pl.pallas_call(
        exchange_kernel,
        out_shape=(jax.ShapeDtypeStruct((4, 2, 2, 2, ROWS, LANES), F32), jax.ShapeDtypeStruct((ROWS, LANES), F32)),
        in_specs=[pl.BlockSpec(memory_space=pltpu.SMEM)] + [vm] * 3,
        out_specs=(vm, vm),
        scratch_shapes=[
            VMEM((4, 2, 2, ROWS, LANES), F32), VMEM((4, 2, 2, ROWS, LANES), F32), VMEM((4, 2, ROWS, LANES), F32),
            VMEM((4, ROWS, LANES), F32), VMEM((3, ROWS, LANES), F32), VMEM((ROWS, LANES), F32),
            VMEM((count, N_DEV, 1, LANES), F32),
            pltpu.SemaphoreType.DMA((count * N_SEMS,)), pltpu.SemaphoreType.DMA((count * N_SEMS,)),
            pltpu.SemaphoreType.DMA((count,)), pltpu.SemaphoreType.DMA((count,)),
        ],
        compiler_params=pltpu.CompilerParams(vmem_limit_bytes=60 * 2**20, collective_id=0, has_side_effects=True),
    )(learn_rate.reshape(1), packed.reshape(4, 2, 2, 2, ROWS, LANES), w_own, v_own)
    return full.reshape(N_DEV * ROWS, LANES), v_new


def solution(mesh):
    spec_full = P()
    spec_lead = P('dp')
    spec_cols = P(None, 'dp')
    moment_specs = (spec_lead, spec_lead, spec_cols, spec_cols, spec_cols, spec_lead, spec_lead, spec_lead)
    in_specs = (spec_full,) * 8 + (spec_lead,) * 8 + moment_specs + (spec_full,)
    out_specs = (spec_full,) * 14 + moment_specs

    def body(w_in0, w_short, w_in, w_mid, w_out, w_fc, w_bn, w_bias,
             g_in0, g_short, g_in, g_mid, g_out, g_bn, pooled, dlogits,
             v_in0, v_short, v_in, v_mid, v_out, v_fc, v_bn, v_bias, learn_rate):
        rank = lax.axis_index('dp')
        odd = rank % 2 == 1
        lane = jnp.arange(LANES)
        v_bn_rows = jnp.where(odd, jnp.pad(v_bn, (64, 0)), jnp.pad(v_bn, (0, 64))).reshape(4, LANES)
        v_bias_row = lax.dynamic_update_slice(jnp.zeros((1, LANES), F32), v_bias[None], (0, 4 * rank))
        v_small = jnp.concatenate([
            jnp.pad(v_in0.reshape(2, LANES), ((0, 6), (0, 0))), v_short.reshape(8, LANES),
            jnp.pad(v_fc.reshape(8, CLASSES), ((0, 0), (0, LANES - CLASSES))),
            v_bn_rows, v_bias_row, jnp.zeros((3, LANES), F32)])
        packed, w_own, v_own = pack_grads((
            g_mid.reshape(N_MID, 576, 64), jnp.swapaxes(g_in[0], 1, 2), g_in0[0].T, g_out[0], g_short[0],
            g_bn.reshape(112, LANES), pooled, dlogits.T,
            w_mid.reshape(N_MID, 576, 64), jnp.swapaxes(w_in, 1, 2), w_in0.T, w_out, w_short, w_fc.T,
            w_bn.reshape(112, LANES), jnp.pad(w_bias, (0, LANES - CLASSES))[None], v_mid, v_in, v_out, v_small))
        gathered, v_next = exchange(packed, w_own, v_own, learn_rate)
        (n_mid, n_in, n_in0, n_out, n_short, n_fc, n_bn, n_bias, b_mid, b_in, b_in0, b_out, b_short, b_fc,
         m_mid, m_in, m_out, m_small) = unpack_weights(gathered, v_next)
        m_bn = m_small[24:28].reshape(-1)
        m_bn = jnp.where(odd, m_bn[64:], m_bn[:448])
        m_bias = lax.dynamic_slice(m_small, (28, 4 * rank), (1, 4))[0]
        return (n_in0.T, n_short, jnp.swapaxes(n_in, 1, 2), n_mid.reshape(w_mid.shape), n_out, n_fc.T,
                n_bn.reshape(-1), n_bias[0, :CLASSES],
                b_in0.T, b_short, jnp.swapaxes(b_in, 1, 2), b_mid.reshape(w_mid.shape), b_out, b_fc.T,
                m_small[0:2].reshape(-1), m_small[8:16].reshape(-1), m_in, m_mid, m_out,
                m_small[16:24, :CLASSES].reshape(-1), m_bn, m_bias)

    return jax.shard_map(body, mesh=mesh, in_specs=in_specs, out_specs=out_specs, check_vma=False)
```

```python
import jax
import jax.numpy as jnp
from jax import lax
from jax.experimental import pallas as pl
from jax.experimental.pallas import tpu as pltpu
from jax.sharding import PartitionSpec as P

MOMENTUM = 0.9
TRUST_COEF = 0.001
DECAY = 0.0001
N_DEV = 32
LANES = 128
MID, IN0, IN, OUT, SHORT, FC, BN, BIAS, ROWS = 0, 162, 164, 232, 304, 312, 320, 324, 328
N_MID, N_IN, N_OUT = 18, 17, 18
CLASSES = 100
ID_IN0, ID_IN, ID_OUT, ID_SHORT, ID_FC, ID_PLAIN = 18, 19, 36, 54, 55, 56
F32 = jnp.float32
VMEM = pltpu.VMEM
MESH = pl.DeviceIdType.MESH
CHUNKS = ((0, 72, 'x'), (72, 72, 'y'), (144, 48, 'x'), (192, 48, 'y'), (240, 48, 'x'), (288, 40, 'y'))
STEPS = (
    (0, 0), (1, 0), (0, 1), (4, 0), (2, 0), (3, 0), (4, 1), (1, 1), (0, 2), (3, 1), (1, 2), (0, 3), (2, 1), (4, 2),
    (5, 0), (1, 3), (5, 1), (3, 2), (4, 3), (2, 2), (3, 3), (1, 4), (5, 2), (2, 3), (0, 4), (4, 4), (5, 3), (1, 5),
    (3, 4), (0, 5), (2, 4), (5, 4), (3, 5), (1, 6), (5, 5), (0, 6), (2, 5), (1, 7), (3, 6), (0, 7), (4, 5), (2, 6),
    (4, 6), (1, 8), (5, 6), (3, 7), (2, 7), (4, 7), (5, 7), (2, 8), (1, 9), (0, 8), (2, 9), (3, 8), (5, 8), (0, 9),
    (3, 9), (4, 8), (5, 9), (4, 9),
)
S_CORE, S_ONE, S_TWO, S_Z, A_Z, A_TWO, A_ONE, A_CORE, N_SEMS = 0, 1, 2, 2, 5, 9, 10, 11, 12
VMEM_LIMIT = 60 * 2**20


def first_row(t):
    out = jnp.where(t < N_MID, 9 * t, IN0)
    out = jnp.where(t >= ID_IN, IN + 4 * (t - ID_IN), out)
    out = jnp.where(t >= ID_OUT, OUT + 4 * (t - ID_OUT), out)
    return jnp.where(t >= ID_SHORT, SHORT + 8 * (t - ID_SHORT), out)


def left(a, b):
    return jnp.concatenate([a[:, :64], b[:, :64]], axis=1)


def right(a, b):
    return jnp.concatenate([a[:, 64:], b[:, 64:]], axis=1)


def across(piece8, row):
    return pl.ds(piece8 * 8 * ROWS + row, 8, stride=ROWS)


def exchange_kernel(lr, g_mid, g_in, g_in0, g_out, g_short, g_bn, pooled, dlog_t,
                    w_mid, w_in, w_in0, w_out, w_short, w_fc, w_bn, w_bias,
                    v_mid, v_in, v_in0, v_out, v_short, v_fc, v_bn, v_bias,
                    full_out, v_out_rows,
                    s_mid, s_in, s_in0, s_out, s_short, s_bn, s_x, s_d, xt, fct,
                    o_mid, o_in, o_in0, o_out, o_short, o_fc, o_bn, o_bias, ot,
                    p_mid, p_in, p_in0, p_out, p_short, p_fc, p_bn, p_bias,
                    packed, w_own, v_own, v_new, full,
                    got_core, acc, got_one, got_two, got_z, grad, norms,
                    sems, out_sems, send, recv, n_send, n_recv):
    rank = lax.axis_index('dp')
    core = lax.rem(rank, 2)
    x = lax.rem(rank // 2, 2)
    y = lax.rem(rank // 4, 2)
    z = rank // 8

    def device(zz, yy, xx, cc):
        return (((zz * 2 + yy) * 2 + xx) * 2 + cc,)

    core_peer = device(z, y, x, 1 - core)
    x_peer = device(z, y, 1 - x, core)
    y_peer = device(z, 1 - y, x, core)

    barrier = pltpu.get_barrier_semaphore()

    def greet(d, carry):
        pl.semaphore_signal(barrier, inc=1, device_id=(lax.rem(rank + d, N_DEV),), device_id_type=MESH)
        return carry

    lax.fori_loop(1, N_DEV, greet, 0)

    waiting = {}
    count = [0]

    def fetch(name, src, dst):
        copy = pltpu.make_async_copy(src, dst, sems.at[count[0]])
        count[0] += 1
        copy.start()
        waiting.setdefault(name, []).append(copy)

    def need(*names):
        for name in names:
            for copy in waiting.pop(name, []):
                copy.wait()

    def halves(name, src, dst):
        for h in range(2):
            fetch(name, src(pl.ds(128 * h, 128)), dst.at[h])

    fetchers = {
        'mid0': lambda: fetch('mid0', g_mid.at[pl.ds(0, 8)], s_mid.at[pl.ds(0, 8)]),
        'mid1': lambda: fetch('mid1', g_mid.at[pl.ds(8, 8)], s_mid.at[pl.ds(8, 8)]),
        'mid2': lambda: fetch('mid2', g_mid.at[pl.ds(16, 2)], s_mid.at[pl.ds(16, 2)]),
        'in': lambda: fetch('in', g_in, s_in),
        'in0': lambda: fetch('in0', g_in0, s_in0),
        'out': lambda: halves('out', lambda c: g_out.at[:, :, c], s_out),
        'short': lambda: halves('short', lambda c: g_short.at[:, c], s_short),
        'fc': lambda: (fetch('fc', pooled, s_x), fetch('fc', dlog_t, s_d)),
        'bn': lambda: fetch('bn', g_bn, s_bn),
    }
    units = [(0, 72, ('mid0',)), (72, 144, ('mid1',)), (144, 168, ('mid2', 'in0', 'in'))]
    units += [(168 + 8 * j, 176 + 8 * j, ('in',)) for j in range(8)]
    units += [(232 + 8 * j, 240 + 8 * j, ('out',)) for j in range(9)]
    units += [(304, 312, ('short',)), (312, 320, ('fc',)), (320, 328, ('bn', 'fc'))]
    for at, size, _ in CHUNKS:
        for lo, hi, names in units:
            if at <= lo < at + size:
                for name in names:
                    if name in fetchers:
                        fetchers.pop(name)()

    mid_at = pl.multiple_of((18 * rank) // 8 * 8, 8)
    mid_off = lax.rem(18 * rank, 8)
    out_at = pl.multiple_of((2 * rank) // 8 * 8, 8)
    out_off = 2 * lax.rem(rank, 4)
    short_at = pl.multiple_of((4 * rank) // 8 * 8, 8)
    short_off = 4 * lax.rem(rank, 2)
    col_at = pl.multiple_of((rank // 16) * 128, 128)
    col_off = pl.multiple_of(lax.rem(rank, 16) * 8, 8)
    fetch('own', w_mid.at[:, pl.ds(mid_at, 24), :], o_mid)
    fetch('own', w_in.at[:, :, pl.ds(col_at, 128)], o_in)
    fetch('own', w_in0, o_in0)
    halves('own', lambda c: w_out.at[:, pl.ds(out_at, 8), c], o_out)
    halves('own', lambda c: w_short.at[pl.ds(short_at, 8), c], o_short)
    fetch('own', w_fc.at[:, pl.ds(col_at, 128)], o_fc)
    fetch('own', w_bn, o_bn)
    fetch('own', w_bias, o_bias)
    for src, dst in ((v_mid, p_mid), (v_in, p_in), (v_in0, p_in0), (v_out, p_out), (v_short, p_short), (v_fc, p_fc),
                     (v_bn, p_bn), (v_bias, p_bias)):
        fetch('own', src, dst)

    pieces = packed.reshape(N_DEV * ROWS, LANES)

    def pack_mid(first, last):
        def body(t, carry):
            for a in range(4):
                for k in range(9):
                    even = s_mid[t, pl.ds(144 * a + 2 * k, 8, stride=18), :]
                    odd = s_mid[t, pl.ds(144 * a + 2 * k + 1, 8, stride=18), :]
                    pieces[across(a, MID + 9 * t + k), :] = jnp.concatenate([even, odd], axis=1)
            return carry

        lax.fori_loop(first, last, body, 0)

    def pack_in_rows(t, pair):
        for a in range(4):
            for k in range(4):
                even = xt[pl.ds(64 * a + 2 * k, 8, stride=8), :]
                odd = xt[pl.ds(64 * a + 2 * k + 1, 8, stride=8), :]
                pieces[across(a, IN + 4 * t + k), :] = left(even, odd)
                if pair:
                    pieces[across(a, IN + 4 * t + 4 + k), :] = right(even, odd)

    def pack_in(first, last):
        def body(j, carry):
            t = 2 * j + 1
            both = jnp.concatenate([s_in[t], s_in[t + 1]], axis=0)
            for h in range(2):
                xt[128 * h:128 * h + 128, :] = both[:, 128 * h:128 * h + 128].T
            pack_in_rows(t, True)
            return carry

        lax.fori_loop(first, last, body, 0)

    def pack_in_first():
        both = jnp.concatenate([s_in[0], jnp.concatenate([s_in0[...], s_in0[...]], axis=1)], axis=0)
        for h in range(2):
            xt[128 * h:128 * h + 128, :] = both[:, 128 * h:128 * h + 128].T
        pack_in_rows(0, False)
        for a in range(4):
            for k in range(2):
                even = xt[pl.ds(32 * a + 2 * k, 8, stride=4), :]
                odd = xt[pl.ds(32 * a + 2 * k + 1, 8, stride=4), :]
                pieces[across(a, IN0 + k), :] = right(even, odd)

    def pack_out(first, last):
        def body(t, carry):
            for a in range(4):
                for p in range(2):
                    for h in range(2):
                        pieces[across(a, OUT + 4 * t + 2 * p + h), :] = s_out[h, t, pl.ds(16 * a + p, 8, stride=2), :]
            return carry

        lax.fori_loop(first, last, body, 0)

    def pack_short():
        for a in range(4):
            for p in range(4):
                for h in range(2):
                    pieces[across(a, SHORT + 2 * p + h), :] = s_short[h, pl.ds(32 * a + p, 8, stride=4), :]

    scale = 1.0 / pooled.shape[0]

    def pack_fc():
        fct[CLASSES:LANES, :] = jnp.zeros((LANES - CLASSES, 256), F32)
        fct[0:CLASSES, :] = jnp.dot(s_d[...], s_x[...], preferred_element_type=F32) * scale
        for h in range(2):
            cols = fct[:, 128 * h:128 * h + 128].T
            for j in range(16):
                at = (16 * h + j) * ROWS + FC
                pieces[at:at + 8, :] = cols[8 * j:8 * j + 8, :]

    def pack_bn():
        for i in range(N_DEV):
            pieces[i * ROWS + BN:i * ROWS + ROWS, :] = jnp.zeros((8, LANES), F32)
        for b in range(2):
            for k in range(4):
                for half in range(2):
                    pieces[pl.ds((16 * b + half) * ROWS + BN + k, 8, stride=2 * ROWS), :] = (
                        s_bn[pl.ds(56 * b + 3 * half + k, 8, stride=7), :])
        bias = lax.dot_general(jnp.ones((8, s_d.shape[1]), jnp.bfloat16), s_d[...], (((1,), (1,)), ((), ())),
                               preferred_element_type=F32) * scale
        bias = jnp.concatenate([bias, jnp.zeros((8, LANES - CLASSES), F32)], axis=1)
        for a in range(4):
            pieces[across(a, BIAS), :] = bias

    def pack(at, size):
        end = at + size
        for lo, hi, names in units:
            if at <= lo < end:
                need(*names)
        for lo, first, last in ((0, 0, 8), (72, 8, 16), (144, 16, 18)):
            if at <= lo < end:
                pack_mid(first, last)
        if at <= 144 < end:
            pack_in_first()
        lo, hi = max(at, 168), min(end, 232)
        if lo < hi:
            pack_in((lo - 168) // 8, (hi - 168) // 8)
        lo, hi = max(at, OUT), min(end, SHORT)
        if lo < hi:
            pack_out((lo - OUT) // 4, (hi - OUT) // 4)
        if at <= SHORT < end:
            pack_short()
        if at <= FC < end:
            pack_fc()
        if at <= BN < end:
            pack_bn()

    lane_row = lax.broadcasted_iota(jnp.int32, (1, LANES), 1)

    def own_pieces():
        need('own')
        for ref, base, tiles, tensors in ((p_mid, MID, 9, N_MID), (p_in, IN, 4, N_IN), (p_out, OUT, 4, N_OUT)):
            for m in range(tiles):
                for t in range(0, tensors, 8):
                    size = min(8, tensors - t)
                    v_own[pl.ds(base + tiles * t + m, size, stride=tiles), :] = (
                        ref[t:t + size, 128 * m:128 * m + 128])
        v_own[IN0:IN0 + 2, :] = p_in0[...]
        v_own[SHORT:SHORT + 8, :] = p_short[...]
        flat = [p_fc[pl.ds(128 * q, 128)].reshape(1, LANES) for q in range(6)]
        flat.append(jnp.concatenate([p_fc[pl.ds(768, 32)].reshape(1, 32), jnp.zeros((1, 96), F32)], axis=1))
        for r in range(8):
            q, s = divmod(CLASSES * r, LANES)
            row = pltpu.roll(flat[q], (LANES - s) % LANES, 1)
            if s + CLASSES > LANES:
                row = jnp.where(lane_row < LANES - s, row, pltpu.roll(flat[q + 1], LANES - s, 1))
            v_own[FC + r:FC + r + 1, :] = jnp.where(lane_row < CLASSES, row, 0.0)
        v_own[BN:ROWS, :] = jnp.zeros((8, LANES), F32)
        odd = lax.rem(rank, 2) == 1
        rows = [p_bn[pl.ds(128 * k, 128)].reshape(1, LANES) for k in range(3)]
        rows.append(jnp.concatenate([p_bn[pl.ds(384, 64)].reshape(1, 64), jnp.zeros((1, 64), F32)], axis=1))
        for k in range(4):
            before = pltpu.roll(rows[k - 1], 64, 1) if k else jnp.zeros((1, LANES), F32)
            moved = jnp.where(lane_row < 64, before, pltpu.roll(rows[k], 64, 1))
            v_own[BN + k:BN + k + 1, :] = jnp.where(odd, moved, rows[k])
        four = jnp.concatenate([p_bias[...].reshape(1, 4), jnp.zeros((1, LANES - 4), F32)], axis=1)
        v_own[BIAS:BIAS + 1, :] = pltpu.roll(four, 4 * rank, 1)

        for t in range(N_MID):
            even = o_mid[t, pl.ds(mid_off, 9, stride=2), :]
            odds = o_mid[t, pl.ds(mid_off + 1, 9, stride=2), :]
            w_own[MID + 9 * t:MID + 9 * t + 9, :] = jnp.concatenate([even, odds], axis=1)
        for j in range(9):
            other = o_in[2 * j - 1] if j else o_in0[...]
            ot[...] = jnp.concatenate([other, o_in[2 * j]], axis=0).T
            if j == 0:
                w_own[IN0:IN0 + 2, :] = left(ot[pl.ds(4 * rank, 2, stride=2), :], ot[pl.ds(4 * rank + 1, 2, stride=2), :])
            even = ot[pl.ds(col_off, 4, stride=2), :]
            odds = ot[pl.ds(col_off + 1, 4, stride=2), :]
            if j:
                w_own[IN + 8 * j - 4:IN + 8 * j, :] = left(even, odds)
            w_own[IN + 8 * j:IN + 8 * j + 4, :] = right(even, odds)
        for p in range(2):
            for h in range(2):
                for t in range(N_OUT):
                    at = OUT + 4 * t + 2 * p + h
                    w_own[at:at + 1, :] = o_out[h, t, pl.ds(out_off + p, 1), :]
        for p in range(4):
            for h in range(2):
                w_own[SHORT + 2 * p + h:SHORT + 2 * p + h + 1, :] = o_short[h, pl.ds(short_off + p, 1), :]
        ot[0:CLASSES, :] = o_fc[...]
        ot[CLASSES:LANES, :] = jnp.zeros((LANES - CLASSES, LANES), F32)
        ot[...] = ot[...].T
        w_own[FC:FC + 8, :] = ot[pl.ds(col_off, 8), :]
        w_own[BN:ROWS, :] = jnp.zeros((8, LANES), F32)
        bn_at = 7 * (rank // 2) + 3 * lax.rem(rank, 2)
        for k in range(4):
            w_own[BN + k:BN + k + 1, :] = o_bn[pl.ds(bn_at + k, 1), :]
        bias = jnp.concatenate([o_bias[...].reshape(1, CLASSES), jnp.zeros((1, LANES - CLASSES), F32)], axis=1)
        w_own[BIAS:BIAS + 1, :] = jnp.where((lane_row >= 4 * rank) & (lane_row < 4 * rank + 4), bias, 0.0)

    copies = {}
    outs = []

    def start(c, k, src, dst, peer):
        copy = pltpu.make_async_remote_copy(src_ref=src, dst_ref=dst, send_sem=send.at[c * N_SEMS + k],
                                            recv_sem=recv.at[c * N_SEMS + k], device_id=peer, device_id_type=MESH)
        copy.start()
        copies[c, k] = copy

    def arrived(c, k):
        copies[c, k].wait_recv()

    def keep(src, dst):
        copy = pltpu.make_async_copy(src, dst, out_sems.at[len(outs)])
        copy.start()
        outs.append(copy)

    def step(c, stage):
        at, size, first = CHUNKS[c]
        rows = pl.ds(at, size)
        x_first = first == 'x'
        one_peer, two_peer = (x_peer, y_peer) if x_first else (y_peer, x_peer)

        def half(zz, yx, mine):
            return (zz, yx, x if mine else 1 - x) if x_first else (zz, y if mine else 1 - y, yx)

        if stage == 0:
            pack(at, size)
            if not copies:
                pl.semaphore_wait(barrier, N_DEV - 1)
            start(c, S_CORE, packed.at[:, :, :, 1 - core, rows, :], got_core.at[:, :, :, rows, :], core_peer)
        elif stage == 1:
            arrived(c, S_CORE)

            def add(mine):
                def body(m, carry):
                    zz, yx = m // 2, lax.rem(m, 2)
                    a, b, d = half(zz, yx, mine)
                    acc[a, b, d, rows, :] = packed[a, b, d, core, rows, :] + got_core[a, b, d, rows, :]
                    return carry

                lax.fori_loop(0, 8, body, 0)

            add(False)
            src = acc.at[:, :, 1 - x, rows, :] if x_first else acc.at[:, 1 - y, :, rows, :]
            start(c, S_ONE, src, got_one.at[:, :, rows, :], one_peer)
            add(True)
        elif stage == 2:
            arrived(c, S_ONE)

            def add(other):
                def body(zz, carry):
                    a, b, d = half(zz, other, True)
                    acc[a, b, d, rows, :] = acc[a, b, d, rows, :] + got_one[zz, other, rows, :]
                    return carry

                lax.fori_loop(0, 4, body, 0)

            here = y if x_first else x
            add(1 - here)
            src = acc.at[:, 1 - y, x, rows, :] if x_first else acc.at[:, y, 1 - x, rows, :]
            start(c, S_TWO, src, got_two.at[:, rows, :], two_peer)
            add(here)
        elif stage == 3:
            arrived(c, S_TWO)
            for d in (1, 2, 3, 0):
                zz = lax.rem(z + d, 4)
                acc[zz, y, x, rows, :] = acc[zz, y, x, rows, :] + got_two[zz, rows, :]
                if d:
                    start(c, S_Z + d, acc.at[zz, y, x, rows, :], got_z.at[d - 1, rows, :], device(zz, y, x, core))
        elif stage == 4:
            for d in (1, 2, 3):
                arrived(c, S_Z + d)
            mean = (acc[z, y, x, rows, :] + got_z[0, rows, :] + got_z[1, rows, :] + got_z[2, rows, :]) * (1.0 / N_DEV)
            grad[rows, :] = mean
            own = w_own[rows, :]
            g_sum = jnp.sum(mean * mean, axis=1, keepdims=True)
            w_sum = jnp.sum(own * own, axis=1, keepdims=True)
            row = lax.broadcasted_iota(jnp.int32, (size, LANES), 0) + at
            lane = lax.broadcasted_iota(jnp.int32, (size, LANES), 1)
            tensor = jnp.where(lane < 64, lane, lane - 64)
            member = (row >= first_row(tensor)) & (row < first_row(tensor + 1))
            part = jnp.where(member, jnp.where(lane < 64, g_sum, w_sum), 0.0)
            norms[c, rank] = jnp.sum(part, axis=0, keepdims=True)

            def tell(d, carry):
                pltpu.make_async_remote_copy(
                    src_ref=norms.at[c, rank], dst_ref=norms.at[c, rank], send_sem=n_send.at[c],
                    recv_sem=n_recv.at[c], device_id=(lax.rem(rank + d, N_DEV),), device_id_type=MESH).start()
                return carry

            lax.fori_loop(1, N_DEV, tell, 0)
        elif stage == 5:
            others = norms.at[c, pl.ds(0, N_DEV - 1)]
            pltpu.make_async_copy(others, others, n_recv.at[c]).wait()
            total = jnp.sum(norms[c], axis=0)
            g_norm = jnp.sqrt(total)
            w_norm = pltpu.roll(g_norm, 64, 1)
            trust = jnp.where((w_norm > 0) & (g_norm > 0), TRUST_COEF * w_norm / (g_norm + DECAY * w_norm), 1.0)
            row = lax.broadcasted_iota(jnp.int32, (size, LANES), 0) + at
            lane = lax.broadcasted_iota(jnp.int32, (size, LANES), 1)
            trust = jnp.where(lane == ID_PLAIN, 1.0, trust)
            member = (row >= first_row(lane)) & (row < first_row(lane + 1)) & (lane <= ID_PLAIN)
            rate = lr[0] * jnp.sum(jnp.where(member, trust, 0.0), axis=1, keepdims=True)
            decay = jnp.where(row < BN, DECAY, 0.0)
            own = w_own[rows, :]
            moment = MOMENTUM * v_own[rows, :] + rate * (grad[rows, :] + decay * own)
            v_new[rows, :] = moment
            keep(v_new.at[rows, :], v_out_rows.at[rows, :])
            mine = (row != BIAS) | ((lane >= 4 * rank) & (lane < 4 * rank + 4))
            full[z, y, x, core, rows, :] = jnp.where(mine, own - moment, 0.0)
            for d in (1, 2, 3):
                piece = full.at[z, y, x, core, rows, :]
                start(c, A_Z + d, piece, piece, device(lax.rem(z + d, 4), y, x, core))
        elif stage == 6:
            for d in (1, 2, 3):
                arrived(c, A_Z + d)
            pieces = full.at[:, y, x, core, rows, :]
            start(c, A_TWO, pieces, pieces, two_peer)
        elif stage == 7:
            arrived(c, A_TWO)
            pieces = full.at[:, :, x, core, rows, :] if x_first else full.at[:, y, :, core, rows, :]
            start(c, A_ONE, pieces, pieces, one_peer)
        elif stage == 8:
            arrived(c, A_ONE)
            pieces = full.at[:, :, :, core, rows, :]
            start(c, A_CORE, pieces, pieces, core_peer)
        else:
            arrived(c, A_CORE)
            keep(full.at[:, :, :, :, rows, :], full_out.at[:, :, :, :, rows, :])

    for c, stage in STEPS:
        if stage == 3 and not any(k[1] == S_Z + 1 for k in copies):
            own_pieces()
        step(c, stage)
    for copy in copies.values():
        copy.wait_send()
    for c in range(len(CHUNKS)):
        others = norms.at[c, pl.ds(0, N_DEV - 1)]
        pltpu.make_async_copy(others, others, n_send.at[c]).wait()
    for copy in outs:
        copy.wait()


def exchange(operands):
    any_ = pl.BlockSpec(memory_space=pl.ANY)
    count = len(CHUNKS)
    bf = jnp.bfloat16
    shapes = [(N_MID, 576, 64), (N_IN, 64, 256), (64, 128), (2, N_OUT, 64, 128), (2, 128, 128), (112, 128)]
    own = [(N_MID, 24, 64), (N_IN, 64, 128), (64, 128), (2, N_OUT, 8, 128), (2, 8, 128), (CLASSES, 128), (112, 128),
           (CLASSES,), (128, 128), (N_MID, 1152), (N_IN, 512), (2, LANES), (N_OUT, 512), (8, LANES), (800,), (448,), (4,)]
    rows = (ROWS, LANES)
    exchanged = [(4, 2, 2) + rows, (4, 2, 2) + rows, (4, 2) + rows, (4,) + rows, (3,) + rows, rows,
                 (count, N_DEV, 1, LANES)]
    dma = pltpu.SemaphoreType.DMA
    full, v_new = pl.pallas_call(
        exchange_kernel,
        out_shape=(jax.ShapeDtypeStruct((4, 2, 2, 2) + rows, F32), jax.ShapeDtypeStruct(rows, F32)),
        in_specs=[pl.BlockSpec(memory_space=pltpu.SMEM)] + [any_] * 24,
        out_specs=(any_, any_),
        scratch_shapes=[VMEM(s, F32) for s in shapes]
        + [VMEM((1024, 256), bf), VMEM((CLASSES, 1024), bf), VMEM((256, 128), F32), VMEM((128, 256), F32)]
        + [VMEM(s, F32) for s in own]
        + [VMEM((4, 2, 2, 2) + rows, F32), VMEM(rows, F32), VMEM(rows, F32), VMEM(rows, F32),
           VMEM((4, 2, 2, 2) + rows, F32)]
        + [VMEM(s, F32) for s in exchanged]
        + [dma((32,)), dma((2 * count,)), dma((count * N_SEMS,)), dma((count * N_SEMS,)), dma((count,)), dma((count,))],
        compiler_params=pltpu.CompilerParams(vmem_limit_bytes=VMEM_LIMIT, collective_id=0, has_side_effects=True),
    )(*operands)
    return full.reshape(N_DEV, ROWS, LANES), v_new


def unpack_kernel(packed_rows, v_rows, n_mid, n_in, n_in0, n_out, n_short, n_fc, n_bn, n_bias,
                  b_mid, b_in, b_in0, b_out, b_short, b_fc, v_mid, v_in, v_in0, v_out, v_short, v_fc, v_bn, v_bias,
                  packed, v_own, s_mid, s_in, s_out, s_short, s_in0, s_fc, t_mid, t_in, t_out, t_short, t_in0, t_fc, xt, sems):
    bf = jnp.bfloat16
    lane_row = lax.broadcasted_iota(jnp.int32, (1, LANES), 1)
    pieces = packed.reshape(N_DEV, ROWS, LANES)
    fetches = []
    for k, (at, size) in enumerate(((0, 40), (40, 104), (144, 24), (168, 64), (232, 72), (304, 24))):
        fetches.append(pltpu.make_async_copy(packed_rows.at[:, pl.ds(at, size), :], pieces.at[:, pl.ds(at, size), :],
                                             sems.at[12 + k]))
    fetches.append(pltpu.make_async_copy(v_rows, v_own, sems.at[18]))
    for copy in fetches:
        copy.start()

    def put(src, dst, k):
        pltpu.make_async_copy(src, dst, sems.at[k]).start()

    def mid_body(t, carry):
        for a in range(4):
            for k in range(9):
                x = packed[across(a, MID + 9 * t + k), :]
                s_mid[t, pl.ds(144 * a + 2 * k, 8, stride=18), :] = x[:, :64]
                s_mid[t, pl.ds(144 * a + 2 * k + 1, 8, stride=18), :] = x[:, 64:]
        put(s_mid.at[t], n_mid.at[t], 0)
        t_mid[t] = s_mid[t].astype(bf)
        put(t_mid.at[t], b_mid.at[t], 1)
        return carry

    fetches[0].wait()
    lax.fori_loop(0, 4, mid_body, 0)
    fetches[1].wait()
    lax.fori_loop(4, 15, mid_body, 0)
    fetches[2].wait()
    lax.fori_loop(15, N_MID, mid_body, 0)
    fetches[3].wait()

    def in_rows(t, other):
        for a in range(4):
            for k in range(4):
                x = packed[across(a, IN + 4 * t + k), :]
                y = packed[across(a, IN + 4 * other + k), :]
                xt[pl.ds(64 * a + 2 * k, 8, stride=8), :] = left(x, y)
                xt[pl.ds(64 * a + 2 * k + 1, 8, stride=8), :] = right(x, y)

    def in_body(j, carry):
        t = 2 * j + 1
        in_rows(t, t + 1)
        for h in range(2):
            cols = xt[128 * h:128 * h + 128, :].T
            for u in range(2):
                s_in[t + u, :, 128 * h:128 * h + 128] = cols[64 * u:64 * u + 64]
                t_in[t + u, :, 128 * h:128 * h + 128] = cols[64 * u:64 * u + 64].astype(bf)
        for u in range(2):
            put(s_in.at[t + u], n_in.at[t + u], 2)
            put(t_in.at[t + u], b_in.at[t + u], 3)
        return carry

    lax.fori_loop(0, 8, in_body, 0)
    in_rows(0, 0)
    for h in range(2):
        cols = xt[128 * h:128 * h + 128, :].T
        s_in[0, :, 128 * h:128 * h + 128] = cols[:64]
        t_in[0, :, 128 * h:128 * h + 128] = cols[:64].astype(bf)
    put(s_in.at[0], n_in.at[0], 2)
    put(t_in.at[0], b_in.at[0], 3)
    for a in range(4):
        for k in range(2):
            x = packed[across(a, IN0 + k), :]
            xt[pl.ds(32 * a + 2 * k, 8, stride=4), :] = x
            xt[pl.ds(32 * a + 2 * k + 1, 8, stride=4), :] = right(x, x)
    cols = xt[0:128, :].T
    s_in0[...] = cols[:64]
    t_in0[...] = cols[:64].astype(bf)
    put(s_in0, n_in0, 4)
    put(t_in0, b_in0, 5)

    def out_body(t, carry):
        for a in range(4):
            for p in range(2):
                for h in range(2):
                    s_out[h, t, pl.ds(16 * a + p, 8, stride=2), :] = packed[across(a, OUT + 4 * t + 2 * p + h), :]
        for h in range(2):
            t_out[h, t] = s_out[h, t].astype(bf)
            put(s_out.at[h, t], n_out.at[t, :, pl.ds(128 * h, 128)], 6)
            put(t_out.at[h, t], b_out.at[t, :, pl.ds(128 * h, 128)], 7)
        return carry

    fetches[4].wait()
    lax.fori_loop(0, N_OUT, out_body, 0)
    fetches[5].wait()
    for h in range(2):
        for a in range(4):
            for p in range(4):
                s_short[h, pl.ds(32 * a + p, 8, stride=4), :] = packed[across(a, SHORT + 2 * p + h), :]
        t_short[h] = s_short[h].astype(bf)
        put(s_short.at[h], n_short.at[:, pl.ds(128 * h, 128)], 8)
        put(t_short.at[h], b_short.at[:, pl.ds(128 * h, 128)], 9)
    for i in range(N_DEV):
        xt[8 * i:8 * i + 8, :] = packed[i * ROWS + FC:i * ROWS + FC + 8, :]
    for h in range(2):
        cols = xt[128 * h:128 * h + 128, :].T
        s_fc[:, 128 * h:128 * h + 128] = cols[:CLASSES]
        t_fc[:, 128 * h:128 * h + 128] = cols[:CLASSES].astype(bf)
    put(s_fc, n_fc, 10)
    put(t_fc, b_fc, 11)

    lane = lax.broadcasted_iota(jnp.int32, (8, LANES), 1)
    for b in range(2):
        def even(k):
            return packed[pl.ds(16 * b * ROWS + BN + k, 8, stride=2 * ROWS), :]

        def odd(k):
            return packed[pl.ds((16 * b + 1) * ROWS + BN + k, 8, stride=2 * ROWS), :]

        for k in range(3):
            n_bn[pl.ds(56 * b + k, 8, stride=7), :] = even(k)
            n_bn[pl.ds(56 * b + 4 + k, 8, stride=7), :] = odd(1 + k)
        n_bn[pl.ds(56 * b + 3, 8, stride=7), :] = jnp.where(lane < 64, even(3), odd(0))
    total = packed[across(0, BIAS), :]
    for a in range(1, 4):
        total = total + packed[across(a, BIAS), :]
    n_bias[...] = jnp.sum(total, axis=0, keepdims=True)[0, :CLASSES]
    fetches[6].wait()

    for ref, base, tiles, count in ((v_mid, MID, 9, N_MID), (v_in, IN, 4, N_IN), (v_out, OUT, 4, N_OUT)):
        for m in range(tiles):
            for t in range(0, count, 8):
                size = min(8, count - t)
                ref[t:t + size, 128 * m:128 * m + 128] = v_own[pl.ds(base + tiles * t + m, size, stride=tiles), :]
    rank = lax.axis_index('dp')
    v_in0[...] = v_own[IN0:IN0 + 2, :]
    v_short[...] = v_own[SHORT:SHORT + 8, :]
    for q in range(7):
        flat = jnp.zeros((1, LANES), F32)
        for r in range(8):
            d = CLASSES * r - LANES * q
            if -CLASSES < d < LANES:
                row = pltpu.roll(v_own[FC + r:FC + r + 1, :], d % LANES, 1)
                flat = jnp.where((lane_row >= d) & (lane_row < d + CLASSES), row, flat)
        size = min(LANES, 800 - LANES * q)
        v_fc[pl.ds(LANES * q, size)] = flat[0, :size]
    odd = lax.rem(rank, 2) == 1
    for k in range(4):
        here = v_own[BN + k:BN + k + 1, :]
        after = v_own[BN + k + 1:BN + k + 2, :]
        moved = jnp.where(lane_row < 64, pltpu.roll(here, 64, 1), pltpu.roll(after, 64, 1))
        size = min(LANES, 448 - LANES * k)
        v_bn[pl.ds(LANES * k, size)] = jnp.where(odd, moved, here)[0, :size]
    v_bias[...] = pltpu.roll(v_own[BIAS:BIAS + 1, :], lax.rem(N_DEV - rank, N_DEV) * 4, 1)[0, :4]

    for k, (src, dst) in enumerate(((s_mid, n_mid), (t_mid, b_mid), (s_in, n_in), (t_in, b_in), (s_in0, n_in0),
                                    (t_in0, b_in0))):
        pltpu.make_async_copy(src, dst, sems.at[k]).wait()
    for h in range(2):
        half = pl.ds(128 * h, 128)
        for k, (src, dst) in enumerate(((s_out, n_out.at[:, :, half]), (t_out, b_out.at[:, :, half]),
                                        (s_short, n_short.at[:, half]), (t_short, b_short.at[:, half]))):
            pltpu.make_async_copy(src.at[h], dst, sems.at[6 + k]).wait()
    pltpu.make_async_copy(s_fc, n_fc, sems.at[10]).wait()
    pltpu.make_async_copy(t_fc, b_fc, sems.at[11]).wait()


def unpack_weights(packed, v_own):
    any_ = pl.BlockSpec(memory_space=pl.ANY)
    vm = pl.BlockSpec(memory_space=VMEM)
    bf = jnp.bfloat16
    kernels = ((N_MID, 576, 64), (N_IN, 64, 256), (64, 128), (N_OUT, 64, 256), (128, 256), (CLASSES, 256))
    shapes = [(s, F32) for s in kernels] + [((112, 128), F32), ((CLASSES,), F32)] + [(s, bf) for s in kernels]
    shapes += [(s, F32) for s in ((N_MID, 1152), (N_IN, 512), (2, LANES), (N_OUT, 512), (8, LANES), (800,), (448,), (4,))]
    scratch = ((N_MID, 576, 64), (N_IN, 64, 256), (2, N_OUT, 64, 128), (2, 128, 128), (64, 128), (CLASSES, 256))
    return pl.pallas_call(
        unpack_kernel,
        out_shape=[jax.ShapeDtypeStruct(s, d) for s, d in shapes],
        in_specs=[any_, any_],
        out_specs=[any_] * 6 + [vm] * 2 + [any_] * 6 + [vm] * 8,
        scratch_shapes=[VMEM((N_DEV * ROWS, LANES), F32), VMEM((ROWS, LANES), F32)] + [VMEM(s, F32) for s in scratch] + [VMEM(s, bf) for s in scratch]
        + [VMEM((256, 128), F32), pltpu.SemaphoreType.DMA((19,))],
        compiler_params=pltpu.CompilerParams(vmem_limit_bytes=VMEM_LIMIT),
    )(packed, v_own)


def solution(mesh):
    spec_full = P()
    spec_lead = P('dp')
    spec_cols = P(None, 'dp')
    moment_specs = (spec_lead, spec_lead, spec_cols, spec_cols, spec_cols, spec_lead, spec_lead, spec_lead)
    in_specs = (spec_full,) * 8 + (spec_lead,) * 8 + moment_specs + (spec_full,)
    out_specs = (spec_full,) * 14 + moment_specs

    def body(w_in0, w_short, w_in, w_mid, w_out, w_fc, w_bn, w_bias,
             g_in0, g_short, g_in, g_mid, g_out, g_bn, pooled, dlogits,
             v_in0, v_short, v_in, v_mid, v_out, v_fc, v_bn, v_bias, learn_rate):
        gathered, v_next = exchange((
            learn_rate.reshape(1), g_mid.reshape(N_MID, 576, 64), jnp.swapaxes(g_in[0], 1, 2), g_in0[0].T, g_out[0],
            g_short[0], g_bn.reshape(112, LANES), pooled, dlogits.T,
            w_mid.reshape(N_MID, 576, 64), jnp.swapaxes(w_in, 1, 2), w_in0.T, w_out, w_short, w_fc.T,
            w_bn.reshape(112, LANES), w_bias, v_mid, v_in, v_in0.reshape(2, LANES), v_out, v_short.reshape(8, LANES),
            v_fc, v_bn, v_bias))
        (n_mid, n_in, n_in0, n_out, n_short, n_fc, n_bn, n_bias, b_mid, b_in, b_in0, b_out, b_short, b_fc,
         m_mid, m_in, m_in0, m_out, m_short, m_fc, m_bn, m_bias) = unpack_weights(gathered, v_next)
        return (n_in0.T, n_short, jnp.swapaxes(n_in, 1, 2), n_mid.reshape(w_mid.shape), n_out, n_fc.T,
                n_bn.reshape(-1), n_bias,
                b_in0.T, b_short, jnp.swapaxes(b_in, 1, 2), b_mid.reshape(w_mid.shape), b_out, b_fc.T,
                m_in0.reshape(-1), m_short.reshape(-1), m_in, m_mid, m_out, m_fc, m_bn, m_bias)

    return jax.shard_map(body, mesh=mesh, in_specs=in_specs, out_specs=out_specs, check_vma=False)
```

```python
import jax
import jax.numpy as jnp
from jax import lax
from jax.experimental import pallas as pl
from jax.experimental.pallas import tpu as pltpu
from jax.sharding import PartitionSpec as P

MOMENTUM = 0.9
TRUST_COEF = 0.001
DECAY = 0.0001
N_DEV = 32
LANES = 128
IN0, OUT, SHORT, FC, BN, BIAS, ROWS = 178, 232, 304, 312, 320, 324, 328
N_MID, N_IN, N_OUT = 18, 17, 18
CLASSES = 100
ID_IN0, ID_IN, ID_OUT, ID_SHORT, ID_FC, ID_PLAIN = 18, 19, 36, 54, 55, 56
F32 = jnp.float32
VMEM = pltpu.VMEM
MESH = pl.DeviceIdType.MESH
CHUNKS = (
    (0, 40, 'x'), (40, 40, 'y'), (80, 40, 'y'), (120, 40, 'x'), (160, 24, 'x'),
    (184, 24, 'y'), (208, 24, 'x'), (232, 24, 'y'), (256, 24, 'y'), (280, 24, 'x'),
    (304, 24, 'y'),
)
STEPS = (
    (10, 0), (9, 0), (8, 0), (10, 1), (9, 1), (4, 0), (6, 0), (8, 1), (4, 1), (7, 0), (2, 0), (10, 2), (9, 2), (7, 1),
    (6, 1), (5, 0), (8, 2), (3, 0), (4, 2), (2, 1), (9, 3), (7, 2), (3, 1), (10, 3), (0, 0), (8, 3), (6, 2), (1, 0),
    (4, 3), (2, 2), (5, 1), (7, 3), (9, 4), (10, 4), (3, 2), (6, 3), (8, 4), (5, 2), (1, 1), (2, 3), (4, 4), (0, 1),
    (7, 4), (3, 3), (5, 3), (6, 4), (9, 5), (1, 2), (0, 2), (10, 5), (2, 4), (8, 5), (3, 4), (1, 3), (5, 4), (9, 6),
    (0, 3), (10, 6), (7, 5), (4, 5), (8, 6), (6, 5), (10, 7), (1, 4), (3, 5), (8, 7), (9, 7), (0, 4), (7, 6), (10, 8),
    (5, 5), (2, 5), (4, 6), (6, 6), (7, 7), (3, 6), (1, 5), (5, 6), (0, 5), (4, 7), (8, 8), (2, 6), (10, 9), (6, 7),
    (5, 7), (1, 6), (3, 7), (0, 6), (7, 8), (2, 7), (4, 8), (9, 8), (7, 9), (1, 7), (5, 8), (8, 9), (0, 7), (6, 8),
    (6, 9), (2, 8), (3, 8), (1, 8), (0, 8), (3, 9), (2, 9), (1, 9), (5, 9), (9, 9), (4, 9), (0, 9),
)
S_CORE, S_ONE, S_TWO, S_Z, A_Z, A_TWO, A_ONE, A_CORE, N_SEMS = 0, 2, 4, 6, 7, 8, 10, 12, 14
VMEM_LIMIT = 60 * 2**20


def mid_row(t):
    return 40 * (t // 4) + 9 * (t % 4)


def in_row(t):
    return 36 + 40 * t if t < 4 else 164 + 4 * t


def member_rows(row, t):
    first = 9 * t
    for group in (4, 8, 12, 16):
        first = jnp.where(t >= group, first + 4, first)
    size = jnp.where(t < N_MID, 9, jnp.where(t == ID_IN0, 2, jnp.where(t < ID_SHORT, 4, 8)))
    first = jnp.where(t >= ID_IN0, IN0, first)
    first = jnp.where(t >= ID_IN, 36 + 40 * (t - ID_IN), first)
    first = jnp.where(t >= ID_IN + 4, 164 + 4 * (t - ID_IN), first)
    first = jnp.where(t >= ID_OUT, OUT + 4 * (t - ID_OUT), first)
    first = jnp.where(t >= ID_SHORT, SHORT + 8 * (t - ID_SHORT), first)
    return (row >= first) & (row < first + size)


def momentum_rows(mid, inn, out):
    runs = [(mid, mid_row(t), 9, t, min(4, N_MID - t)) for t in range(0, N_MID, 4)]
    runs += [(inn, 36, 40, 0, 4)] + [(inn, 164 + 4 * t, 4, t, min(8, N_IN - t)) for t in (4, 12)]
    runs += [(out, OUT + 4 * t, 4, t, min(8, N_OUT - t)) for t in (0, 8, 16)]
    for ref, base, stride, t, count in runs:
        for m in range(9 if ref is mid else 4):
            yield pl.ds(base + m, count, stride=stride), pl.ds(128 * m, 128), ref, pl.ds(t, count)


def left(a, b):
    return jnp.concatenate([a[:, :64], b[:, :64]], axis=1)


def right(a, b):
    return jnp.concatenate([a[:, 64:], b[:, 64:]], axis=1)


def across(piece8, row):
    return pl.ds(piece8 * 8 * ROWS + row, 8, stride=ROWS)


def exchange_kernel(lr, g_mid, g_in, g_in0, g_out, g_short, g_bn, pooled, dlog_t,
                    w_mid, w_in, w_in0, w_out, w_short, w_fc, w_bn, w_bias,
                    v_mid, v_in, v_in0, v_out, v_short, v_fc, v_bn, v_bias,
                    full_out, v_out_rows,
                    s_mid, s_in, s_in0, s_out, s_short, s_bn, s_x, s_d, xt, fct,
                    o_mid, o_in, o_in0, o_out, o_short, o_fc, o_bn, o_bias, ot,
                    p_mid, p_in, p_in0, p_out, p_short, p_fc, p_bn, p_bias,
                    packed, w_own, v_own, v_new, full,
                    got_core, acc, got_one, got_two, got_z, grad, norms,
                    sems, out_sems, send, recv, n_send, n_recv):
    rank = lax.axis_index('dp')
    core = lax.rem(rank, 2)
    x = lax.rem(rank // 2, 2)
    y = lax.rem(rank // 4, 2)
    z = rank // 8

    def device(zz, yy, xx, cc):
        return (((zz * 2 + yy) * 2 + xx) * 2 + cc,)

    core_peer = device(z, y, x, 1 - core)
    x_peer = device(z, y, 1 - x, core)
    y_peer = device(z, 1 - y, x, core)

    barrier = pltpu.get_barrier_semaphore()

    def greet(d, carry):
        pl.semaphore_signal(barrier, inc=1, device_id=(lax.rem(rank + d, N_DEV),), device_id_type=MESH)
        return carry

    lax.fori_loop(1, N_DEV, greet, 0)

    waiting = {}
    count = [0]

    def fetch(name, src, dst):
        copy = pltpu.make_async_copy(src, dst, sems.at[count[0]])
        count[0] += 1
        copy.start()
        waiting.setdefault(name, []).append(copy)

    def need(*names):
        for name in names:
            for copy in waiting.pop(name, []):
                copy.wait()

    def halves(name, src, dst):
        for h in range(2):
            fetch(name, src(pl.ds(128 * h, 128)), dst.at[h])

    fetchers = {
        'in': lambda: fetch('in', g_in.at[pl.ds(5, 12)], s_in.at[pl.ds(5, 12)]),
        'in1': lambda: fetch('in1', g_in.at[pl.ds(0, 5)], s_in.at[pl.ds(0, 5)]),
        'in0': lambda: fetch('in0', g_in0, s_in0),
        'out': lambda: halves('out', lambda c: g_out.at[:, :, c], s_out),
        'short': lambda: halves('short', lambda c: g_short.at[:, c], s_short),
        'fc': lambda: (fetch('fc', pooled, s_x), fetch('fc', dlog_t, s_d)),
        'bn': lambda: fetch('bn', g_bn, s_bn),
    }
    for i in range(5):
        part = pl.ds(4 * i, min(4, N_MID - 4 * i))
        fetchers['mid%d' % i] = lambda i=i, part=part: fetch('mid%d' % i, g_mid.at[part], s_mid.at[part])
    units = [(40 * i, 40 * i + 40, ('mid%d' % i, 'in1')) for i in range(4)] + [(160, 184, ('mid4', 'in0', 'in1'))]
    units += [(184 + 8 * j, 192 + 8 * j, ('in',)) for j in range(6)]
    units += [(232 + 8 * j, 240 + 8 * j, ('out',)) for j in range(9)]
    units += [(304, 312, ('short',)), (312, 320, ('fc',)), (320, 328, ('bn', 'fc'))]
    for at, size, _ in CHUNKS:
        for lo, hi, names in units:
            if at <= lo < at + size:
                for name in names:
                    if name in fetchers:
                        fetchers.pop(name)()

    mid_at = pl.multiple_of((18 * rank) // 8 * 8, 8)
    mid_off = lax.rem(18 * rank, 8)
    out_at = pl.multiple_of((2 * rank) // 8 * 8, 8)
    out_off = 2 * lax.rem(rank, 4)
    short_at = pl.multiple_of((4 * rank) // 8 * 8, 8)
    short_off = 4 * lax.rem(rank, 2)
    col_at = pl.multiple_of((rank // 16) * 128, 128)
    col_off = pl.multiple_of(lax.rem(rank, 16) * 8, 8)
    fetch('own', w_mid.at[:, pl.ds(mid_at, 24), :], o_mid)
    fetch('own', w_in.at[:, :, pl.ds(col_at, 128)], o_in)
    fetch('own', w_in0, o_in0)
    halves('own', lambda c: w_out.at[:, pl.ds(out_at, 8), c], o_out)
    halves('own', lambda c: w_short.at[pl.ds(short_at, 8), c], o_short)
    fetch('own', w_fc.at[:, pl.ds(col_at, 128)], o_fc)
    fetch('own', w_bn, o_bn)
    fetch('own', w_bias, o_bias)
    for src, dst in ((v_mid, p_mid), (v_in, p_in), (v_in0, p_in0), (v_out, p_out), (v_short, p_short), (v_fc, p_fc),
                     (v_bn, p_bn), (v_bias, p_bias)):
        fetch('own', src, dst)

    pieces = packed.reshape(N_DEV * ROWS, LANES)

    def pack_mid(base, first, count):
        def body(u, carry):
            t = first + u
            for a in range(4):
                for k in range(9):
                    even = s_mid[t, pl.ds(144 * a + 2 * k, 8, stride=18), :]
                    odd = s_mid[t, pl.ds(144 * a + 2 * k + 1, 8, stride=18), :]
                    pieces[across(a, base + 9 * u + k), :] = jnp.concatenate([even, odd], axis=1)
            return carry

        lax.fori_loop(0, count, body, 0)

    def pack_in_rows(base, pair):
        for a in range(4):
            for k in range(4):
                even = xt[pl.ds(64 * a + 2 * k, 8, stride=8), :]
                odd = xt[pl.ds(64 * a + 2 * k + 1, 8, stride=8), :]
                pieces[across(a, base + k), :] = left(even, odd)
                if pair:
                    pieces[across(a, base + 4 + k), :] = right(even, odd)

    def transpose(a, b):
        both = jnp.concatenate([a, b], axis=0)
        for h in range(2):
            xt[128 * h:128 * h + 128, :] = both[:, 128 * h:128 * h + 128].T

    def pack_in(first, last):
        def body(j, carry):
            transpose(s_in[2 * j + 5], s_in[2 * j + 6])
            pack_in_rows(184 + 8 * j, True)
            return carry

        lax.fori_loop(first, last, body, 0)

    def pack_in_one(t):
        wide = jnp.concatenate([s_in0[...], s_in0[...]], axis=1) if t == 4 else s_in[t]
        transpose(s_in[t], wide)
        pack_in_rows(in_row(t), False)
        if t == 4:
            for a in range(4):
                for k in range(2):
                    even = xt[pl.ds(32 * a + 2 * k, 8, stride=4), :]
                    odd = xt[pl.ds(32 * a + 2 * k + 1, 8, stride=4), :]
                    pieces[across(a, IN0 + k), :] = right(even, odd)

    def pack_out(first, last):
        def body(t, carry):
            for a in range(4):
                for p in range(2):
                    for h in range(2):
                        pieces[across(a, OUT + 4 * t + 2 * p + h), :] = s_out[h, t, pl.ds(16 * a + p, 8, stride=2), :]
            return carry

        lax.fori_loop(first, last, body, 0)

    def pack_short():
        for a in range(4):
            for p in range(4):
                for h in range(2):
                    pieces[across(a, SHORT + 2 * p + h), :] = s_short[h, pl.ds(32 * a + p, 8, stride=4), :]

    scale = 1.0 / pooled.shape[0]

    def pack_fc():
        fct[CLASSES:LANES, :] = jnp.zeros((LANES - CLASSES, 256), F32)
        fct[0:CLASSES, :] = jnp.dot(s_d[...], s_x[...], preferred_element_type=F32) * scale
        for h in range(2):
            cols = fct[:, 128 * h:128 * h + 128].T
            for j in range(16):
                at = (16 * h + j) * ROWS + FC
                pieces[at:at + 8, :] = cols[8 * j:8 * j + 8, :]

    def pack_bn():
        def clear(i, carry):
            pieces[pl.ds(pl.multiple_of(i * ROWS + BN, 8), 8), :] = jnp.zeros((8, LANES), F32)
            return carry

        lax.fori_loop(0, N_DEV, clear, 0)
        for b in range(2):
            for k in range(4):
                for half in range(2):
                    pieces[pl.ds((16 * b + half) * ROWS + BN + k, 8, stride=2 * ROWS), :] = (
                        s_bn[pl.ds(56 * b + 3 * half + k, 8, stride=7), :])
        bias = lax.dot_general(jnp.ones((8, s_d.shape[1]), jnp.bfloat16), s_d[...], (((1,), (1,)), ((), ())),
                               preferred_element_type=F32) * scale
        bias = jnp.concatenate([bias, jnp.zeros((8, LANES - CLASSES), F32)], axis=1)
        for a in range(4):
            pieces[across(a, BIAS), :] = bias

    def pack(at, size):
        end = at + size
        for lo, hi, names in units:
            if at <= lo < end:
                need(*names)
        for i in range(5):
            if at <= 40 * i < end:
                pack_mid(40 * i, 4 * i, min(4, N_MID - 4 * i))
                pack_in_one(i)
        lo, hi = max(at, 184), min(end, 232)
        if lo < hi:
            pack_in((lo - 184) // 8, (hi - 184) // 8)
        lo, hi = max(at, OUT), min(end, SHORT)
        if lo < hi:
            pack_out((lo - OUT) // 4, (hi - OUT) // 4)
        if at <= SHORT < end:
            pack_short()
        if at <= FC < end:
            pack_fc()
        if at <= BN < end:
            pack_bn()

    lane_row = lax.broadcasted_iota(jnp.int32, (1, LANES), 1)

    def own_pieces():
        need('own')
        for rows, tile, ref, tensors in momentum_rows(p_mid, p_in, p_out):
            v_own[rows, :] = ref[tensors, tile]
        v_own[IN0:IN0 + 2, :] = p_in0[...]
        v_own[SHORT:SHORT + 8, :] = p_short[...]
        flat = [p_fc[pl.ds(128 * q, 128)].reshape(1, LANES) for q in range(6)]
        flat.append(jnp.concatenate([p_fc[pl.ds(768, 32)].reshape(1, 32), jnp.zeros((1, 96), F32)], axis=1))
        for r in range(8):
            q, s = divmod(CLASSES * r, LANES)
            row = pltpu.roll(flat[q], (LANES - s) % LANES, 1)
            if s + CLASSES > LANES:
                row = jnp.where(lane_row < LANES - s, row, pltpu.roll(flat[q + 1], LANES - s, 1))
            v_own[FC + r:FC + r + 1, :] = jnp.where(lane_row < CLASSES, row, 0.0)
        v_own[BN:ROWS, :] = jnp.zeros((8, LANES), F32)
        odd = lax.rem(rank, 2) == 1
        rows = [p_bn[pl.ds(128 * k, 128)].reshape(1, LANES) for k in range(3)]
        rows.append(jnp.concatenate([p_bn[pl.ds(384, 64)].reshape(1, 64), jnp.zeros((1, 64), F32)], axis=1))
        for k in range(4):
            before = pltpu.roll(rows[k - 1], 64, 1) if k else jnp.zeros((1, LANES), F32)
            moved = jnp.where(lane_row < 64, before, pltpu.roll(rows[k], 64, 1))
            v_own[BN + k:BN + k + 1, :] = jnp.where(odd, moved, rows[k])
        four = jnp.concatenate([p_bias[...].reshape(1, 4), jnp.zeros((1, LANES - 4), F32)], axis=1)
        v_own[BIAS:BIAS + 1, :] = pltpu.roll(four, 4 * rank, 1)

        for t in range(N_MID):
            even = o_mid[t, pl.ds(mid_off, 9, stride=2), :]
            odds = o_mid[t, pl.ds(mid_off + 1, 9, stride=2), :]
            w_own[mid_row(t):mid_row(t) + 9, :] = jnp.concatenate([even, odds], axis=1)
        for j in range(9):
            other = o_in[2 * j - 1] if j else o_in0[...]
            ot[...] = jnp.concatenate([other, o_in[2 * j]], axis=0).T
            if j == 0:
                w_own[IN0:IN0 + 2, :] = left(ot[pl.ds(4 * rank, 2, stride=2), :], ot[pl.ds(4 * rank + 1, 2, stride=2), :])
            even = ot[pl.ds(col_off, 4, stride=2), :]
            odds = ot[pl.ds(col_off + 1, 4, stride=2), :]
            if j:
                w_own[in_row(2 * j - 1):in_row(2 * j - 1) + 4, :] = left(even, odds)
            w_own[in_row(2 * j):in_row(2 * j) + 4, :] = right(even, odds)
        def own_out(t, carry):
            for p in range(2):
                for h in range(2):
                    w_own[pl.ds(OUT + 4 * t + 2 * p + h, 1), :] = o_out[h, t, pl.ds(out_off + p, 1), :]
            return carry

        lax.fori_loop(0, N_OUT, own_out, 0)
        for p in range(4):
            for h in range(2):
                w_own[SHORT + 2 * p + h:SHORT + 2 * p + h + 1, :] = o_short[h, pl.ds(short_off + p, 1), :]
        ot[0:CLASSES, :] = o_fc[...]
        ot[CLASSES:LANES, :] = jnp.zeros((LANES - CLASSES, LANES), F32)
        ot[...] = ot[...].T
        w_own[FC:FC + 8, :] = ot[pl.ds(col_off, 8), :]
        w_own[BN:ROWS, :] = jnp.zeros((8, LANES), F32)
        bn_at = 7 * (rank // 2) + 3 * lax.rem(rank, 2)
        for k in range(4):
            w_own[BN + k:BN + k + 1, :] = o_bn[pl.ds(bn_at + k, 1), :]
        bias = jnp.concatenate([o_bias[...].reshape(1, CLASSES), jnp.zeros((1, LANES - CLASSES), F32)], axis=1)
        w_own[BIAS:BIAS + 1, :] = jnp.where((lane_row >= 4 * rank) & (lane_row < 4 * rank + 4), bias, 0.0)

    outs = []
    sent = {}

    def start(c, k, src, dst, peer):
        pltpu.make_async_remote_copy(src_ref=src, dst_ref=dst, send_sem=send.at[c * N_SEMS + k],
                                     recv_sem=recv.at[c * N_SEMS + k], device_id=peer, device_id_type=MESH).start()
        sent[c, k] = sent.get((c, k), 0) + (1 if len(src.shape) == 2 else src.size // (src.shape[-1] * src.shape[-2]))

    def wait(c, k, semaphores):
        at, size, _ = CHUNKS[c]
        rows = pl.ds(at, size)
        count = sent[c, k]
        if count == 8:
            block = got_core.at[:, :, 0, rows, :]
        elif count == 1:
            block = got_core.at[0, 0, 0, rows, :]
        else:
            block = got_core.at[pl.ds(0, count), 0, 0, rows, :]
        pltpu.make_async_copy(block, block, semaphores.at[c * N_SEMS + k]).wait()

    def arrived(c, *numbers):
        for k in numbers:
            wait(c, k, recv)

    def keep(src, dst):
        copy = pltpu.make_async_copy(src, dst, out_sems.at[len(outs)])
        copy.start()
        outs.append(copy)

    def step(c, stage):
        at, size, first = CHUNKS[c]
        rows = pl.ds(at, size)
        x_first = first == 'x'
        one_peer, two_peer = (x_peer, y_peer) if x_first else (y_peer, x_peer)

        here = y if x_first else x

        def block(ref, near, *rest):
            first_at = (x if near else 1 - x) if x_first else (y if near else 1 - y)
            return ref.at[(slice(None), slice(None), first_at) + rest] if x_first else (
                ref.at[(slice(None), first_at, slice(None)) + rest])

        def spot(second, near):
            return (second, x if near else 1 - x) if x_first else (y if near else 1 - y, second)

        def both_cores(zz, second, near):
            a, b = spot(second, near)
            return packed[zz, a, b, core, rows, :] + got_core[zz, a, b, rows, :]

        def over_z(body):
            def run(zz, carry):
                body(zz)
                return carry

            lax.fori_loop(0, 4, run, 0)

        if stage == 0:
            pack(at, size)
            if not sent:
                pl.semaphore_wait(barrier, N_DEV - 1)
            for k, near in enumerate((False, True)):
                start(c, S_CORE + k, block(packed, near, 1 - core, rows), block(got_core, near, rows), core_peer)
        elif stage == 1:
            arrived(c, S_CORE)
            for k, second in enumerate((1 - here, here)):
                a, b = spot(second, False)

                def body(zz, a=a, b=b, second=second):
                    acc[zz, a, b, rows, :] = both_cores(zz, second, False)

                over_z(body)
                start(c, S_ONE + k, acc.at[:, a, b, rows, :], got_one.at[:, second, rows, :], one_peer)
        elif stage == 2:
            arrived(c, S_CORE + 1, S_ONE)
            a, b = spot(1 - here, True)

            def body(zz):
                acc[zz, a, b, rows, :] = both_cores(zz, 1 - here, True) + got_one[zz, 1 - here, rows, :]

            over_z(body)
            for d in (1, 2, 3, 0):
                zz = lax.rem(z + d, 4)
                start(c, S_TWO + (d == 0), acc.at[zz, a, b, rows, :], got_two.at[zz, rows, :], two_peer)
        elif stage == 3:
            arrived(c, S_ONE + 1, S_TWO)
            for d in (2, 3, 1):
                zz = lax.rem(z + d, 4)
                acc[zz, y, x, rows, :] = (
                    both_cores(zz, here, True) + got_one[zz, here, rows, :] + got_two[zz, rows, :])
                start(c, S_Z, acc.at[zz, y, x, rows, :], got_z.at[d - 1, rows, :], device(zz, y, x, core))
        elif stage == 4:
            arrived(c, S_TWO + 1, S_Z)
            mean = both_cores(z, here, True) + got_one[z, here, rows, :] + got_two[z, rows, :]
            mean = (mean + got_z[0, rows, :] + got_z[1, rows, :] + got_z[2, rows, :]) * (1.0 / N_DEV)
            grad[rows, :] = mean
            own = w_own[rows, :]
            g_sum = jnp.sum(mean * mean, axis=1, keepdims=True)
            w_sum = jnp.sum(own * own, axis=1, keepdims=True)
            row = lax.broadcasted_iota(jnp.int32, (size, LANES), 0) + at
            lane = lax.broadcasted_iota(jnp.int32, (size, LANES), 1)
            tensor = jnp.where(lane < 64, lane, lane - 64)
            member = member_rows(row, tensor)
            part = jnp.where(member, jnp.where(lane < 64, g_sum, w_sum), 0.0)
            norms[c, rank] = jnp.sum(part, axis=0, keepdims=True)

            def tell(d, carry):
                pltpu.make_async_remote_copy(
                    src_ref=norms.at[c, rank], dst_ref=norms.at[c, rank], send_sem=n_send.at[c],
                    recv_sem=n_recv.at[c], device_id=(lax.rem(rank + d, N_DEV),), device_id_type=MESH).start()
                return carry

            lax.fori_loop(1, N_DEV, tell, 0)
        elif stage == 5:
            others = norms.at[c, pl.ds(0, N_DEV - 1)]
            pltpu.make_async_copy(others, others, n_recv.at[c]).wait()
            total = jnp.sum(norms[c], axis=0)
            g_norm = jnp.sqrt(total)
            w_norm = pltpu.roll(g_norm, 64, 1)
            trust = jnp.where((w_norm > 0) & (g_norm > 0), TRUST_COEF * w_norm / (g_norm + DECAY * w_norm), 1.0)
            row = lax.broadcasted_iota(jnp.int32, (size, LANES), 0) + at
            lane = lax.broadcasted_iota(jnp.int32, (size, LANES), 1)
            trust = jnp.where(lane == ID_PLAIN, 1.0, trust)
            member = member_rows(row, lane) & (lane <= ID_PLAIN)
            rate = lr[0] * jnp.sum(jnp.where(member, trust, 0.0), axis=1, keepdims=True)
            decay = jnp.where(row < BN, DECAY, 0.0)
            own = w_own[rows, :]
            moment = MOMENTUM * v_own[rows, :] + rate * (grad[rows, :] + decay * own)
            v_new[rows, :] = moment
            keep(v_new.at[rows, :], v_out_rows.at[rows, :])
            mine = (row != BIAS) | ((lane >= 4 * rank) & (lane < 4 * rank + 4))
            full[z, y, x, core, rows, :] = jnp.where(mine, own - moment, 0.0)
            piece = full.at[z, y, x, core, rows, :]
            for d in (2, 3, 1):
                start(c, A_Z, piece, piece, device(lax.rem(z + d, 4), y, x, core))
            start(c, A_TWO, piece, piece, two_peer)
        elif stage == 6:
            arrived(c, A_Z)
            for d in (1, 2, 3):
                piece = full.at[lax.rem(z + d, 4), y, x, core, rows, :]
                start(c, A_TWO + 1, piece, piece, two_peer)
            line = full.at[:, y, x, core, rows, :]
            start(c, A_ONE, line, line, one_peer)
        elif stage == 7:
            arrived(c, A_TWO, A_TWO + 1)
            a, b = spot(1 - here, True)
            line = full.at[:, a, b, core, rows, :]
            start(c, A_ONE + 1, line, line, one_peer)
            plane = block(full, True, core, rows)
            start(c, A_CORE, plane, plane, core_peer)
        elif stage == 8:
            arrived(c, A_ONE, A_ONE + 1)
            plane = block(full, False, core, rows)
            start(c, A_CORE + 1, plane, plane, core_peer)
        else:
            arrived(c, A_CORE, A_CORE + 1)
            keep(full.at[:, :, :, :, rows, :], full_out.at[:, :, :, :, rows, :])

    for c, stage in STEPS:
        if stage == 3 and not any(k == S_Z for _, k in sent):
            own_pieces()
        step(c, stage)
    for c, k in sent:
        wait(c, k, send)
    for c in range(len(CHUNKS)):
        others = norms.at[c, pl.ds(0, N_DEV - 1)]
        pltpu.make_async_copy(others, others, n_send.at[c]).wait()
    for copy in outs:
        copy.wait()


def exchange(operands):
    any_ = pl.BlockSpec(memory_space=pl.ANY)
    count = len(CHUNKS)
    bf = jnp.bfloat16
    shapes = [(N_MID, 576, 64), (N_IN, 64, 256), (64, 128), (2, N_OUT, 64, 128), (2, 128, 128), (112, 128)]
    own = [(N_MID, 24, 64), (N_IN, 64, 128), (64, 128), (2, N_OUT, 8, 128), (2, 8, 128), (CLASSES, 128), (112, 128),
           (CLASSES,), (128, 128), (N_MID, 1152), (N_IN, 512), (2, LANES), (N_OUT, 512), (8, LANES), (800,), (448,), (4,)]
    rows = (ROWS, LANES)
    exchanged = [(4, 2, 2) + rows, (4, 2, 2) + rows, (4, 2) + rows, (4,) + rows, (3,) + rows, rows,
                 (count, N_DEV, 1, LANES)]
    dma = pltpu.SemaphoreType.DMA
    full, v_new = pl.pallas_call(
        exchange_kernel,
        out_shape=(jax.ShapeDtypeStruct((4, 2, 2, 2) + rows, F32), jax.ShapeDtypeStruct(rows, F32)),
        in_specs=[pl.BlockSpec(memory_space=pltpu.SMEM)] + [any_] * 24,
        out_specs=(any_, any_),
        scratch_shapes=[VMEM(s, F32) for s in shapes]
        + [VMEM((1024, 256), bf), VMEM((CLASSES, 1024), bf), VMEM((256, 128), F32), VMEM((128, 256), F32)]
        + [VMEM(s, F32) for s in own]
        + [VMEM((4, 2, 2, 2) + rows, F32), VMEM(rows, F32), VMEM(rows, F32), VMEM(rows, F32),
           VMEM((4, 2, 2, 2) + rows, F32)]
        + [VMEM(s, F32) for s in exchanged]
        + [dma((40,)), dma((2 * count,)), dma((count * N_SEMS,)), dma((count * N_SEMS,)), dma((count,)), dma((count,))],
        compiler_params=pltpu.CompilerParams(vmem_limit_bytes=VMEM_LIMIT, collective_id=0, has_side_effects=True),
    )(*operands)
    return full.reshape(N_DEV, ROWS, LANES), v_new


def unpack_kernel(packed_rows, v_rows, n_mid, n_in, n_in0, n_out, n_short, n_fc, n_bn, n_bias,
                  b_mid, b_in, b_in0, b_out, b_short, b_fc, v_mid, v_in, v_in0, v_out, v_short, v_fc, v_bn, v_bias,
                  packed, v_own, s_mid, s_in, s_out, s_short, s_in0, s_fc, t_mid, t_in, t_out, t_short, t_in0, t_fc, xt, sems):
    bf = jnp.bfloat16
    lane_row = lax.broadcasted_iota(jnp.int32, (1, LANES), 1)
    pieces = packed.reshape(N_DEV, ROWS, LANES)
    fetches = []
    for k, (at, size) in enumerate(((0, 40), (40, 120), (160, 24), (184, 48), (232, 72), (304, 24))):
        fetches.append(pltpu.make_async_copy(packed_rows.at[:, pl.ds(at, size), :], pieces.at[:, pl.ds(at, size), :],
                                             sems.at[12 + k]))
    fetches.append(pltpu.make_async_copy(v_rows, v_own, sems.at[18]))
    for copy in fetches:
        copy.start()

    def put(src, dst, k):
        pltpu.make_async_copy(src, dst, sems.at[k]).start()

    def mid_body(t, carry):
        for a in range(4):
            for k in range(9):
                x = packed[across(a, mid_row(t) + k), :]
                s_mid[t, pl.ds(144 * a + 2 * k, 8, stride=18), :] = x[:, :64]
                s_mid[t, pl.ds(144 * a + 2 * k + 1, 8, stride=18), :] = x[:, 64:]
        put(s_mid.at[t], n_mid.at[t], 0)
        t_mid[t] = s_mid[t].astype(bf)
        put(t_mid.at[t], b_mid.at[t], 1)
        return carry

    fetches[0].wait()
    lax.fori_loop(0, 4, mid_body, 0)
    fetches[1].wait()
    lax.fori_loop(4, 16, mid_body, 0)
    fetches[2].wait()
    lax.fori_loop(16, N_MID, mid_body, 0)
    fetches[3].wait()

    def in_pair(first, second, row, other):
        for a in range(4):
            for k in range(4):
                x = packed[across(a, row + k), :]
                y = packed[across(a, other + k), :]
                xt[pl.ds(64 * a + 2 * k, 8, stride=8), :] = left(x, y)
                xt[pl.ds(64 * a + 2 * k + 1, 8, stride=8), :] = right(x, y)
        for h in range(2):
            cols = xt[128 * h:128 * h + 128, :].T
            for u, t in enumerate((first, second)):
                s_in[t, :, 128 * h:128 * h + 128] = cols[64 * u:64 * u + 64]
                t_in[t, :, 128 * h:128 * h + 128] = cols[64 * u:64 * u + 64].astype(bf)
        for t in (first, second):
            put(s_in.at[t], n_in.at[t], 2)
            put(t_in.at[t], b_in.at[t], 3)

    def in_body(j, carry):
        in_pair(2 * j + 5, 2 * j + 6, 184 + 8 * j, 188 + 8 * j)
        return carry

    lax.fori_loop(0, 6, in_body, 0)
    in_pair(0, 1, in_row(0), in_row(1))
    in_pair(2, 3, in_row(2), in_row(3))
    for a in range(4):
        for k in range(4):
            x = packed[across(a, in_row(4) + k), :]
            xt[pl.ds(64 * a + 2 * k, 8, stride=8), :] = x
            xt[pl.ds(64 * a + 2 * k + 1, 8, stride=8), :] = right(x, x)
    for h in range(2):
        cols = xt[128 * h:128 * h + 128, :].T
        s_in[4, :, 128 * h:128 * h + 128] = cols[:64]
        t_in[4, :, 128 * h:128 * h + 128] = cols[:64].astype(bf)
    put(s_in.at[4], n_in.at[4], 2)
    put(t_in.at[4], b_in.at[4], 3)
    for a in range(4):
        for k in range(2):
            x = packed[across(a, IN0 + k), :]
            xt[pl.ds(32 * a + 2 * k, 8, stride=4), :] = x
            xt[pl.ds(32 * a + 2 * k + 1, 8, stride=4), :] = right(x, x)
    cols = xt[0:128, :].T
    s_in0[...] = cols[:64]
    t_in0[...] = cols[:64].astype(bf)
    put(s_in0, n_in0, 4)
    put(t_in0, b_in0, 5)

    def out_body(t, carry):
        for a in range(4):
            for p in range(2):
                for h in range(2):
                    s_out[h, t, pl.ds(16 * a + p, 8, stride=2), :] = packed[across(a, OUT + 4 * t + 2 * p + h), :]
        for h in range(2):
            t_out[h, t] = s_out[h, t].astype(bf)
            put(s_out.at[h, t], n_out.at[t, :, pl.ds(128 * h, 128)], 6)
            put(t_out.at[h, t], b_out.at[t, :, pl.ds(128 * h, 128)], 7)
        return carry

    fetches[4].wait()
    lax.fori_loop(0, N_OUT, out_body, 0)
    fetches[5].wait()
    for h in range(2):
        for a in range(4):
            for p in range(4):
                s_short[h, pl.ds(32 * a + p, 8, stride=4), :] = packed[across(a, SHORT + 2 * p + h), :]
        t_short[h] = s_short[h].astype(bf)
        put(s_short.at[h], n_short.at[:, pl.ds(128 * h, 128)], 8)
        put(t_short.at[h], b_short.at[:, pl.ds(128 * h, 128)], 9)
    for i in range(N_DEV):
        xt[8 * i:8 * i + 8, :] = packed[i * ROWS + FC:i * ROWS + FC + 8, :]
    for h in range(2):
        cols = xt[128 * h:128 * h + 128, :].T
        s_fc[:, 128 * h:128 * h + 128] = cols[:CLASSES]
        t_fc[:, 128 * h:128 * h + 128] = cols[:CLASSES].astype(bf)
    put(s_fc, n_fc, 10)
    put(t_fc, b_fc, 11)

    lane = lax.broadcasted_iota(jnp.int32, (8, LANES), 1)
    for b in range(2):
        def even(k):
            return packed[pl.ds(16 * b * ROWS + BN + k, 8, stride=2 * ROWS), :]

        def odd(k):
            return packed[pl.ds((16 * b + 1) * ROWS + BN + k, 8, stride=2 * ROWS), :]

        for k in range(3):
            n_bn[pl.ds(56 * b + k, 8, stride=7), :] = even(k)
            n_bn[pl.ds(56 * b + 4 + k, 8, stride=7), :] = odd(1 + k)
        n_bn[pl.ds(56 * b + 3, 8, stride=7), :] = jnp.where(lane < 64, even(3), odd(0))
    total = packed[across(0, BIAS), :]
    for a in range(1, 4):
        total = total + packed[across(a, BIAS), :]
    n_bias[...] = jnp.sum(total, axis=0, keepdims=True)[0, :CLASSES]
    fetches[6].wait()

    for rows, tile, ref, tensors in momentum_rows(v_mid, v_in, v_out):
        ref[tensors, tile] = v_own[rows, :]
    rank = lax.axis_index('dp')
    v_in0[...] = v_own[IN0:IN0 + 2, :]
    v_short[...] = v_own[SHORT:SHORT + 8, :]
    for q in range(7):
        flat = jnp.zeros((1, LANES), F32)
        for r in range(8):
            d = CLASSES * r - LANES * q
            if -CLASSES < d < LANES:
                row = pltpu.roll(v_own[FC + r:FC + r + 1, :], d % LANES, 1)
                flat = jnp.where((lane_row >= d) & (lane_row < d + CLASSES), row, flat)
        size = min(LANES, 800 - LANES * q)
        v_fc[pl.ds(LANES * q, size)] = flat[0, :size]
    odd = lax.rem(rank, 2) == 1
    for k in range(4):
        here = v_own[BN + k:BN + k + 1, :]
        after = v_own[BN + k + 1:BN + k + 2, :]
        moved = jnp.where(lane_row < 64, pltpu.roll(here, 64, 1), pltpu.roll(after, 64, 1))
        size = min(LANES, 448 - LANES * k)
        v_bn[pl.ds(LANES * k, size)] = jnp.where(odd, moved, here)[0, :size]
    v_bias[...] = pltpu.roll(v_own[BIAS:BIAS + 1, :], lax.rem(N_DEV - rank, N_DEV) * 4, 1)[0, :4]

    for k, (src, dst) in enumerate(((s_mid, n_mid), (t_mid, b_mid), (s_in, n_in), (t_in, b_in), (s_in0, n_in0),
                                    (t_in0, b_in0))):
        pltpu.make_async_copy(src, dst, sems.at[k]).wait()
    for h in range(2):
        half = pl.ds(128 * h, 128)
        for k, (src, dst) in enumerate(((s_out, n_out.at[:, :, half]), (t_out, b_out.at[:, :, half]),
                                        (s_short, n_short.at[:, half]), (t_short, b_short.at[:, half]))):
            pltpu.make_async_copy(src.at[h], dst, sems.at[6 + k]).wait()
    pltpu.make_async_copy(s_fc, n_fc, sems.at[10]).wait()
    pltpu.make_async_copy(t_fc, b_fc, sems.at[11]).wait()


def unpack_weights(packed, v_own):
    any_ = pl.BlockSpec(memory_space=pl.ANY)
    vm = pl.BlockSpec(memory_space=VMEM)
    bf = jnp.bfloat16
    kernels = ((N_MID, 576, 64), (N_IN, 64, 256), (64, 128), (N_OUT, 64, 256), (128, 256), (CLASSES, 256))
    shapes = [(s, F32) for s in kernels] + [((112, 128), F32), ((CLASSES,), F32)] + [(s, bf) for s in kernels]
    shapes += [(s, F32) for s in ((N_MID, 1152), (N_IN, 512), (2, LANES), (N_OUT, 512), (8, LANES), (800,), (448,), (4,))]
    scratch = ((N_MID, 576, 64), (N_IN, 64, 256), (2, N_OUT, 64, 128), (2, 128, 128), (64, 128), (CLASSES, 256))
    return pl.pallas_call(
        unpack_kernel,
        out_shape=[jax.ShapeDtypeStruct(s, d) for s, d in shapes],
        in_specs=[any_, any_],
        out_specs=[any_] * 6 + [vm] * 2 + [any_] * 6 + [vm] * 8,
        scratch_shapes=[VMEM((N_DEV * ROWS, LANES), F32), VMEM((ROWS, LANES), F32)] + [VMEM(s, F32) for s in scratch] + [VMEM(s, bf) for s in scratch]
        + [VMEM((256, 128), F32), pltpu.SemaphoreType.DMA((19,))],
        compiler_params=pltpu.CompilerParams(vmem_limit_bytes=VMEM_LIMIT),
    )(packed, v_own)


def solution(mesh):
    spec_full = P()
    spec_lead = P('dp')
    spec_cols = P(None, 'dp')
    moment_specs = (spec_lead, spec_lead, spec_cols, spec_cols, spec_cols, spec_lead, spec_lead, spec_lead)
    in_specs = (spec_full,) * 8 + (spec_lead,) * 8 + moment_specs + (spec_full,)
    out_specs = (spec_full,) * 14 + moment_specs

    def body(w_in0, w_short, w_in, w_mid, w_out, w_fc, w_bn, w_bias,
             g_in0, g_short, g_in, g_mid, g_out, g_bn, pooled, dlogits,
             v_in0, v_short, v_in, v_mid, v_out, v_fc, v_bn, v_bias, learn_rate):
        gathered, v_next = exchange((
            learn_rate.reshape(1), g_mid.reshape(N_MID, 576, 64), jnp.swapaxes(g_in[0], 1, 2), g_in0[0].T, g_out[0],
            g_short[0], g_bn.reshape(112, LANES), pooled, dlogits.T,
            w_mid.reshape(N_MID, 576, 64), jnp.swapaxes(w_in, 1, 2), w_in0.T, w_out, w_short, w_fc.T,
            w_bn.reshape(112, LANES), w_bias, v_mid, v_in, v_in0.reshape(2, LANES), v_out, v_short.reshape(8, LANES),
            v_fc, v_bn, v_bias))
        (n_mid, n_in, n_in0, n_out, n_short, n_fc, n_bn, n_bias, b_mid, b_in, b_in0, b_out, b_short, b_fc,
         m_mid, m_in, m_in0, m_out, m_short, m_fc, m_bn, m_bias) = unpack_weights(gathered, v_next)
        return (n_in0.T, n_short, jnp.swapaxes(n_in, 1, 2), n_mid.reshape(w_mid.shape), n_out, n_fc.T,
                n_bn.reshape(-1), n_bias,
                b_in0.T, b_short, jnp.swapaxes(b_in, 1, 2), b_mid.reshape(w_mid.shape), b_out, b_fc.T,
                m_in0.reshape(-1), m_short.reshape(-1), m_in, m_mid, m_out, m_fc, m_bn, m_bias)

    return jax.shard_map(body, mesh=mesh, in_specs=in_specs, out_specs=out_specs, check_vma=False)
```

```python
import jax
import jax.numpy as jnp
from jax import lax
from jax.experimental import pallas as pl
from jax.experimental.pallas import tpu as pltpu
from jax.sharding import PartitionSpec as P

MOMENTUM = 0.9
TRUST_COEF = 0.001
DECAY = 0.0001
N_DEV = 32
LANES = 128
IN0, OUT, SHORT, FC, BN, BIAS, ROWS = 178, 232, 304, 312, 320, 324, 328
N_MID, N_IN, N_OUT = 18, 17, 18
CLASSES = 100
ID_IN0, ID_IN, ID_OUT, ID_SHORT, ID_FC, ID_PLAIN = 18, 19, 36, 54, 55, 56
F32 = jnp.float32
VMEM = pltpu.VMEM
MESH = pl.DeviceIdType.MESH
CHUNKS = (
    (0, 40, 'x'), (40, 40, 'y'), (80, 40, 'x'), (120, 40, 'y'), (160, 24, 'y'),
    (184, 24, 'y'), (208, 24, 'y'), (232, 32, 'y'), (264, 40, 'x'), (304, 24, 'x'),
)
STEPS = (
    (3, 0), (8, 0), (6, 0), (3, 1), (8, 1), (0, 0), (6, 1), (5, 0), (4, 0), (3, 2), (7, 0), (4, 1), (2, 0), (8, 2),
    (0, 1), (1, 0), (6, 2), (3, 3), (4, 2), (0, 2), (1, 1), (8, 3), (2, 1), (9, 0), (6, 3), (4, 3), (3, 4), (0, 3),
    (1, 2), (2, 2), (8, 4), (7, 1), (9, 1), (3, 5), (1, 3), (6, 4), (2, 3), (4, 4), (5, 1), (7, 2), (8, 5), (9, 2),
    (3, 6), (4, 5), (7, 3), (0, 4), (6, 5), (1, 4), (5, 2), (9, 3), (2, 4), (8, 6), (3, 7), (0, 5), (5, 3), (4, 6),
    (1, 5), (7, 4), (6, 6), (9, 4), (3, 8), (2, 5), (8, 7), (0, 6), (5, 4), (7, 5), (4, 7), (1, 6), (6, 7), (9, 5),
    (2, 6), (8, 8), (4, 8), (5, 5), (0, 7), (6, 8), (7, 6), (1, 7), (9, 6), (0, 8), (2, 7), (5, 6), (1, 8), (7, 7),
    (9, 7), (5, 7), (2, 8), (4, 9), (6, 9), (7, 8), (4, 10), (9, 8), (8, 9), (0, 9), (5, 8), (2, 9), (3, 9), (1, 9),
    (7, 9), (8, 10), (9, 9), (5, 9), (1, 10), (7, 10), (0, 10), (6, 10), (9, 10), (3, 10), (2, 10), (5, 10),
)
S_CORE, S_ONE, S_TWO, S_Z, A_Z, A_TWO, A_ONE, A_CORE, N_SEMS = 0, 2, 4, 6, 7, 8, 10, 12, 14
VMEM_LIMIT = 60 * 2**20


def mid_row(t):
    return 40 * (t // 4) + 9 * (t % 4)


def in_row(t):
    return 36 + 40 * t if t < 4 else 164 + 4 * t


def member_rows(row, t):
    first = 9 * t
    for group in (4, 8, 12, 16):
        first = jnp.where(t >= group, first + 4, first)
    size = jnp.where(t < N_MID, 9, jnp.where(t == ID_IN0, 2, jnp.where(t < ID_SHORT, 4, 8)))
    first = jnp.where(t >= ID_IN0, IN0, first)
    first = jnp.where(t >= ID_IN, 36 + 40 * (t - ID_IN), first)
    first = jnp.where(t >= ID_IN + 4, 164 + 4 * (t - ID_IN), first)
    first = jnp.where(t >= ID_OUT, OUT + 4 * (t - ID_OUT), first)
    first = jnp.where(t >= ID_SHORT, SHORT + 8 * (t - ID_SHORT), first)
    return (row >= first) & (row < first + size)


def momentum_rows(mid, inn, out):
    runs = [(mid, mid_row(t), 9, t, min(4, N_MID - t)) for t in range(0, N_MID, 4)]
    runs += [(inn, 36, 40, 0, 4)] + [(inn, 164 + 4 * t, 4, t, min(8, N_IN - t)) for t in (4, 12)]
    runs += [(out, OUT + 4 * t, 4, t, min(8, N_OUT - t)) for t in (0, 8, 16)]
    for ref, base, stride, t, count in runs:
        for m in range(9 if ref is mid else 4):
            yield pl.ds(base + m, count, stride=stride), pl.ds(128 * m, 128), ref, pl.ds(t, count)


def left(a, b):
    return jnp.concatenate([a[:, :64], b[:, :64]], axis=1)


def right(a, b):
    return jnp.concatenate([a[:, 64:], b[:, 64:]], axis=1)


def across(piece8, row):
    return pl.ds(piece8 * 8 * ROWS + row, 8, stride=ROWS)


def exchange_kernel(lr, g_mid, g_in, g_in0, g_out, g_short, g_bn, pooled, dlog_t,
                    w_mid, w_in, w_in0, w_out, w_short, w_fc, w_bn, w_bias,
                    v_mid, v_in, v_in0, v_out, v_short, v_fc, v_bn, v_bias,
                    full_out, v_out_rows,
                    s_mid, s_in, s_in0, s_out, s_short, s_bn, s_x, s_d, xt, fct,
                    o_mid, o_in, o_in0, o_out, o_short, o_fc, o_bn, o_bias, ot,
                    p_mid, p_in, p_in0, p_out, p_short, p_fc, p_bn, p_bias,
                    packed, w_own, v_own, v_new, full,
                    got_core, acc, got_one, got_two, got_z, grad, layer_norms, norms,
                    sems, out_sems, send, recv, n_send, n_recv):
    rank = lax.axis_index('dp')
    core = lax.rem(rank, 2)
    x = lax.rem(rank // 2, 2)
    y = lax.rem(rank // 4, 2)
    z = rank // 8

    def device(zz, yy, xx, cc):
        return (((zz * 2 + yy) * 2 + xx) * 2 + cc,)

    core_peer = device(z, y, x, 1 - core)
    x_peer = device(z, y, 1 - x, core)
    y_peer = device(z, 1 - y, x, core)

    barrier = pltpu.get_barrier_semaphore()

    def layer(d):
        return (z * 8 + lax.rem(rank + d, 8),)

    def line(d):
        return (lax.rem(rank + 8 * d, N_DEV),)

    for d in range(1, 8):
        pl.semaphore_signal(barrier, inc=1, device_id=layer(d), device_id_type=MESH)
    for d in range(1, 4):
        pl.semaphore_signal(barrier, inc=1, device_id=line(d), device_id_type=MESH)

    waiting = {}
    count = [0]

    def fetch(name, src, dst):
        copy = pltpu.make_async_copy(src, dst, sems.at[count[0]])
        count[0] += 1
        copy.start()
        waiting.setdefault(name, []).append(copy)

    def need(*names):
        for name in names:
            for copy in waiting.pop(name, []):
                copy.wait()

    def halves(name, src, dst):
        for h in range(2):
            fetch(name, src(pl.ds(128 * h, 128)), dst.at[h])

    fetchers = {
        'in': lambda: fetch('in', g_in.at[pl.ds(5, 12)], s_in.at[pl.ds(5, 12)]),
        'in1': lambda: fetch('in1', g_in.at[pl.ds(0, 5)], s_in.at[pl.ds(0, 5)]),
        'in0': lambda: fetch('in0', g_in0, s_in0),
        'out': lambda: halves('out', lambda c: g_out.at[:, :, c], s_out),
        'short': lambda: halves('short', lambda c: g_short.at[:, c], s_short),
        'fc': lambda: (fetch('fc', pooled, s_x), fetch('fc', dlog_t, s_d)),
        'bn': lambda: fetch('bn', g_bn, s_bn),
    }
    for i in range(5):
        part = pl.ds(4 * i, min(4, N_MID - 4 * i))
        fetchers['mid%d' % i] = lambda i=i, part=part: fetch('mid%d' % i, g_mid.at[part], s_mid.at[part])
    units = [(40 * i, 40 * i + 40, ('mid%d' % i, 'in1')) for i in range(4)] + [(160, 184, ('mid4', 'in0', 'in1'))]
    units += [(184 + 8 * j, 192 + 8 * j, ('in',)) for j in range(6)]
    units += [(232 + 8 * j, 240 + 8 * j, ('out',)) for j in range(9)]
    units += [(304, 312, ('short',)), (312, 320, ('fc',)), (320, 328, ('bn', 'fc'))]
    for at, size, _ in CHUNKS:
        for lo, hi, names in units:
            if at <= lo < at + size:
                for name in names:
                    if name in fetchers:
                        fetchers.pop(name)()

    mid_at = pl.multiple_of((18 * rank) // 8 * 8, 8)
    mid_off = lax.rem(18 * rank, 8)
    out_at = pl.multiple_of((2 * rank) // 8 * 8, 8)
    out_off = 2 * lax.rem(rank, 4)
    short_at = pl.multiple_of((4 * rank) // 8 * 8, 8)
    short_off = 4 * lax.rem(rank, 2)
    col_at = pl.multiple_of((rank // 16) * 128, 128)
    col_off = pl.multiple_of(lax.rem(rank, 16) * 8, 8)
    fetch('own', w_mid.at[:, pl.ds(mid_at, 24), :], o_mid)
    fetch('own', w_in.at[:, :, pl.ds(col_at, 128)], o_in)
    fetch('own', w_in0, o_in0)
    halves('own', lambda c: w_out.at[:, pl.ds(out_at, 8), c], o_out)
    halves('own', lambda c: w_short.at[pl.ds(short_at, 8), c], o_short)
    fetch('own', w_fc.at[:, pl.ds(col_at, 128)], o_fc)
    fetch('own', w_bn, o_bn)
    fetch('own', w_bias, o_bias)
    for src, dst in ((v_mid, p_mid), (v_in, p_in), (v_in0, p_in0), (v_out, p_out), (v_short, p_short), (v_fc, p_fc),
                     (v_bn, p_bn), (v_bias, p_bias)):
        fetch('own', src, dst)

    pieces = packed.reshape(N_DEV * ROWS, LANES)

    def pack_mid(base, first, count):
        def body(u, carry):
            t = first + u
            for a in range(4):
                for k in range(9):
                    even = s_mid[t, pl.ds(144 * a + 2 * k, 8, stride=18), :]
                    odd = s_mid[t, pl.ds(144 * a + 2 * k + 1, 8, stride=18), :]
                    pieces[across(a, base + 9 * u + k), :] = jnp.concatenate([even, odd], axis=1)
            return carry

        lax.fori_loop(0, count, body, 0)

    def pack_in_rows(base, pair):
        for a in range(4):
            for k in range(4):
                even = xt[pl.ds(64 * a + 2 * k, 8, stride=8), :]
                odd = xt[pl.ds(64 * a + 2 * k + 1, 8, stride=8), :]
                pieces[across(a, base + k), :] = left(even, odd)
                if pair:
                    pieces[across(a, base + 4 + k), :] = right(even, odd)

    def transpose(a, b):
        both = jnp.concatenate([a, b], axis=0)
        for h in range(2):
            xt[128 * h:128 * h + 128, :] = both[:, 128 * h:128 * h + 128].T

    def pack_in(first, last):
        def body(j, carry):
            transpose(s_in[2 * j + 5], s_in[2 * j + 6])
            pack_in_rows(184 + 8 * j, True)
            return carry

        lax.fori_loop(first, last, body, 0)

    def pack_in_one(t):
        wide = jnp.concatenate([s_in0[...], s_in0[...]], axis=1) if t == 4 else s_in[t]
        transpose(s_in[t], wide)
        pack_in_rows(in_row(t), False)
        if t == 4:
            for a in range(4):
                for k in range(2):
                    even = xt[pl.ds(32 * a + 2 * k, 8, stride=4), :]
                    odd = xt[pl.ds(32 * a + 2 * k + 1, 8, stride=4), :]
                    pieces[across(a, IN0 + k), :] = right(even, odd)

    def pack_out(first, last):
        def body(t, carry):
            for a in range(4):
                for p in range(2):
                    for h in range(2):
                        pieces[across(a, OUT + 4 * t + 2 * p + h), :] = s_out[h, t, pl.ds(16 * a + p, 8, stride=2), :]
            return carry

        lax.fori_loop(first, last, body, 0)

    def pack_short():
        for a in range(4):
            for p in range(4):
                for h in range(2):
                    pieces[across(a, SHORT + 2 * p + h), :] = s_short[h, pl.ds(32 * a + p, 8, stride=4), :]

    scale = 1.0 / pooled.shape[0]

    def pack_fc():
        fct[CLASSES:LANES, :] = jnp.zeros((LANES - CLASSES, 256), F32)
        fct[0:CLASSES, :] = jnp.dot(s_d[...], s_x[...], preferred_element_type=F32) * scale
        for h in range(2):
            cols = fct[:, 128 * h:128 * h + 128].T
            for j in range(16):
                at = (16 * h + j) * ROWS + FC
                pieces[at:at + 8, :] = cols[8 * j:8 * j + 8, :]

    def pack_bn():
        def clear(i, carry):
            pieces[pl.ds(pl.multiple_of(i * ROWS + BN, 8), 8), :] = jnp.zeros((8, LANES), F32)
            return carry

        lax.fori_loop(0, N_DEV, clear, 0)
        for b in range(2):
            for k in range(4):
                for half in range(2):
                    pieces[pl.ds((16 * b + half) * ROWS + BN + k, 8, stride=2 * ROWS), :] = (
                        s_bn[pl.ds(56 * b + 3 * half + k, 8, stride=7), :])
        bias = lax.dot_general(jnp.ones((8, s_d.shape[1]), jnp.bfloat16), s_d[...], (((1,), (1,)), ((), ())),
                               preferred_element_type=F32) * scale
        bias = jnp.concatenate([bias, jnp.zeros((8, LANES - CLASSES), F32)], axis=1)
        for a in range(4):
            pieces[across(a, BIAS), :] = bias

    def pack(at, size):
        end = at + size
        for lo, hi, names in units:
            if at <= lo < end:
                need(*names)
        for i in range(5):
            if at <= 40 * i < end:
                pack_mid(40 * i, 4 * i, min(4, N_MID - 4 * i))
                pack_in_one(i)
        lo, hi = max(at, 184), min(end, 232)
        if lo < hi:
            pack_in((lo - 184) // 8, (hi - 184) // 8)
        lo, hi = max(at, OUT), min(end, SHORT)
        if lo < hi:
            pack_out((lo - OUT) // 4, (hi - OUT) // 4)
        if at <= SHORT < end:
            pack_short()
        if at <= FC < end:
            pack_fc()
        if at <= BN < end:
            pack_bn()

    lane_row = lax.broadcasted_iota(jnp.int32, (1, LANES), 1)

    def own_pieces():
        need('own')
        for rows, tile, ref, tensors in momentum_rows(p_mid, p_in, p_out):
            v_own[rows, :] = ref[tensors, tile]
        v_own[IN0:IN0 + 2, :] = p_in0[...]
        v_own[SHORT:SHORT + 8, :] = p_short[...]
        flat = [p_fc[pl.ds(128 * q, 128)].reshape(1, LANES) for q in range(6)]
        flat.append(jnp.concatenate([p_fc[pl.ds(768, 32)].reshape(1, 32), jnp.zeros((1, 96), F32)], axis=1))
        for r in range(8):
            q, s = divmod(CLASSES * r, LANES)
            row = pltpu.roll(flat[q], (LANES - s) % LANES, 1)
            if s + CLASSES > LANES:
                row = jnp.where(lane_row < LANES - s, row, pltpu.roll(flat[q + 1], LANES - s, 1))
            v_own[FC + r:FC + r + 1, :] = jnp.where(lane_row < CLASSES, row, 0.0)
        v_own[BN:ROWS, :] = jnp.zeros((8, LANES), F32)
        odd = lax.rem(rank, 2) == 1
        rows = [p_bn[pl.ds(128 * k, 128)].reshape(1, LANES) for k in range(3)]
        rows.append(jnp.concatenate([p_bn[pl.ds(384, 64)].reshape(1, 64), jnp.zeros((1, 64), F32)], axis=1))
        for k in range(4):
            before = pltpu.roll(rows[k - 1], 64, 1) if k else jnp.zeros((1, LANES), F32)
            moved = jnp.where(lane_row < 64, before, pltpu.roll(rows[k], 64, 1))
            v_own[BN + k:BN + k + 1, :] = jnp.where(odd, moved, rows[k])
        four = jnp.concatenate([p_bias[...].reshape(1, 4), jnp.zeros((1, LANES - 4), F32)], axis=1)
        v_own[BIAS:BIAS + 1, :] = pltpu.roll(four, 4 * rank, 1)

        for t in range(N_MID):
            even = o_mid[t, pl.ds(mid_off, 9, stride=2), :]
            odds = o_mid[t, pl.ds(mid_off + 1, 9, stride=2), :]
            w_own[mid_row(t):mid_row(t) + 9, :] = jnp.concatenate([even, odds], axis=1)
        for j in range(9):
            other = o_in[2 * j - 1] if j else o_in0[...]
            ot[...] = jnp.concatenate([other, o_in[2 * j]], axis=0).T
            if j == 0:
                w_own[IN0:IN0 + 2, :] = left(ot[pl.ds(4 * rank, 2, stride=2), :], ot[pl.ds(4 * rank + 1, 2, stride=2), :])
            even = ot[pl.ds(col_off, 4, stride=2), :]
            odds = ot[pl.ds(col_off + 1, 4, stride=2), :]
            if j:
                w_own[in_row(2 * j - 1):in_row(2 * j - 1) + 4, :] = left(even, odds)
            w_own[in_row(2 * j):in_row(2 * j) + 4, :] = right(even, odds)
        def own_out(t, carry):
            for p in range(2):
                for h in range(2):
                    w_own[pl.ds(OUT + 4 * t + 2 * p + h, 1), :] = o_out[h, t, pl.ds(out_off + p, 1), :]
            return carry

        lax.fori_loop(0, N_OUT, own_out, 0)
        for p in range(4):
            for h in range(2):
                w_own[SHORT + 2 * p + h:SHORT + 2 * p + h + 1, :] = o_short[h, pl.ds(short_off + p, 1), :]
        ot[0:CLASSES, :] = o_fc[...]
        ot[CLASSES:LANES, :] = jnp.zeros((LANES - CLASSES, LANES), F32)
        ot[...] = ot[...].T
        w_own[FC:FC + 8, :] = ot[pl.ds(col_off, 8), :]
        w_own[BN:ROWS, :] = jnp.zeros((8, LANES), F32)
        bn_at = 7 * (rank // 2) + 3 * lax.rem(rank, 2)
        for k in range(4):
            w_own[BN + k:BN + k + 1, :] = o_bn[pl.ds(bn_at + k, 1), :]
        bias = jnp.concatenate([o_bias[...].reshape(1, CLASSES), jnp.zeros((1, LANES - CLASSES), F32)], axis=1)
        w_own[BIAS:BIAS + 1, :] = jnp.where((lane_row >= 4 * rank) & (lane_row < 4 * rank + 4), bias, 0.0)

    outs = []
    sent = {}

    def start(c, k, src, dst, peer):
        pltpu.make_async_remote_copy(src_ref=src, dst_ref=dst, send_sem=send.at[c * N_SEMS + k],
                                     recv_sem=recv.at[c * N_SEMS + k], device_id=peer, device_id_type=MESH).start()
        sent[c, k] = sent.get((c, k), 0) + (1 if len(src.shape) == 2 else src.size // (src.shape[-1] * src.shape[-2]))

    def wait(c, k, semaphores):
        at, size, _ = CHUNKS[c]
        rows = pl.ds(at, size)
        count = sent[c, k]
        if count == 8:
            block = got_core.at[:, :, 0, rows, :]
        elif count == 1:
            block = got_core.at[0, 0, 0, rows, :]
        else:
            block = got_core.at[pl.ds(0, count), 0, 0, rows, :]
        pltpu.make_async_copy(block, block, semaphores.at[c * N_SEMS + k]).wait()

    def arrived(c, *numbers):
        for k in numbers:
            wait(c, k, recv)

    def keep(src, dst):
        copy = pltpu.make_async_copy(src, dst, out_sems.at[len(outs)])
        copy.start()
        outs.append(copy)

    def tell(k, row, peer):
        pltpu.make_async_remote_copy(src_ref=row, dst_ref=row, send_sem=n_send.at[k], recv_sem=n_recv.at[k],
                                     device_id=peer, device_id_type=MESH).start()

    def told(k, semaphores):
        rows = layer_norms.at[k // 2, pl.ds(0, 3 if k % 2 else 7)]
        pltpu.make_async_copy(rows, rows, semaphores.at[k]).wait()

    def step(c, stage):
        at, size, first = CHUNKS[c]
        rows = pl.ds(at, size)
        x_first = first == 'x'
        one_peer, two_peer = (x_peer, y_peer) if x_first else (y_peer, x_peer)

        here = y if x_first else x

        def block(ref, near, *rest):
            first_at = (x if near else 1 - x) if x_first else (y if near else 1 - y)
            return ref.at[(slice(None), slice(None), first_at) + rest] if x_first else (
                ref.at[(slice(None), first_at, slice(None)) + rest])

        def spot(second, near):
            return (second, x if near else 1 - x) if x_first else (y if near else 1 - y, second)

        def both_cores(zz, second, near):
            a, b = spot(second, near)
            return packed[zz, a, b, core, rows, :] + got_core[zz, a, b, rows, :]

        def over_z(body):
            def run(zz, carry):
                body(zz)
                return carry

            lax.fori_loop(0, 4, run, 0)

        if stage == 0:
            pack(at, size)
            if not sent:
                pl.semaphore_wait(barrier, 10)
            for k, near in enumerate((False, True)):
                start(c, S_CORE + k, block(packed, near, 1 - core, rows), block(got_core, near, rows), core_peer)
        elif stage == 1:
            arrived(c, S_CORE)
            for k, second in enumerate((1 - here, here)):
                a, b = spot(second, False)

                def body(zz, a=a, b=b, second=second):
                    acc[zz, a, b, rows, :] = both_cores(zz, second, False)

                over_z(body)
                start(c, S_ONE + k, acc.at[:, a, b, rows, :], got_one.at[:, second, rows, :], one_peer)
        elif stage == 2:
            arrived(c, S_CORE + 1, S_ONE)
            a, b = spot(1 - here, True)

            def body(zz):
                acc[zz, a, b, rows, :] = both_cores(zz, 1 - here, True) + got_one[zz, 1 - here, rows, :]

            over_z(body)
            for d in (1, 2, 3, 0):
                zz = lax.rem(z + d, 4)
                start(c, S_TWO + (d == 0), acc.at[zz, a, b, rows, :], got_two.at[zz, rows, :], two_peer)
        elif stage == 3:
            arrived(c, S_ONE + 1, S_TWO)
            for d in (2, 3, 1):
                zz = lax.rem(z + d, 4)
                acc[zz, y, x, rows, :] = (
                    both_cores(zz, here, True) + got_one[zz, here, rows, :] + got_two[zz, rows, :])
                start(c, S_Z, acc.at[zz, y, x, rows, :], got_z.at[d - 1, rows, :], line(d))
        elif stage == 4:
            arrived(c, S_TWO + 1, S_Z)
            mean = both_cores(z, here, True) + got_one[z, here, rows, :] + got_two[z, rows, :]
            mean = (mean + got_z[0, rows, :] + got_z[1, rows, :] + got_z[2, rows, :]) * (1.0 / N_DEV)
            grad[rows, :] = mean
            own = w_own[rows, :]
            g_sum = jnp.sum(mean * mean, axis=1, keepdims=True)
            w_sum = jnp.sum(own * own, axis=1, keepdims=True)
            row = lax.broadcasted_iota(jnp.int32, (size, LANES), 0) + at
            lane = lax.broadcasted_iota(jnp.int32, (size, LANES), 1)
            tensor = jnp.where(lane < 64, lane, lane - 64)
            member = member_rows(row, tensor)
            part = jnp.where(member, jnp.where(lane < 64, g_sum, w_sum), 0.0)
            here8 = lax.rem(rank, 8)
            layer_norms[c, here8] = jnp.sum(part, axis=0, keepdims=True)
            row8 = layer_norms.at[c, here8]
            for d in range(1, 8):
                tell(2 * c, row8, layer(d))
        elif stage == 5:
            told(2 * c, n_recv)
            norms[c, z] = jnp.sum(layer_norms[c], axis=0)
            for d in range(1, 4):
                tell(2 * c + 1, norms.at[c, z], line(d))
        elif stage == 6:
            told(2 * c + 1, n_recv)
            total = jnp.sum(norms[c], axis=0)
            g_norm = jnp.sqrt(total)
            w_norm = pltpu.roll(g_norm, 64, 1)
            trust = jnp.where((w_norm > 0) & (g_norm > 0), TRUST_COEF * w_norm / (g_norm + DECAY * w_norm), 1.0)
            row = lax.broadcasted_iota(jnp.int32, (size, LANES), 0) + at
            lane = lax.broadcasted_iota(jnp.int32, (size, LANES), 1)
            trust = jnp.where(lane == ID_PLAIN, 1.0, trust)
            member = member_rows(row, lane) & (lane <= ID_PLAIN)
            rate = lr[0] * jnp.sum(jnp.where(member, trust, 0.0), axis=1, keepdims=True)
            decay = jnp.where(row < BN, DECAY, 0.0)
            own = w_own[rows, :]
            moment = MOMENTUM * v_own[rows, :] + rate * (grad[rows, :] + decay * own)
            v_new[rows, :] = moment
            keep(v_new.at[rows, :], v_out_rows.at[rows, :])
            mine = (row != BIAS) | ((lane >= 4 * rank) & (lane < 4 * rank + 4))
            full[z, y, x, core, rows, :] = jnp.where(mine, own - moment, 0.0)
            piece = full.at[z, y, x, core, rows, :]
            for d in (2, 3, 1):
                start(c, A_Z, piece, piece, line(d))
            start(c, A_TWO, piece, piece, two_peer)
        elif stage == 7:
            arrived(c, A_Z)
            for d in (1, 2, 3):
                piece = full.at[lax.rem(z + d, 4), y, x, core, rows, :]
                start(c, A_TWO + 1, piece, piece, two_peer)
            column = full.at[:, y, x, core, rows, :]
            start(c, A_ONE, column, column, one_peer)
        elif stage == 8:
            arrived(c, A_TWO, A_TWO + 1)
            a, b = spot(1 - here, True)
            column = full.at[:, a, b, core, rows, :]
            start(c, A_ONE + 1, column, column, one_peer)
            plane = block(full, True, core, rows)
            start(c, A_CORE, plane, plane, core_peer)
        elif stage == 9:
            arrived(c, A_ONE, A_ONE + 1)
            plane = block(full, False, core, rows)
            start(c, A_CORE + 1, plane, plane, core_peer)
        else:
            arrived(c, A_CORE, A_CORE + 1)
            keep(full.at[:, :, :, :, rows, :], full_out.at[:, :, :, :, rows, :])

    for c, stage in STEPS:
        if stage == 3 and not any(k == S_Z for _, k in sent):
            own_pieces()
        step(c, stage)
    for c, k in sent:
        wait(c, k, send)
    for k in range(2 * len(CHUNKS)):
        told(k, n_send)
    for copy in outs:
        copy.wait()


def exchange(operands):
    any_ = pl.BlockSpec(memory_space=pl.ANY)
    count = len(CHUNKS)
    bf = jnp.bfloat16
    shapes = [(N_MID, 576, 64), (N_IN, 64, 256), (64, 128), (2, N_OUT, 64, 128), (2, 128, 128), (112, 128)]
    own = [(N_MID, 24, 64), (N_IN, 64, 128), (64, 128), (2, N_OUT, 8, 128), (2, 8, 128), (CLASSES, 128), (112, 128),
           (CLASSES,), (128, 128), (N_MID, 1152), (N_IN, 512), (2, LANES), (N_OUT, 512), (8, LANES), (800,), (448,), (4,)]
    rows = (ROWS, LANES)
    exchanged = [(4, 2, 2) + rows, (4, 2, 2) + rows, (4, 2) + rows, (4,) + rows, (3,) + rows, rows,
                 (count, 8, 1, LANES), (count, 4, 1, LANES)]
    dma = pltpu.SemaphoreType.DMA
    full, v_new = pl.pallas_call(
        exchange_kernel,
        out_shape=(jax.ShapeDtypeStruct((4, 2, 2, 2) + rows, F32), jax.ShapeDtypeStruct(rows, F32)),
        in_specs=[pl.BlockSpec(memory_space=pltpu.SMEM)] + [any_] * 24,
        out_specs=(any_, any_),
        scratch_shapes=[VMEM(s, F32) for s in shapes]
        + [VMEM((1024, 256), bf), VMEM((CLASSES, 1024), bf), VMEM((256, 128), F32), VMEM((128, 256), F32)]
        + [VMEM(s, F32) for s in own]
        + [VMEM((4, 2, 2, 2) + rows, F32), VMEM(rows, F32), VMEM(rows, F32), VMEM(rows, F32),
           VMEM((4, 2, 2, 2) + rows, F32)]
        + [VMEM(s, F32) for s in exchanged]
        + [dma((40,)), dma((2 * count,)), dma((count * N_SEMS,)), dma((count * N_SEMS,)), dma((2 * count,)), dma((2 * count,))],
        compiler_params=pltpu.CompilerParams(vmem_limit_bytes=VMEM_LIMIT, collective_id=0, has_side_effects=True),
    )(*operands)
    return full.reshape(N_DEV, ROWS, LANES), v_new


def unpack_kernel(packed_rows, v_rows, n_mid, n_in, n_in0, n_out, n_short, n_fc, n_bn, n_bias,
                  b_mid, b_in, b_in0, b_out, b_short, b_fc, v_mid, v_in, v_in0, v_out, v_short, v_fc, v_bn, v_bias,
                  packed, v_own, s_mid, s_in, s_out, s_short, s_in0, s_fc, t_mid, t_in, t_out, t_short, t_in0, t_fc, xt, sems):
    bf = jnp.bfloat16
    lane_row = lax.broadcasted_iota(jnp.int32, (1, LANES), 1)
    pieces = packed.reshape(N_DEV, ROWS, LANES)
    fetches = []
    for k, (at, size) in enumerate(((0, 40), (40, 120), (160, 24), (184, 48), (232, 72), (304, 24))):
        fetches.append(pltpu.make_async_copy(packed_rows.at[:, pl.ds(at, size), :], pieces.at[:, pl.ds(at, size), :],
                                             sems.at[12 + k]))
    fetches.append(pltpu.make_async_copy(v_rows, v_own, sems.at[18]))
    for copy in fetches:
        copy.start()

    def put(src, dst, k):
        pltpu.make_async_copy(src, dst, sems.at[k]).start()

    def mid_body(t, carry):
        for a in range(4):
            for k in range(9):
                x = packed[across(a, mid_row(t) + k), :]
                s_mid[t, pl.ds(144 * a + 2 * k, 8, stride=18), :] = x[:, :64]
                s_mid[t, pl.ds(144 * a + 2 * k + 1, 8, stride=18), :] = x[:, 64:]
        put(s_mid.at[t], n_mid.at[t], 0)
        t_mid[t] = s_mid[t].astype(bf)
        put(t_mid.at[t], b_mid.at[t], 1)
        return carry

    fetches[0].wait()
    lax.fori_loop(0, 4, mid_body, 0)
    fetches[1].wait()
    lax.fori_loop(4, 16, mid_body, 0)
    fetches[2].wait()
    lax.fori_loop(16, N_MID, mid_body, 0)
    fetches[3].wait()

    def in_pair(first, second, row, other):
        for a in range(4):
            for k in range(4):
                x = packed[across(a, row + k), :]
                y = packed[across(a, other + k), :]
                xt[pl.ds(64 * a + 2 * k, 8, stride=8), :] = left(x, y)
                xt[pl.ds(64 * a + 2 * k + 1, 8, stride=8), :] = right(x, y)
        for h in range(2):
            cols = xt[128 * h:128 * h + 128, :].T
            for u, t in enumerate((first, second)):
                s_in[t, :, 128 * h:128 * h + 128] = cols[64 * u:64 * u + 64]
                t_in[t, :, 128 * h:128 * h + 128] = cols[64 * u:64 * u + 64].astype(bf)
        for t in (first, second):
            put(s_in.at[t], n_in.at[t], 2)
            put(t_in.at[t], b_in.at[t], 3)

    def in_body(j, carry):
        in_pair(2 * j + 5, 2 * j + 6, 184 + 8 * j, 188 + 8 * j)
        return carry

    lax.fori_loop(0, 6, in_body, 0)
    in_pair(0, 1, in_row(0), in_row(1))
    in_pair(2, 3, in_row(2), in_row(3))
    for a in range(4):
        for k in range(4):
            x = packed[across(a, in_row(4) + k), :]
            xt[pl.ds(64 * a + 2 * k, 8, stride=8), :] = x
            xt[pl.ds(64 * a + 2 * k + 1, 8, stride=8), :] = right(x, x)
    for h in range(2):
        cols = xt[128 * h:128 * h + 128, :].T
        s_in[4, :, 128 * h:128 * h + 128] = cols[:64]
        t_in[4, :, 128 * h:128 * h + 128] = cols[:64].astype(bf)
    put(s_in.at[4], n_in.at[4], 2)
    put(t_in.at[4], b_in.at[4], 3)
    for a in range(4):
        for k in range(2):
            x = packed[across(a, IN0 + k), :]
            xt[pl.ds(32 * a + 2 * k, 8, stride=4), :] = x
            xt[pl.ds(32 * a + 2 * k + 1, 8, stride=4), :] = right(x, x)
    cols = xt[0:128, :].T
    s_in0[...] = cols[:64]
    t_in0[...] = cols[:64].astype(bf)
    put(s_in0, n_in0, 4)
    put(t_in0, b_in0, 5)

    def out_body(t, carry):
        for a in range(4):
            for p in range(2):
                for h in range(2):
                    s_out[h, t, pl.ds(16 * a + p, 8, stride=2), :] = packed[across(a, OUT + 4 * t + 2 * p + h), :]
        for h in range(2):
            t_out[h, t] = s_out[h, t].astype(bf)
            put(s_out.at[h, t], n_out.at[t, :, pl.ds(128 * h, 128)], 6)
            put(t_out.at[h, t], b_out.at[t, :, pl.ds(128 * h, 128)], 7)
        return carry

    fetches[4].wait()
    lax.fori_loop(0, N_OUT, out_body, 0)
    fetches[5].wait()
    for h in range(2):
        for a in range(4):
            for p in range(4):
                s_short[h, pl.ds(32 * a + p, 8, stride=4), :] = packed[across(a, SHORT + 2 * p + h), :]
        t_short[h] = s_short[h].astype(bf)
        put(s_short.at[h], n_short.at[:, pl.ds(128 * h, 128)], 8)
        put(t_short.at[h], b_short.at[:, pl.ds(128 * h, 128)], 9)
    for i in range(N_DEV):
        xt[8 * i:8 * i + 8, :] = packed[i * ROWS + FC:i * ROWS + FC + 8, :]
    for h in range(2):
        cols = xt[128 * h:128 * h + 128, :].T
        s_fc[:, 128 * h:128 * h + 128] = cols[:CLASSES]
        t_fc[:, 128 * h:128 * h + 128] = cols[:CLASSES].astype(bf)
    put(s_fc, n_fc, 10)
    put(t_fc, b_fc, 11)

    lane = lax.broadcasted_iota(jnp.int32, (8, LANES), 1)
    for b in range(2):
        def even(k):
            return packed[pl.ds(16 * b * ROWS + BN + k, 8, stride=2 * ROWS), :]

        def odd(k):
            return packed[pl.ds((16 * b + 1) * ROWS + BN + k, 8, stride=2 * ROWS), :]

        for k in range(3):
            n_bn[pl.ds(56 * b + k, 8, stride=7), :] = even(k)
            n_bn[pl.ds(56 * b + 4 + k, 8, stride=7), :] = odd(1 + k)
        n_bn[pl.ds(56 * b + 3, 8, stride=7), :] = jnp.where(lane < 64, even(3), odd(0))
    total = packed[across(0, BIAS), :]
    for a in range(1, 4):
        total = total + packed[across(a, BIAS), :]
    n_bias[...] = jnp.sum(total, axis=0, keepdims=True)[0, :CLASSES]
    fetches[6].wait()

    for rows, tile, ref, tensors in momentum_rows(v_mid, v_in, v_out):
        ref[tensors, tile] = v_own[rows, :]
    rank = lax.axis_index('dp')
    v_in0[...] = v_own[IN0:IN0 + 2, :]
    v_short[...] = v_own[SHORT:SHORT + 8, :]
    for q in range(7):
        flat = jnp.zeros((1, LANES), F32)
        for r in range(8):
            d = CLASSES * r - LANES * q
            if -CLASSES < d < LANES:
                row = pltpu.roll(v_own[FC + r:FC + r + 1, :], d % LANES, 1)
                flat = jnp.where((lane_row >= d) & (lane_row < d + CLASSES), row, flat)
        size = min(LANES, 800 - LANES * q)
        v_fc[pl.ds(LANES * q, size)] = flat[0, :size]
    odd = lax.rem(rank, 2) == 1
    for k in range(4):
        here = v_own[BN + k:BN + k + 1, :]
        after = v_own[BN + k + 1:BN + k + 2, :]
        moved = jnp.where(lane_row < 64, pltpu.roll(here, 64, 1), pltpu.roll(after, 64, 1))
        size = min(LANES, 448 - LANES * k)
        v_bn[pl.ds(LANES * k, size)] = jnp.where(odd, moved, here)[0, :size]
    v_bias[...] = pltpu.roll(v_own[BIAS:BIAS + 1, :], lax.rem(N_DEV - rank, N_DEV) * 4, 1)[0, :4]

    for k, (src, dst) in enumerate(((s_mid, n_mid), (t_mid, b_mid), (s_in, n_in), (t_in, b_in), (s_in0, n_in0),
                                    (t_in0, b_in0))):
        pltpu.make_async_copy(src, dst, sems.at[k]).wait()
    for h in range(2):
        half = pl.ds(128 * h, 128)
        for k, (src, dst) in enumerate(((s_out, n_out.at[:, :, half]), (t_out, b_out.at[:, :, half]),
                                        (s_short, n_short.at[:, half]), (t_short, b_short.at[:, half]))):
            pltpu.make_async_copy(src.at[h], dst, sems.at[6 + k]).wait()
    pltpu.make_async_copy(s_fc, n_fc, sems.at[10]).wait()
    pltpu.make_async_copy(t_fc, b_fc, sems.at[11]).wait()


def unpack_weights(packed, v_own):
    any_ = pl.BlockSpec(memory_space=pl.ANY)
    vm = pl.BlockSpec(memory_space=VMEM)
    bf = jnp.bfloat16
    kernels = ((N_MID, 576, 64), (N_IN, 64, 256), (64, 128), (N_OUT, 64, 256), (128, 256), (CLASSES, 256))
    shapes = [(s, F32) for s in kernels] + [((112, 128), F32), ((CLASSES,), F32)] + [(s, bf) for s in kernels]
    shapes += [(s, F32) for s in ((N_MID, 1152), (N_IN, 512), (2, LANES), (N_OUT, 512), (8, LANES), (800,), (448,), (4,))]
    scratch = ((N_MID, 576, 64), (N_IN, 64, 256), (2, N_OUT, 64, 128), (2, 128, 128), (64, 128), (CLASSES, 256))
    return pl.pallas_call(
        unpack_kernel,
        out_shape=[jax.ShapeDtypeStruct(s, d) for s, d in shapes],
        in_specs=[any_, any_],
        out_specs=[any_] * 6 + [vm] * 2 + [any_] * 6 + [vm] * 8,
        scratch_shapes=[VMEM((N_DEV * ROWS, LANES), F32), VMEM((ROWS, LANES), F32)] + [VMEM(s, F32) for s in scratch] + [VMEM(s, bf) for s in scratch]
        + [VMEM((256, 128), F32), pltpu.SemaphoreType.DMA((19,))],
        compiler_params=pltpu.CompilerParams(vmem_limit_bytes=VMEM_LIMIT),
    )(packed, v_own)


def solution(mesh):
    spec_full = P()
    spec_lead = P('dp')
    spec_cols = P(None, 'dp')
    moment_specs = (spec_lead, spec_lead, spec_cols, spec_cols, spec_cols, spec_lead, spec_lead, spec_lead)
    in_specs = (spec_full,) * 8 + (spec_lead,) * 8 + moment_specs + (spec_full,)
    out_specs = (spec_full,) * 14 + moment_specs

    def body(w_in0, w_short, w_in, w_mid, w_out, w_fc, w_bn, w_bias,
             g_in0, g_short, g_in, g_mid, g_out, g_bn, pooled, dlogits,
             v_in0, v_short, v_in, v_mid, v_out, v_fc, v_bn, v_bias, learn_rate):
        gathered, v_next = exchange((
            learn_rate.reshape(1), g_mid.reshape(N_MID, 576, 64), jnp.swapaxes(g_in[0], 1, 2), g_in0[0].T, g_out[0],
            g_short[0], g_bn.reshape(112, LANES), pooled, dlogits.T,
            w_mid.reshape(N_MID, 576, 64), jnp.swapaxes(w_in, 1, 2), w_in0.T, w_out, w_short, w_fc.T,
            w_bn.reshape(112, LANES), w_bias, v_mid, v_in, v_in0.reshape(2, LANES), v_out, v_short.reshape(8, LANES),
            v_fc, v_bn, v_bias))
        (n_mid, n_in, n_in0, n_out, n_short, n_fc, n_bn, n_bias, b_mid, b_in, b_in0, b_out, b_short, b_fc,
         m_mid, m_in, m_in0, m_out, m_short, m_fc, m_bn, m_bias) = unpack_weights(gathered, v_next)
        return (n_in0.T, n_short, jnp.swapaxes(n_in, 1, 2), n_mid.reshape(w_mid.shape), n_out, n_fc.T,
                n_bn.reshape(-1), n_bias,
                b_in0.T, b_short, jnp.swapaxes(b_in, 1, 2), b_mid.reshape(w_mid.shape), b_out, b_fc.T,
                m_in0.reshape(-1), m_short.reshape(-1), m_in, m_mid, m_out, m_fc, m_bn, m_bias)

    return jax.shard_map(body, mesh=mesh, in_specs=in_specs, out_specs=out_specs, check_vma=False)
```

```python
import jax
import jax.numpy as jnp
from jax import lax
from jax.experimental import pallas as pl
from jax.experimental.pallas import tpu as pltpu
from jax.sharding import PartitionSpec as P

MOMENTUM = 0.9
TRUST_COEF = 0.001
DECAY = 0.0001
N_DEV = 32
LANES = 128
IN0, OUT, SHORT, FC, BN, BIAS, ROWS = 178, 232, 304, 312, 320, 324, 328
N_MID, N_IN, N_OUT = 18, 17, 18
CLASSES = 100
ID_IN0, ID_IN, ID_OUT, ID_SHORT, ID_FC, ID_PLAIN = 18, 19, 36, 54, 55, 56
F32 = jnp.float32
VMEM = pltpu.VMEM
MESH = pl.DeviceIdType.MESH
CHUNKS = (
    (0, 40, 'x'), (40, 40, 'y'), (80, 40, 'x'), (120, 40, 'y'), (160, 24, 'y'),
    (184, 24, 'x'), (208, 24, 'zx'), (232, 24, 'y'), (256, 24, 'x'), (280, 24, 'zx'),
    (304, 24, 'y'),
)
STEPS = (
    (1, 0), (8, 0), (9, 0), (7, 0), (1, 1), (8, 1), (2, 0), (9, 1), (6, 0), (2, 1), (4, 0), (8, 2), (1, 2), (6, 1),
    (7, 1), (3, 0), (0, 0), (2, 2), (0, 1), (3, 1), (8, 3), (7, 2), (1, 3), (10, 0), (2, 3), (0, 2), (9, 2), (5, 0),
    (3, 2), (4, 1), (7, 3), (8, 4), (10, 1), (5, 1), (0, 3), (1, 4), (9, 3), (3, 3), (4, 2), (2, 4), (5, 2), (6, 2),
    (7, 4), (8, 5), (10, 2), (4, 3), (9, 4), (6, 3), (1, 5), (5, 3), (0, 4), (2, 5), (10, 3), (3, 4), (8, 6), (7, 5),
    (6, 4), (9, 5), (1, 6), (4, 4), (0, 5), (5, 4), (3, 5), (2, 6), (10, 4), (7, 6), (9, 6), (6, 5), (8, 7), (5, 5),
    (4, 5), (1, 7), (0, 6), (9, 7), (10, 5), (3, 6), (2, 7), (7, 7), (4, 6), (6, 6), (1, 8), (8, 8), (5, 6), (2, 8),
    (10, 6), (9, 8), (7, 8), (6, 7), (3, 7), (0, 7), (4, 7), (2, 9), (10, 7), (6, 8), (5, 7), (3, 8), (0, 8), (8, 9),
    (4, 8), (7, 9), (9, 9), (2, 10), (5, 8), (1, 9), (10, 8), (1, 10), (3, 9), (0, 9), (3, 10), (4, 9), (9, 10),
    (5, 9), (6, 9), (7, 10), (8, 10), (10, 9), (5, 10), (6, 10), (0, 10), (4, 10), (10, 10),
)
FIRST_NORMS = [step for step in STEPS if step[1] == 4][0]
S_CORE, S_ONE, S_TWO, S_Z, A_Z, A_TWO, A_ONE, A_CORE, N_SEMS = 0, 2, 4, 6, 7, 8, 10, 12, 14
VMEM_LIMIT = 60 * 2**20


def mid_row(t):
    return 40 * (t // 4) + 9 * (t % 4)


def in_row(t):
    return 36 + 40 * t if t < 4 else 164 + 4 * t


def member_rows(row, t):
    first = 9 * t
    for group in (4, 8, 12, 16):
        first = jnp.where(t >= group, first + 4, first)
    size = jnp.where(t < N_MID, 9, jnp.where(t == ID_IN0, 2, jnp.where(t < ID_SHORT, 4, 8)))
    first = jnp.where(t >= ID_IN0, IN0, first)
    first = jnp.where(t >= ID_IN, 36 + 40 * (t - ID_IN), first)
    first = jnp.where(t >= ID_IN + 4, 164 + 4 * (t - ID_IN), first)
    first = jnp.where(t >= ID_OUT, OUT + 4 * (t - ID_OUT), first)
    first = jnp.where(t >= ID_SHORT, SHORT + 8 * (t - ID_SHORT), first)
    return (row >= first) & (row < first + size)


def momentum_rows(mid, inn, out):
    runs = [(mid, mid_row(t), 9, t, min(4, N_MID - t)) for t in range(0, N_MID, 4)]
    runs += [(inn, 36, 40, 0, 4)] + [(inn, 164 + 4 * t, 4, t, min(8, N_IN - t)) for t in (4, 12)]
    runs += [(out, OUT + 4 * t, 4, t, min(8, N_OUT - t)) for t in (0, 8, 16)]
    for ref, base, stride, t, count in runs:
        for m in range(9 if ref is mid else 4):
            yield pl.ds(base + m, count, stride=stride), pl.ds(128 * m, 128), ref, pl.ds(t, count)


def left(a, b):
    return jnp.concatenate([a[:, :64], b[:, :64]], axis=1)


def right(a, b):
    return jnp.concatenate([a[:, 64:], b[:, 64:]], axis=1)


def across(piece8, row):
    return pl.ds(piece8 * 8 * ROWS + row, 8, stride=ROWS)


def exchange_kernel(lr, g_mid, g_in, g_in0, g_out, g_short, g_bn, pooled, dlog_t,
                    w_mid, w_in, w_in0, w_out, w_short, w_fc, w_bn, w_bias,
                    v_mid, v_in, v_in0, v_out, v_short, v_fc, v_bn, v_bias,
                    full_out, v_out_rows,
                    s_mid, s_in, s_in0, s_out, s_short, s_bn, s_x, s_d, xt, fct,
                    o_mid, o_in, o_in0, o_out, o_short, o_fc, o_bn, o_bias, ot,
                    p_mid, p_in, p_in0, p_out, p_short, p_fc, p_bn, p_bias,
                    packed, w_own, v_own, v_new, full,
                    got_core, acc, got_one, got_two, got_z, got_line, grad, layer_norms, norms,
                    sems, out_sems, send, recv, n_send, n_recv):
    rank = lax.axis_index('dp')
    core = lax.rem(rank, 2)
    x = lax.rem(rank // 2, 2)
    y = lax.rem(rank // 4, 2)
    z = rank // 8

    def device(zz, yy, xx, cc):
        return (((zz * 2 + yy) * 2 + xx) * 2 + cc,)

    core_peer = device(z, y, x, 1 - core)
    x_peer = device(z, y, 1 - x, core)
    y_peer = device(z, 1 - y, x, core)

    barrier = pltpu.get_barrier_semaphore()

    def layer(d):
        return (z * 8 + lax.rem(rank + d, 8),)

    def line(d):
        return (lax.rem(rank + 8 * d, N_DEV),)

    for d in range(1, 8):
        pl.semaphore_signal(barrier, inc=1, device_id=layer(d), device_id_type=MESH)
    for d in range(1, 4):
        pl.semaphore_signal(barrier, inc=1, device_id=line(d), device_id_type=MESH)

    waiting = {}
    count = [0]

    def fetch(name, src, dst):
        copy = pltpu.make_async_copy(src, dst, sems.at[count[0]])
        count[0] += 1
        copy.start()
        waiting.setdefault(name, []).append(copy)

    def need(*names):
        for name in names:
            for copy in waiting.pop(name, []):
                copy.wait()

    def halves(name, src, dst):
        for h in range(2):
            fetch(name, src(pl.ds(128 * h, 128)), dst.at[h])

    fetchers = {
        'in': lambda: fetch('in', g_in.at[pl.ds(5, 12)], s_in.at[pl.ds(5, 12)]),
        'in1': lambda: fetch('in1', g_in.at[pl.ds(0, 5)], s_in.at[pl.ds(0, 5)]),
        'in0': lambda: fetch('in0', g_in0, s_in0),
        'out': lambda: halves('out', lambda c: g_out.at[:, :, c], s_out),
        'short': lambda: halves('short', lambda c: g_short.at[:, c], s_short),
        'fc': lambda: (fetch('fc', pooled, s_x), fetch('fc', dlog_t, s_d)),
        'bn': lambda: fetch('bn', g_bn, s_bn),
    }
    for i in range(5):
        part = pl.ds(4 * i, min(4, N_MID - 4 * i))
        fetchers['mid%d' % i] = lambda i=i, part=part: fetch('mid%d' % i, g_mid.at[part], s_mid.at[part])
    units = [(40 * i, 40 * i + 40, ('mid%d' % i, 'in1')) for i in range(4)] + [(160, 184, ('mid4', 'in0', 'in1'))]
    units += [(184 + 8 * j, 192 + 8 * j, ('in',)) for j in range(6)]
    units += [(232 + 8 * j, 240 + 8 * j, ('out',)) for j in range(9)]
    units += [(304, 312, ('short',)), (312, 320, ('fc',)), (320, 328, ('bn', 'fc'))]
    for at, size, _ in CHUNKS:
        for lo, hi, names in units:
            if at <= lo < at + size:
                for name in names:
                    if name in fetchers:
                        fetchers.pop(name)()

    mid_at = pl.multiple_of((18 * rank) // 8 * 8, 8)
    mid_off = lax.rem(18 * rank, 8)
    out_at = pl.multiple_of((2 * rank) // 8 * 8, 8)
    out_off = 2 * lax.rem(rank, 4)
    short_at = pl.multiple_of((4 * rank) // 8 * 8, 8)
    short_off = 4 * lax.rem(rank, 2)
    col_at = pl.multiple_of((rank // 16) * 128, 128)
    col_off = pl.multiple_of(lax.rem(rank, 16) * 8, 8)
    fetch('own', w_mid.at[:, pl.ds(mid_at, 24), :], o_mid)
    fetch('own', w_in.at[:, :, pl.ds(col_at, 128)], o_in)
    fetch('own', w_in0, o_in0)
    halves('own', lambda c: w_out.at[:, pl.ds(out_at, 8), c], o_out)
    halves('own', lambda c: w_short.at[pl.ds(short_at, 8), c], o_short)
    fetch('own', w_fc.at[:, pl.ds(col_at, 128)], o_fc)
    fetch('own', w_bn, o_bn)
    fetch('own', w_bias, o_bias)
    for src, dst in ((v_mid, p_mid), (v_in, p_in), (v_in0, p_in0), (v_out, p_out), (v_short, p_short), (v_fc, p_fc),
                     (v_bn, p_bn), (v_bias, p_bias)):
        fetch('own', src, dst)

    pieces = packed.reshape(N_DEV * ROWS, LANES)

    def pack_mid(base, first, count):
        def body(u, carry):
            t = first + u
            for a in range(4):
                for k in range(9):
                    even = s_mid[t, pl.ds(144 * a + 2 * k, 8, stride=18), :]
                    odd = s_mid[t, pl.ds(144 * a + 2 * k + 1, 8, stride=18), :]
                    pieces[across(a, base + 9 * u + k), :] = jnp.concatenate([even, odd], axis=1)
            return carry

        lax.fori_loop(0, count, body, 0)

    def pack_in_rows(base, pair):
        for a in range(4):
            for k in range(4):
                even = xt[pl.ds(64 * a + 2 * k, 8, stride=8), :]
                odd = xt[pl.ds(64 * a + 2 * k + 1, 8, stride=8), :]
                pieces[across(a, base + k), :] = left(even, odd)
                if pair:
                    pieces[across(a, base + 4 + k), :] = right(even, odd)

    def transpose(a, b):
        both = jnp.concatenate([a, b], axis=0)
        for h in range(2):
            xt[128 * h:128 * h + 128, :] = both[:, 128 * h:128 * h + 128].T

    def pack_in(first, last):
        def body(j, carry):
            transpose(s_in[2 * j + 5], s_in[2 * j + 6])
            pack_in_rows(184 + 8 * j, True)
            return carry

        lax.fori_loop(first, last, body, 0)

    def pack_in_one(t):
        wide = jnp.concatenate([s_in0[...], s_in0[...]], axis=1) if t == 4 else s_in[t]
        transpose(s_in[t], wide)
        pack_in_rows(in_row(t), False)
        if t == 4:
            for a in range(4):
                for k in range(2):
                    even = xt[pl.ds(32 * a + 2 * k, 8, stride=4), :]
                    odd = xt[pl.ds(32 * a + 2 * k + 1, 8, stride=4), :]
                    pieces[across(a, IN0 + k), :] = right(even, odd)

    def pack_out(first, last):
        def body(t, carry):
            for a in range(4):
                for p in range(2):
                    for h in range(2):
                        pieces[across(a, OUT + 4 * t + 2 * p + h), :] = s_out[h, t, pl.ds(16 * a + p, 8, stride=2), :]
            return carry

        lax.fori_loop(first, last, body, 0)

    def pack_short():
        for a in range(4):
            for p in range(4):
                for h in range(2):
                    pieces[across(a, SHORT + 2 * p + h), :] = s_short[h, pl.ds(32 * a + p, 8, stride=4), :]

    scale = 1.0 / pooled.shape[0]

    def pack_fc():
        fct[CLASSES:LANES, :] = jnp.zeros((LANES - CLASSES, 256), F32)
        fct[0:CLASSES, :] = jnp.dot(s_d[...], s_x[...], preferred_element_type=F32) * scale
        for h in range(2):
            cols = fct[:, 128 * h:128 * h + 128].T
            for j in range(16):
                at = (16 * h + j) * ROWS + FC
                pieces[at:at + 8, :] = cols[8 * j:8 * j + 8, :]

    def pack_bn():
        def clear(i, carry):
            pieces[pl.ds(pl.multiple_of(i * ROWS + BN, 8), 8), :] = jnp.zeros((8, LANES), F32)
            return carry

        lax.fori_loop(0, N_DEV, clear, 0)
        for b in range(2):
            for k in range(4):
                for half in range(2):
                    pieces[pl.ds((16 * b + half) * ROWS + BN + k, 8, stride=2 * ROWS), :] = (
                        s_bn[pl.ds(56 * b + 3 * half + k, 8, stride=7), :])
        bias = lax.dot_general(jnp.ones((8, s_d.shape[1]), jnp.bfloat16), s_d[...], (((1,), (1,)), ((), ())),
                               preferred_element_type=F32) * scale
        bias = jnp.concatenate([bias, jnp.zeros((8, LANES - CLASSES), F32)], axis=1)
        for a in range(4):
            pieces[across(a, BIAS), :] = bias

    def pack(at, size):
        end = at + size
        for lo, hi, names in units:
            if at <= lo < end:
                need(*names)
        for i in range(5):
            if at <= 40 * i < end:
                pack_mid(40 * i, 4 * i, min(4, N_MID - 4 * i))
                pack_in_one(i)
        lo, hi = max(at, 184), min(end, 232)
        if lo < hi:
            pack_in((lo - 184) // 8, (hi - 184) // 8)
        lo, hi = max(at, OUT), min(end, SHORT)
        if lo < hi:
            pack_out((lo - OUT) // 4, (hi - OUT) // 4)
        if at <= SHORT < end:
            pack_short()
        if at <= FC < end:
            pack_fc()
        if at <= BN < end:
            pack_bn()

    lane_row = lax.broadcasted_iota(jnp.int32, (1, LANES), 1)

    def own_pieces():
        need('own')
        for rows, tile, ref, tensors in momentum_rows(p_mid, p_in, p_out):
            v_own[rows, :] = ref[tensors, tile]
        v_own[IN0:IN0 + 2, :] = p_in0[...]
        v_own[SHORT:SHORT + 8, :] = p_short[...]
        flat = [p_fc[pl.ds(128 * q, 128)].reshape(1, LANES) for q in range(6)]
        flat.append(jnp.concatenate([p_fc[pl.ds(768, 32)].reshape(1, 32), jnp.zeros((1, 96), F32)], axis=1))
        for r in range(8):
            q, s = divmod(CLASSES * r, LANES)
            row = pltpu.roll(flat[q], (LANES - s) % LANES, 1)
            if s + CLASSES > LANES:
                row = jnp.where(lane_row < LANES - s, row, pltpu.roll(flat[q + 1], LANES - s, 1))
            v_own[FC + r:FC + r + 1, :] = jnp.where(lane_row < CLASSES, row, 0.0)
        v_own[BN:ROWS, :] = jnp.zeros((8, LANES), F32)
        odd = lax.rem(rank, 2) == 1
        rows = [p_bn[pl.ds(128 * k, 128)].reshape(1, LANES) for k in range(3)]
        rows.append(jnp.concatenate([p_bn[pl.ds(384, 64)].reshape(1, 64), jnp.zeros((1, 64), F32)], axis=1))
        for k in range(4):
            before = pltpu.roll(rows[k - 1], 64, 1) if k else jnp.zeros((1, LANES), F32)
            moved = jnp.where(lane_row < 64, before, pltpu.roll(rows[k], 64, 1))
            v_own[BN + k:BN + k + 1, :] = jnp.where(odd, moved, rows[k])
        four = jnp.concatenate([p_bias[...].reshape(1, 4), jnp.zeros((1, LANES - 4), F32)], axis=1)
        v_own[BIAS:BIAS + 1, :] = pltpu.roll(four, 4 * rank, 1)

        for t in range(N_MID):
            even = o_mid[t, pl.ds(mid_off, 9, stride=2), :]
            odds = o_mid[t, pl.ds(mid_off + 1, 9, stride=2), :]
            w_own[mid_row(t):mid_row(t) + 9, :] = jnp.concatenate([even, odds], axis=1)
        for j in range(9):
            other = o_in[2 * j - 1] if j else o_in0[...]
            ot[...] = jnp.concatenate([other, o_in[2 * j]], axis=0).T
            if j == 0:
                w_own[IN0:IN0 + 2, :] = left(ot[pl.ds(4 * rank, 2, stride=2), :], ot[pl.ds(4 * rank + 1, 2, stride=2), :])
            even = ot[pl.ds(col_off, 4, stride=2), :]
            odds = ot[pl.ds(col_off + 1, 4, stride=2), :]
            if j:
                w_own[in_row(2 * j - 1):in_row(2 * j - 1) + 4, :] = left(even, odds)
            w_own[in_row(2 * j):in_row(2 * j) + 4, :] = right(even, odds)
        def own_out(t, carry):
            for p in range(2):
                for h in range(2):
                    w_own[pl.ds(OUT + 4 * t + 2 * p + h, 1), :] = o_out[h, t, pl.ds(out_off + p, 1), :]
            return carry

        lax.fori_loop(0, N_OUT, own_out, 0)
        for p in range(4):
            for h in range(2):
                w_own[SHORT + 2 * p + h:SHORT + 2 * p + h + 1, :] = o_short[h, pl.ds(short_off + p, 1), :]
        ot[0:CLASSES, :] = o_fc[...]
        ot[CLASSES:LANES, :] = jnp.zeros((LANES - CLASSES, LANES), F32)
        ot[...] = ot[...].T
        w_own[FC:FC + 8, :] = ot[pl.ds(col_off, 8), :]
        w_own[BN:ROWS, :] = jnp.zeros((8, LANES), F32)
        bn_at = 7 * (rank // 2) + 3 * lax.rem(rank, 2)
        for k in range(4):
            w_own[BN + k:BN + k + 1, :] = o_bn[pl.ds(bn_at + k, 1), :]
        bias = jnp.concatenate([o_bias[...].reshape(1, CLASSES), jnp.zeros((1, LANES - CLASSES), F32)], axis=1)
        w_own[BIAS:BIAS + 1, :] = jnp.where((lane_row >= 4 * rank) & (lane_row < 4 * rank + 4), bias, 0.0)

    outs = []
    sent = {}

    def start(c, k, src, dst, peer):
        pltpu.make_async_remote_copy(src_ref=src, dst_ref=dst, send_sem=send.at[c * N_SEMS + k],
                                     recv_sem=recv.at[c * N_SEMS + k], device_id=peer, device_id_type=MESH).start()
        sent[c, k] = sent.get((c, k), 0) + (1 if len(src.shape) == 2 else src.size // (src.shape[-1] * src.shape[-2]))

    def wait(c, k, semaphores):
        at, size, _ = CHUNKS[c]
        rows = pl.ds(at, size)
        count = sent[c, k]
        lead = {1: (0, 0, 0), 2: (0, 0), 3: (pl.ds(0, 3), 0, 0), 4: (0,), 8: (pl.ds(0, 2),), 12: (pl.ds(0, 3),), 16: ()}[count]
        block = got_core.at[lead + (slice(None),) * (3 - len(lead)) + (rows,)]
        pltpu.make_async_copy(block, block, semaphores.at[c * N_SEMS + k]).wait()

    def arrived(c, *numbers):
        for k in numbers:
            wait(c, k, recv)

    def keep(src, dst):
        copy = pltpu.make_async_copy(src, dst, out_sems.at[len(outs)])
        copy.start()
        outs.append(copy)

    def tell(k, row, peer):
        pltpu.make_async_remote_copy(src_ref=row, dst_ref=row, send_sem=n_send.at[k], recv_sem=n_recv.at[k],
                                     device_id=peer, device_id_type=MESH).start()

    def told(k, semaphores):
        rows = layer_norms.at[k // 2, pl.ds(0, 3 if k % 2 else 7)]
        pltpu.make_async_copy(rows, rows, semaphores.at[k]).wait()

    def step(c, stage):
        at, size, first = CHUNKS[c]
        rows = pl.ds(at, size)
        x_first, z_first = first[-1] == 'x', first[0] == 'z'
        one_peer, two_peer = (x_peer, y_peer) if x_first else (y_peer, x_peer)

        here = y if x_first else x

        def block(ref, near, *rest):
            first_at = (x if near else 1 - x) if x_first else (y if near else 1 - y)
            return ref.at[(slice(None), slice(None), first_at) + rest] if x_first else (
                ref.at[(slice(None), first_at, slice(None)) + rest])

        def spot(second, near):
            return (second, x if near else 1 - x) if x_first else (y if near else 1 - y, second)

        def both_cores(zz, second, near):
            a, b = spot(second, near)
            return packed[zz, a, b, core, rows, :] + got_core[zz, a, b, rows, :]

        def over_z(body):
            def run(zz, carry):
                body(zz)
                return carry

            lax.fori_loop(0, 4, run, 0)

        if stage == 0:
            pack(at, size)
            if not sent:
                pl.semaphore_wait(barrier, 10)
            for k, near in enumerate((False, True)):
                start(c, S_CORE + k, block(packed, near, 1 - core, rows), block(got_core, near, rows), core_peer)
        elif stage == 1 and z_first:
            arrived(c, S_CORE, S_CORE + 1)
            for d in (2, 3, 1, 0):
                zz = lax.rem(z + d, 4)
                acc[zz, :, :, rows, :] = packed[zz, :, :, core, rows, :] + got_core[zz, :, :, rows, :]
                if d:
                    start(c, S_Z, acc.at[zz, :, :, rows, :], got_line.at[d - 1, :, :, rows, :], line(d))
        elif stage == 1:
            arrived(c, S_CORE)
            for k, second in enumerate((1 - here, here)):
                a, b = spot(second, False)

                def body(zz, a=a, b=b, second=second):
                    acc[zz, a, b, rows, :] = both_cores(zz, second, False)

                over_z(body)
                start(c, S_ONE + k, acc.at[:, a, b, rows, :], got_one.at[:, second, rows, :], one_peer)
        elif stage == 2 and z_first:
            arrived(c, S_Z)
            for near in (False, True):
                for second in range(2):
                    a, b = spot(second, near)
                    total = acc[z, a, b, rows, :] + got_line[0, a, b, rows, :]
                    acc[z, a, b, rows, :] = total + got_line[1, a, b, rows, :] + got_line[2, a, b, rows, :]
                if not near:
                    far = acc.at[z, :, 1 - x, rows, :] if x_first else acc.at[z, 1 - y, :, rows, :]
                    start(c, S_ONE, far, got_one.at[0, :, rows, :], one_peer)
        elif stage == 2:
            arrived(c, S_CORE + 1, S_ONE)
            a, b = spot(1 - here, True)

            def body(zz):
                acc[zz, a, b, rows, :] = both_cores(zz, 1 - here, True) + got_one[zz, 1 - here, rows, :]

            over_z(body)
            for d in (1, 2, 3, 0):
                zz = lax.rem(z + d, 4)
                start(c, S_TWO + (d == 0), acc.at[zz, a, b, rows, :], got_two.at[zz, rows, :], two_peer)
        elif stage == 3 and z_first:
            arrived(c, S_ONE)
            a, b = spot(1 - here, True)
            acc[z, a, b, rows, :] = acc[z, a, b, rows, :] + got_one[0, 1 - here, rows, :]
            start(c, S_TWO, acc.at[z, a, b, rows, :], got_two.at[0, rows, :], two_peer)
        elif stage == 3:
            arrived(c, S_ONE + 1, S_TWO)
            for d in (2, 3, 1):
                zz = lax.rem(z + d, 4)
                acc[zz, y, x, rows, :] = (
                    both_cores(zz, here, True) + got_one[zz, here, rows, :] + got_two[zz, rows, :])
                start(c, S_Z, acc.at[zz, y, x, rows, :], got_z.at[d - 1, rows, :], line(d))
        elif stage == 4:
            if z_first:
                arrived(c, S_TWO)
                mean = acc[z, y, x, rows, :] + got_one[0, here, rows, :] + got_two[0, rows, :]
            else:
                arrived(c, S_TWO + 1, S_Z)
                mean = both_cores(z, here, True) + got_one[z, here, rows, :] + got_two[z, rows, :]
                mean = mean + got_z[0, rows, :] + got_z[1, rows, :] + got_z[2, rows, :]
            mean = mean * (1.0 / N_DEV)
            grad[rows, :] = mean
            own = w_own[rows, :]
            g_sum = jnp.sum(mean * mean, axis=1, keepdims=True)
            w_sum = jnp.sum(own * own, axis=1, keepdims=True)
            row = lax.broadcasted_iota(jnp.int32, (size, LANES), 0) + at
            lane = lax.broadcasted_iota(jnp.int32, (size, LANES), 1)
            tensor = jnp.where(lane < 64, lane, lane - 64)
            member = member_rows(row, tensor)
            part = jnp.where(member, jnp.where(lane < 64, g_sum, w_sum), 0.0)
            here8 = lax.rem(rank, 8)
            layer_norms[c, here8] = jnp.sum(part, axis=0, keepdims=True)
            row8 = layer_norms.at[c, here8]
            for d in range(1, 8):
                tell(2 * c, row8, layer(d))
        elif stage == 5:
            told(2 * c, n_recv)
            norms[c, z] = jnp.sum(layer_norms[c], axis=0)
            for d in range(1, 4):
                tell(2 * c + 1, norms.at[c, z], line(d))
        elif stage == 6:
            told(2 * c + 1, n_recv)
            total = jnp.sum(norms[c], axis=0)
            g_norm = jnp.sqrt(total)
            w_norm = pltpu.roll(g_norm, 64, 1)
            trust = jnp.where((w_norm > 0) & (g_norm > 0), TRUST_COEF * w_norm / (g_norm + DECAY * w_norm), 1.0)
            row = lax.broadcasted_iota(jnp.int32, (size, LANES), 0) + at
            lane = lax.broadcasted_iota(jnp.int32, (size, LANES), 1)
            trust = jnp.where(lane == ID_PLAIN, 1.0, trust)
            member = member_rows(row, lane) & (lane <= ID_PLAIN)
            rate = lr[0] * jnp.sum(jnp.where(member, trust, 0.0), axis=1, keepdims=True)
            decay = jnp.where(row < BN, DECAY, 0.0)
            own = w_own[rows, :]
            moment = MOMENTUM * v_own[rows, :] + rate * (grad[rows, :] + decay * own)
            v_new[rows, :] = moment
            keep(v_new.at[rows, :], v_out_rows.at[rows, :])
            mine = (row != BIAS) | ((lane >= 4 * rank) & (lane < 4 * rank + 4))
            full[z, y, x, core, rows, :] = jnp.where(mine, own - moment, 0.0)
            piece = full.at[z, y, x, core, rows, :]
            if not z_first:
                for d in (2, 3, 1):
                    start(c, A_Z, piece, piece, line(d))
            start(c, A_TWO, piece, piece, two_peer)
        elif stage == 7 and z_first:
            arrived(c, A_TWO)
            pair = full.at[z, :, x, core, rows, :] if x_first else full.at[z, y, :, core, rows, :]
            start(c, A_ONE, pair, pair, one_peer)
        elif stage == 8 and z_first:
            arrived(c, A_ONE)
            plane = full.at[z, :, :, core, rows, :]
            for d in (2, 3, 1):
                start(c, A_Z, plane, plane, line(d))
        elif stage == 9 and z_first:
            arrived(c, A_Z)
            everything = full.at[:, :, :, core, rows, :]
            start(c, A_CORE, everything, everything, core_peer)
        elif stage == 10 and z_first:
            arrived(c, A_CORE)
            keep(full.at[:, :, :, :, rows, :], full_out.at[:, :, :, :, rows, :])
        elif stage == 7:
            arrived(c, A_Z)
            for d in (1, 2, 3):
                piece = full.at[lax.rem(z + d, 4), y, x, core, rows, :]
                start(c, A_TWO + 1, piece, piece, two_peer)
            column = full.at[:, y, x, core, rows, :]
            start(c, A_ONE, column, column, one_peer)
        elif stage == 8:
            arrived(c, A_TWO, A_TWO + 1)
            a, b = spot(1 - here, True)
            column = full.at[:, a, b, core, rows, :]
            start(c, A_ONE + 1, column, column, one_peer)
            plane = block(full, True, core, rows)
            start(c, A_CORE, plane, plane, core_peer)
        elif stage == 9:
            arrived(c, A_ONE, A_ONE + 1)
            plane = block(full, False, core, rows)
            start(c, A_CORE + 1, plane, plane, core_peer)
        else:
            arrived(c, A_CORE, A_CORE + 1)
            keep(full.at[:, :, :, :, rows, :], full_out.at[:, :, :, :, rows, :])

    for c, stage in STEPS:
        if stage == 4 and (c, stage) == FIRST_NORMS:
            own_pieces()
        step(c, stage)
    for c, k in sent:
        wait(c, k, send)
    for k in range(2 * len(CHUNKS)):
        told(k, n_send)
    for copy in outs:
        copy.wait()


def exchange(operands):
    any_ = pl.BlockSpec(memory_space=pl.ANY)
    count = len(CHUNKS)
    bf = jnp.bfloat16
    shapes = [(N_MID, 576, 64), (N_IN, 64, 256), (64, 128), (2, N_OUT, 64, 128), (2, 128, 128), (112, 128)]
    own = [(N_MID, 24, 64), (N_IN, 64, 128), (64, 128), (2, N_OUT, 8, 128), (2, 8, 128), (CLASSES, 128), (112, 128),
           (CLASSES,), (128, 128), (N_MID, 1152), (N_IN, 512), (2, LANES), (N_OUT, 512), (8, LANES), (800,), (448,), (4,)]
    rows = (ROWS, LANES)
    exchanged = [(4, 2, 2) + rows, (4, 2, 2) + rows, (4, 2) + rows, (4,) + rows, (3,) + rows, (3, 2, 2) + rows, rows,
                 (count, 8, 1, LANES), (count, 4, 1, LANES)]
    dma = pltpu.SemaphoreType.DMA
    full, v_new = pl.pallas_call(
        exchange_kernel,
        out_shape=(jax.ShapeDtypeStruct((4, 2, 2, 2) + rows, F32), jax.ShapeDtypeStruct(rows, F32)),
        in_specs=[pl.BlockSpec(memory_space=pltpu.SMEM)] + [any_] * 24,
        out_specs=(any_, any_),
        scratch_shapes=[VMEM(s, F32) for s in shapes]
        + [VMEM((1024, 256), bf), VMEM((CLASSES, 1024), bf), VMEM((256, 128), F32), VMEM((128, 256), F32)]
        + [VMEM(s, F32) for s in own]
        + [VMEM((4, 2, 2, 2) + rows, F32), VMEM(rows, F32), VMEM(rows, F32), VMEM(rows, F32),
           VMEM((4, 2, 2, 2) + rows, F32)]
        + [VMEM(s, F32) for s in exchanged]
        + [dma((40,)), dma((2 * count,)), dma((count * N_SEMS,)), dma((count * N_SEMS,)), dma((2 * count,)), dma((2 * count,))],
        compiler_params=pltpu.CompilerParams(vmem_limit_bytes=VMEM_LIMIT, collective_id=0, has_side_effects=True),
    )(*operands)
    return full.reshape(N_DEV, ROWS, LANES), v_new


def unpack_kernel(packed_rows, v_rows, n_mid, n_in, n_in0, n_out, n_short, n_fc, bn_out, bias_out,
                  b_mid, b_in, b_in0, b_out, b_short, b_fc, *rest):
    v_outs, rest = rest[:8], rest[8:]
    n_bn, n_bias = rest[:2]
    (v_mid, v_in, v_in0, v_out, v_short, v_fc, v_bn, v_bias), rest = rest[2:10], rest[10:]
    (packed, v_own, s_mid, s_in, s_out, s_short, s_in0, s_fc, t_mid, t_in, t_out, t_short, t_in0, t_fc, xt, sems) = rest
    bf = jnp.bfloat16
    lane_row = lax.broadcasted_iota(jnp.int32, (1, LANES), 1)
    pieces = packed.reshape(N_DEV, ROWS, LANES)
    fetches = []
    for k, (at, size) in enumerate(((0, 40), (40, 120), (160, 24), (184, 48), (232, 72), (304, 24))):
        fetches.append(pltpu.make_async_copy(packed_rows.at[:, pl.ds(at, size), :], pieces.at[:, pl.ds(at, size), :],
                                             sems.at[12 + k]))
    fetches.append(pltpu.make_async_copy(v_rows, v_own, sems.at[18]))
    for copy in fetches:
        copy.start()

    def put(src, dst, k):
        pltpu.make_async_copy(src, dst, sems.at[k]).start()

    def mid_body(t, carry):
        for a in range(4):
            for k in range(9):
                x = packed[across(a, mid_row(t) + k), :]
                s_mid[t, pl.ds(144 * a + 2 * k, 8, stride=18), :] = x[:, :64]
                s_mid[t, pl.ds(144 * a + 2 * k + 1, 8, stride=18), :] = x[:, 64:]
        put(s_mid.at[t], n_mid.at[t], 0)
        t_mid[t] = s_mid[t].astype(bf)
        put(t_mid.at[t], b_mid.at[t], 1)
        return carry

    fetches[0].wait()
    lax.fori_loop(0, 4, mid_body, 0)
    fetches[6].wait()
    for rows, tile, ref, tensors in momentum_rows(v_mid, v_in, v_out):
        ref[tensors, tile] = v_own[rows, :]
    rank = lax.axis_index('dp')
    v_in0[...] = v_own[IN0:IN0 + 2, :]
    v_short[...] = v_own[SHORT:SHORT + 8, :]
    for q in range(7):
        flat = jnp.zeros((1, LANES), F32)
        for r in range(8):
            d = CLASSES * r - LANES * q
            if -CLASSES < d < LANES:
                row = pltpu.roll(v_own[FC + r:FC + r + 1, :], d % LANES, 1)
                flat = jnp.where((lane_row >= d) & (lane_row < d + CLASSES), row, flat)
        size = min(LANES, 800 - LANES * q)
        v_fc[pl.ds(LANES * q, size)] = flat[0, :size]
    odd = lax.rem(rank, 2) == 1
    for k in range(4):
        here = v_own[BN + k:BN + k + 1, :]
        after = v_own[BN + k + 1:BN + k + 2, :]
        turned = jnp.where(lane_row < 64, pltpu.roll(here, 64, 1), pltpu.roll(after, 64, 1))
        size = min(LANES, 448 - LANES * k)
        v_bn[pl.ds(LANES * k, size)] = jnp.where(odd, turned, here)[0, :size]
    v_bias[...] = pltpu.roll(v_own[BIAS:BIAS + 1, :], lax.rem(N_DEV - rank, N_DEV) * 4, 1)[0, :4]
    momenta = (v_mid, v_in, v_in0, v_out, v_short, v_fc, v_bn, v_bias)
    moved = [pltpu.make_async_copy(src, dst, sems.at[19 + k]) for k, (src, dst) in enumerate(zip(momenta, v_outs))]
    for copy in moved:
        copy.start()
    fetches[1].wait()
    lax.fori_loop(4, 16, mid_body, 0)
    fetches[2].wait()
    lax.fori_loop(16, N_MID, mid_body, 0)
    fetches[3].wait()

    def in_pair(first, second, row, other):
        for a in range(4):
            for k in range(4):
                x = packed[across(a, row + k), :]
                y = packed[across(a, other + k), :]
                xt[pl.ds(64 * a + 2 * k, 8, stride=8), :] = left(x, y)
                xt[pl.ds(64 * a + 2 * k + 1, 8, stride=8), :] = right(x, y)
        for h in range(2):
            cols = xt[128 * h:128 * h + 128, :].T
            for u, t in enumerate((first, second)):
                s_in[t, :, 128 * h:128 * h + 128] = cols[64 * u:64 * u + 64]
                t_in[t, :, 128 * h:128 * h + 128] = cols[64 * u:64 * u + 64].astype(bf)
        for t in (first, second):
            put(s_in.at[t], n_in.at[t], 2)
            put(t_in.at[t], b_in.at[t], 3)

    def in_body(j, carry):
        in_pair(2 * j + 5, 2 * j + 6, 184 + 8 * j, 188 + 8 * j)
        return carry

    lax.fori_loop(0, 6, in_body, 0)
    in_pair(0, 1, in_row(0), in_row(1))
    in_pair(2, 3, in_row(2), in_row(3))
    for a in range(4):
        for k in range(4):
            x = packed[across(a, in_row(4) + k), :]
            xt[pl.ds(64 * a + 2 * k, 8, stride=8), :] = x
            xt[pl.ds(64 * a + 2 * k + 1, 8, stride=8), :] = right(x, x)
    for h in range(2):
        cols = xt[128 * h:128 * h + 128, :].T
        s_in[4, :, 128 * h:128 * h + 128] = cols[:64]
        t_in[4, :, 128 * h:128 * h + 128] = cols[:64].astype(bf)
    put(s_in.at[4], n_in.at[4], 2)
    put(t_in.at[4], b_in.at[4], 3)
    for a in range(4):
        for k in range(2):
            x = packed[across(a, IN0 + k), :]
            xt[pl.ds(32 * a + 2 * k, 8, stride=4), :] = x
            xt[pl.ds(32 * a + 2 * k + 1, 8, stride=4), :] = right(x, x)
    cols = xt[0:128, :].T
    s_in0[...] = cols[:64]
    t_in0[...] = cols[:64].astype(bf)
    put(s_in0, n_in0, 4)
    put(t_in0, b_in0, 5)

    def out_body(t, carry):
        for a in range(4):
            for p in range(2):
                for h in range(2):
                    s_out[h, t, pl.ds(16 * a + p, 8, stride=2), :] = packed[across(a, OUT + 4 * t + 2 * p + h), :]
        for h in range(2):
            t_out[h, t] = s_out[h, t].astype(bf)
            put(s_out.at[h, t], n_out.at[t, :, pl.ds(128 * h, 128)], 6)
            put(t_out.at[h, t], b_out.at[t, :, pl.ds(128 * h, 128)], 7)
        return carry

    fetches[4].wait()
    lax.fori_loop(0, N_OUT, out_body, 0)
    fetches[5].wait()
    for h in range(2):
        for a in range(4):
            for p in range(4):
                s_short[h, pl.ds(32 * a + p, 8, stride=4), :] = packed[across(a, SHORT + 2 * p + h), :]
        t_short[h] = s_short[h].astype(bf)
        put(s_short.at[h], n_short.at[:, pl.ds(128 * h, 128)], 8)
        put(t_short.at[h], b_short.at[:, pl.ds(128 * h, 128)], 9)
    for i in range(N_DEV):
        xt[8 * i:8 * i + 8, :] = packed[i * ROWS + FC:i * ROWS + FC + 8, :]
    for h in range(2):
        cols = xt[128 * h:128 * h + 128, :].T
        s_fc[:, 128 * h:128 * h + 128] = cols[:CLASSES]
        t_fc[:, 128 * h:128 * h + 128] = cols[:CLASSES].astype(bf)
    put(s_fc, n_fc, 10)
    put(t_fc, b_fc, 11)

    lane = lax.broadcasted_iota(jnp.int32, (8, LANES), 1)
    for b in range(2):
        def even(k):
            return packed[pl.ds(16 * b * ROWS + BN + k, 8, stride=2 * ROWS), :]

        def odd(k):
            return packed[pl.ds((16 * b + 1) * ROWS + BN + k, 8, stride=2 * ROWS), :]

        for k in range(3):
            n_bn[pl.ds(56 * b + k, 8, stride=7), :] = even(k)
            n_bn[pl.ds(56 * b + 4 + k, 8, stride=7), :] = odd(1 + k)
        n_bn[pl.ds(56 * b + 3, 8, stride=7), :] = jnp.where(lane < 64, even(3), odd(0))
    total = packed[across(0, BIAS), :]
    for a in range(1, 4):
        total = total + packed[across(a, BIAS), :]
    n_bias[...] = jnp.sum(total, axis=0, keepdims=True)[0, :CLASSES]

    last = []
    for k, (src, dst) in enumerate(((n_bn, bn_out), (n_bias, bias_out))):
        last.append(pltpu.make_async_copy(src, dst, sems.at[27 + k]))
        last[-1].start()
    for k, (src, dst) in enumerate(((s_mid, n_mid), (t_mid, b_mid), (s_in, n_in), (t_in, b_in), (s_in0, n_in0),
                                    (t_in0, b_in0))):
        pltpu.make_async_copy(src, dst, sems.at[k]).wait()
    for h in range(2):
        half = pl.ds(128 * h, 128)
        for k, (src, dst) in enumerate(((s_out, n_out.at[:, :, half]), (t_out, b_out.at[:, :, half]),
                                        (s_short, n_short.at[:, half]), (t_short, b_short.at[:, half]))):
            pltpu.make_async_copy(src.at[h], dst, sems.at[6 + k]).wait()
    pltpu.make_async_copy(s_fc, n_fc, sems.at[10]).wait()
    pltpu.make_async_copy(t_fc, b_fc, sems.at[11]).wait()
    for copy in moved + last:
        copy.wait()


def unpack_weights(packed, v_own):
    any_ = pl.BlockSpec(memory_space=pl.ANY)
    bf = jnp.bfloat16
    kernels = ((N_MID, 576, 64), (N_IN, 64, 256), (64, 128), (N_OUT, 64, 256), (128, 256), (CLASSES, 256))
    shapes = [(s, F32) for s in kernels] + [((112, 128), F32), ((CLASSES,), F32)] + [(s, bf) for s in kernels]
    shapes += [(s, F32) for s in ((N_MID, 1152), (N_IN, 512), (2, LANES), (N_OUT, 512), (8, LANES), (800,), (448,), (4,))]
    scratch = ((N_MID, 576, 64), (N_IN, 64, 256), (2, N_OUT, 64, 128), (2, 128, 128), (64, 128), (CLASSES, 256))
    return pl.pallas_call(
        unpack_kernel,
        out_shape=[jax.ShapeDtypeStruct(s, d) for s, d in shapes],
        in_specs=[any_, any_],
        out_specs=[any_] * 22,
        scratch_shapes=[VMEM(s, d) for s, d in shapes[6:8] + shapes[14:]] + [VMEM((N_DEV * ROWS, LANES), F32), VMEM((ROWS, LANES), F32)] + [VMEM(s, F32) for s in scratch] + [VMEM(s, bf) for s in scratch]
        + [VMEM((256, 128), F32), pltpu.SemaphoreType.DMA((29,))],
        compiler_params=pltpu.CompilerParams(vmem_limit_bytes=VMEM_LIMIT),
    )(packed, v_own)


def solution(mesh):
    spec_full = P()
    spec_lead = P('dp')
    spec_cols = P(None, 'dp')
    moment_specs = (spec_lead, spec_lead, spec_cols, spec_cols, spec_cols, spec_lead, spec_lead, spec_lead)
    in_specs = (spec_full,) * 8 + (spec_lead,) * 8 + moment_specs + (spec_full,)
    out_specs = (spec_full,) * 14 + moment_specs

    def body(w_in0, w_short, w_in, w_mid, w_out, w_fc, w_bn, w_bias,
             g_in0, g_short, g_in, g_mid, g_out, g_bn, pooled, dlogits,
             v_in0, v_short, v_in, v_mid, v_out, v_fc, v_bn, v_bias, learn_rate):
        gathered, v_next = exchange((
            learn_rate.reshape(1), g_mid.reshape(N_MID, 576, 64), jnp.swapaxes(g_in[0], 1, 2), g_in0[0].T, g_out[0],
            g_short[0], g_bn.reshape(112, LANES), pooled, dlogits.T,
            w_mid.reshape(N_MID, 576, 64), jnp.swapaxes(w_in, 1, 2), w_in0.T, w_out, w_short, w_fc.T,
            w_bn.reshape(112, LANES), w_bias, v_mid, v_in, v_in0.reshape(2, LANES), v_out, v_short.reshape(8, LANES),
            v_fc, v_bn, v_bias))
        (n_mid, n_in, n_in0, n_out, n_short, n_fc, n_bn, n_bias, b_mid, b_in, b_in0, b_out, b_short, b_fc,
         m_mid, m_in, m_in0, m_out, m_short, m_fc, m_bn, m_bias) = unpack_weights(gathered, v_next)
        return (n_in0.T, n_short, jnp.swapaxes(n_in, 1, 2), n_mid.reshape(w_mid.shape), n_out, n_fc.T,
                n_bn.reshape(-1), n_bias,
                b_in0.T, b_short, jnp.swapaxes(b_in, 1, 2), b_mid.reshape(w_mid.shape), b_out, b_fc.T,
                m_in0.reshape(-1), m_short.reshape(-1), m_in, m_mid, m_out, m_fc, m_bn, m_bias)

    return jax.shard_map(body, mesh=mesh, in_specs=in_specs, out_specs=out_specs, check_vma=False)
```

```python
import jax
import jax.numpy as jnp
from jax import lax
from jax.experimental import pallas as pl
from jax.experimental.pallas import tpu as pltpu
from jax.sharding import PartitionSpec as P

MOMENTUM = 0.9
TRUST_COEF = 0.001
DECAY = 0.0001
N_DEV = 32
LANES = 128
IN0, OUT, SHORT, FC, BN, BIAS, ROWS = 178, 232, 304, 312, 320, 324, 328
N_MID, N_IN, N_OUT = 18, 17, 18
CLASSES = 100
ID_IN0, ID_IN, ID_OUT, ID_SHORT, ID_FC, ID_PLAIN = 18, 19, 36, 54, 55, 56
F32 = jnp.float32
VMEM = pltpu.VMEM
MESH = pl.DeviceIdType.MESH
CHUNKS = (
    (0, 40, 'x'), (40, 40, 'y'), (80, 40, 'x'), (120, 40, 'y'), (160, 24, 'y'),
    (184, 24, 'x'), (208, 24, 'zx'), (232, 24, 'y'), (256, 24, 'x'), (280, 24, 'zx'),
    (304, 24, 'y'),
)
STEPS = (
    (1, 0), (8, 0), (9, 0), (7, 0), (1, 1), (8, 1), (2, 0), (9, 1), (6, 0), (2, 1), (4, 0), (8, 2), (1, 2), (6, 1),
    (7, 1), (3, 0), (0, 0), (2, 2), (0, 1), (3, 1), (8, 3), (7, 2), (1, 3), (10, 0), (2, 3), (0, 2), (9, 2), (5, 0),
    (3, 2), (4, 1), (7, 3), (8, 4), (10, 1), (5, 1), (0, 3), (1, 4), (9, 3), (3, 3), (4, 2), (2, 4), (5, 2), (6, 2),
    (7, 4), (8, 5), (10, 2), (4, 3), (9, 4), (6, 3), (1, 5), (5, 3), (0, 4), (2, 5), (10, 3), (3, 4), (8, 6), (7, 5),
    (6, 4), (9, 5), (1, 6), (4, 4), (0, 5), (5, 4), (3, 5), (2, 6), (10, 4), (7, 6), (9, 6), (6, 5), (8, 7), (5, 5),
    (4, 5), (1, 7), (0, 6), (9, 7), (10, 5), (3, 6), (2, 7), (7, 7), (4, 6), (6, 6), (1, 8), (8, 8), (5, 6), (2, 8),
    (10, 6), (9, 8), (7, 8), (6, 7), (3, 7), (0, 7), (4, 7), (2, 9), (10, 7), (6, 8), (5, 7), (3, 8), (0, 8), (8, 9),
    (4, 8), (7, 9), (9, 9), (2, 10), (5, 8), (1, 9), (10, 8), (1, 10), (3, 9), (0, 9), (3, 10), (4, 9), (9, 10),
    (5, 9), (6, 9), (7, 10), (8, 10), (10, 9), (5, 10), (6, 10), (0, 10), (4, 10), (10, 10),
)
FIRST_NORMS = [step for step in STEPS if step[1] == 4][0]
S_CORE, S_ONE, S_TWO, S_Z, A_Z, A_TWO, A_ONE, A_CORE, N_SEMS = 0, 2, 4, 6, 7, 8, 10, 12, 14
EXCHANGE_VMEM, UNPACK_VMEM = 30 * 2**20, 20 * 2**20


def mid_row(t):
    return 40 * (t // 4) + 9 * (t % 4)


def in_row(t):
    return 36 + 40 * t if t < 4 else 164 + 4 * t


def member_rows(row, t):
    first = 9 * t
    for group in (4, 8, 12, 16):
        first = jnp.where(t >= group, first + 4, first)
    size = jnp.where(t < N_MID, 9, jnp.where(t == ID_IN0, 2, jnp.where(t < ID_SHORT, 4, 8)))
    first = jnp.where(t >= ID_IN0, IN0, first)
    first = jnp.where(t >= ID_IN, 36 + 40 * (t - ID_IN), first)
    first = jnp.where(t >= ID_IN + 4, 164 + 4 * (t - ID_IN), first)
    first = jnp.where(t >= ID_OUT, OUT + 4 * (t - ID_OUT), first)
    first = jnp.where(t >= ID_SHORT, SHORT + 8 * (t - ID_SHORT), first)
    return (row >= first) & (row < first + size)


def momentum_rows(mid, inn, out):
    runs = [(mid, mid_row(t), 9, t, min(4, N_MID - t)) for t in range(0, N_MID, 4)]
    runs += [(inn, 36, 40, 0, 4)] + [(inn, 164 + 4 * t, 4, t, min(8, N_IN - t)) for t in (4, 12)]
    runs += [(out, OUT + 4 * t, 4, t, min(8, N_OUT - t)) for t in (0, 8, 16)]
    for ref, base, stride, t, count in runs:
        for m in range(9 if ref is mid else 4):
            yield pl.ds(base + m, count, stride=stride), pl.ds(128 * m, 128), ref, pl.ds(t, count)


def left(a, b):
    return jnp.concatenate([a[:, :64], b[:, :64]], axis=1)


def right(a, b):
    return jnp.concatenate([a[:, 64:], b[:, 64:]], axis=1)


def across(piece8, row):
    return pl.ds(piece8 * 8 * ROWS + row, 8, stride=ROWS)


def exchange_kernel(lr, g_mid, g_in, g_in0, g_out, g_short, g_bn, pooled, dlog_t,
                    w_mid, w_in, w_in0, w_out, w_short, w_fc, w_bn, w_bias,
                    v_mid, v_in, v_in0, v_out, v_short, v_fc, v_bn, v_bias,
                    full, v_new,
                    s_mid, s_in, s_in0, s_out, s_short, s_bn, s_x, s_d, xt, fct,
                    o_mid, o_in, o_in0, o_out, o_short, o_fc, o_bn, o_bias, ot,
                    p_mid, p_in, p_in0, p_out, p_short, p_fc, p_bn, p_bias,
                    packed, w_own, v_own,
                    got_core, acc, got_one, got_two, got_z, got_line, grad, layer_norms, norms,
                    sems, send, recv, n_send, n_recv):
    rank = lax.axis_index('dp')
    core = lax.rem(rank, 2)
    x = lax.rem(rank // 2, 2)
    y = lax.rem(rank // 4, 2)
    z = rank // 8

    def device(zz, yy, xx, cc):
        return (((zz * 2 + yy) * 2 + xx) * 2 + cc,)

    core_peer = device(z, y, x, 1 - core)
    x_peer = device(z, y, 1 - x, core)
    y_peer = device(z, 1 - y, x, core)

    barrier = pltpu.get_barrier_semaphore()

    def layer(d):
        return (z * 8 + lax.rem(rank + d, 8),)

    def line(d):
        return (lax.rem(rank + 8 * d, N_DEV),)

    for d in range(1, 8):
        pl.semaphore_signal(barrier, inc=1, device_id=layer(d), device_id_type=MESH)
    for d in range(1, 4):
        pl.semaphore_signal(barrier, inc=1, device_id=line(d), device_id_type=MESH)

    waiting = {}
    count = [0]

    def fetch(name, src, dst):
        copy = pltpu.make_async_copy(src, dst, sems.at[count[0]])
        count[0] += 1
        copy.start()
        waiting.setdefault(name, []).append(copy)

    def need(*names):
        for name in names:
            for copy in waiting.pop(name, []):
                copy.wait()

    def halves(name, src, dst):
        for h in range(2):
            fetch(name, src(pl.ds(128 * h, 128)), dst.at[h])

    fetchers = {
        'in': lambda: fetch('in', g_in.at[pl.ds(5, 12)], s_in.at[pl.ds(5, 12)]),
        'in1': lambda: fetch('in1', g_in.at[pl.ds(0, 5)], s_in.at[pl.ds(0, 5)]),
        'in0': lambda: fetch('in0', g_in0, s_in0),
        'out': lambda: halves('out', lambda c: g_out.at[:, :, c], s_out),
        'short': lambda: halves('short', lambda c: g_short.at[:, c], s_short),
        'fc': lambda: (fetch('fc', pooled, s_x), fetch('fc', dlog_t, s_d)),
        'bn': lambda: fetch('bn', g_bn, s_bn),
    }
    for i in range(5):
        part = pl.ds(4 * i, min(4, N_MID - 4 * i))
        fetchers['mid%d' % i] = lambda i=i, part=part: fetch('mid%d' % i, g_mid.at[part], s_mid.at[part])
    units = [(40 * i, 40 * i + 40, ('mid%d' % i, 'in1')) for i in range(4)] + [(160, 184, ('mid4', 'in0', 'in1'))]
    units += [(184 + 8 * j, 192 + 8 * j, ('in',)) for j in range(6)]
    units += [(232 + 8 * j, 240 + 8 * j, ('out',)) for j in range(9)]
    units += [(304, 312, ('short',)), (312, 320, ('fc',)), (320, 328, ('bn', 'fc'))]
    for at, size, _ in CHUNKS:
        for lo, hi, names in units:
            if at <= lo < at + size:
                for name in names:
                    if name in fetchers:
                        fetchers.pop(name)()

    mid_at = pl.multiple_of((18 * rank) // 8 * 8, 8)
    mid_off = lax.rem(18 * rank, 8)
    out_at = pl.multiple_of((2 * rank) // 8 * 8, 8)
    out_off = 2 * lax.rem(rank, 4)
    short_at = pl.multiple_of((4 * rank) // 8 * 8, 8)
    short_off = 4 * lax.rem(rank, 2)
    col_at = pl.multiple_of((rank // 16) * 128, 128)
    col_off = pl.multiple_of(lax.rem(rank, 16) * 8, 8)
    fetch('own', w_mid.at[:, pl.ds(mid_at, 24), :], o_mid)
    fetch('own', w_in.at[:, :, pl.ds(col_at, 128)], o_in)
    fetch('own', w_in0, o_in0)
    halves('own', lambda c: w_out.at[:, pl.ds(out_at, 8), c], o_out)
    halves('own', lambda c: w_short.at[pl.ds(short_at, 8), c], o_short)
    fetch('own', w_fc.at[:, pl.ds(col_at, 128)], o_fc)
    fetch('own', w_bn, o_bn)
    fetch('own', w_bias, o_bias)
    for src, dst in ((v_mid, p_mid), (v_in, p_in), (v_in0, p_in0), (v_out, p_out), (v_short, p_short), (v_fc, p_fc),
                     (v_bn, p_bn), (v_bias, p_bias)):
        fetch('own', src, dst)

    pieces = packed.reshape(N_DEV * ROWS, LANES)

    def pack_mid(base, first, count):
        def body(u, carry):
            t = first + u
            for a in range(4):
                for k in range(9):
                    even = s_mid[t, pl.ds(144 * a + 2 * k, 8, stride=18), :]
                    odd = s_mid[t, pl.ds(144 * a + 2 * k + 1, 8, stride=18), :]
                    pieces[across(a, base + 9 * u + k), :] = jnp.concatenate([even, odd], axis=1)
            return carry

        lax.fori_loop(0, count, body, 0)

    def pack_in_rows(base, pair):
        for a in range(4):
            for k in range(4):
                even = xt[pl.ds(64 * a + 2 * k, 8, stride=8), :]
                odd = xt[pl.ds(64 * a + 2 * k + 1, 8, stride=8), :]
                pieces[across(a, base + k), :] = left(even, odd)
                if pair:
                    pieces[across(a, base + 4 + k), :] = right(even, odd)

    def transpose(a, b):
        both = jnp.concatenate([a, b], axis=0)
        for h in range(2):
            xt[128 * h:128 * h + 128, :] = both[:, 128 * h:128 * h + 128].T

    def pack_in(first, last):
        def body(j, carry):
            transpose(s_in[2 * j + 5], s_in[2 * j + 6])
            pack_in_rows(184 + 8 * j, True)
            return carry

        lax.fori_loop(first, last, body, 0)

    def pack_in_one(t):
        wide = jnp.concatenate([s_in0[...], s_in0[...]], axis=1) if t == 4 else s_in[t]
        transpose(s_in[t], wide)
        pack_in_rows(in_row(t), False)
        if t == 4:
            for a in range(4):
                for k in range(2):
                    even = xt[pl.ds(32 * a + 2 * k, 8, stride=4), :]
                    odd = xt[pl.ds(32 * a + 2 * k + 1, 8, stride=4), :]
                    pieces[across(a, IN0 + k), :] = right(even, odd)

    def pack_out(first, last):
        def body(t, carry):
            for a in range(4):
                for p in range(2):
                    for h in range(2):
                        pieces[across(a, OUT + 4 * t + 2 * p + h), :] = s_out[h, t, pl.ds(16 * a + p, 8, stride=2), :]
            return carry

        lax.fori_loop(first, last, body, 0)

    def pack_short():
        for a in range(4):
            for p in range(4):
                for h in range(2):
                    pieces[across(a, SHORT + 2 * p + h), :] = s_short[h, pl.ds(32 * a + p, 8, stride=4), :]

    scale = 1.0 / pooled.shape[0]

    def pack_fc():
        fct[CLASSES:LANES, :] = jnp.zeros((LANES - CLASSES, 256), F32)
        fct[0:CLASSES, :] = jnp.dot(s_d[...], s_x[...], preferred_element_type=F32) * scale
        for h in range(2):
            cols = fct[:, 128 * h:128 * h + 128].T
            for j in range(16):
                at = (16 * h + j) * ROWS + FC
                pieces[at:at + 8, :] = cols[8 * j:8 * j + 8, :]

    def pack_bn():
        def clear(i, carry):
            pieces[pl.ds(pl.multiple_of(i * ROWS + BN, 8), 8), :] = jnp.zeros((8, LANES), F32)
            return carry

        lax.fori_loop(0, N_DEV, clear, 0)
        for b in range(2):
            for k in range(4):
                for half in range(2):
                    pieces[pl.ds((16 * b + half) * ROWS + BN + k, 8, stride=2 * ROWS), :] = (
                        s_bn[pl.ds(56 * b + 3 * half + k, 8, stride=7), :])
        bias = lax.dot_general(jnp.ones((8, s_d.shape[1]), jnp.bfloat16), s_d[...], (((1,), (1,)), ((), ())),
                               preferred_element_type=F32) * scale
        bias = jnp.concatenate([bias, jnp.zeros((8, LANES - CLASSES), F32)], axis=1)
        for a in range(4):
            pieces[across(a, BIAS), :] = bias

    def pack(at, size):
        end = at + size
        for lo, hi, names in units:
            if at <= lo < end:
                need(*names)
        for i in range(5):
            if at <= 40 * i < end:
                pack_mid(40 * i, 4 * i, min(4, N_MID - 4 * i))
                pack_in_one(i)
        lo, hi = max(at, 184), min(end, 232)
        if lo < hi:
            pack_in((lo - 184) // 8, (hi - 184) // 8)
        lo, hi = max(at, OUT), min(end, SHORT)
        if lo < hi:
            pack_out((lo - OUT) // 4, (hi - OUT) // 4)
        if at <= SHORT < end:
            pack_short()
        if at <= FC < end:
            pack_fc()
        if at <= BN < end:
            pack_bn()

    lane_row = lax.broadcasted_iota(jnp.int32, (1, LANES), 1)

    def own_pieces():
        need('own')
        for rows, tile, ref, tensors in momentum_rows(p_mid, p_in, p_out):
            v_own[rows, :] = ref[tensors, tile]
        v_own[IN0:IN0 + 2, :] = p_in0[...]
        v_own[SHORT:SHORT + 8, :] = p_short[...]
        flat = [p_fc[pl.ds(128 * q, 128)].reshape(1, LANES) for q in range(6)]
        flat.append(jnp.concatenate([p_fc[pl.ds(768, 32)].reshape(1, 32), jnp.zeros((1, 96), F32)], axis=1))
        for r in range(8):
            q, s = divmod(CLASSES * r, LANES)
            row = pltpu.roll(flat[q], (LANES - s) % LANES, 1)
            if s + CLASSES > LANES:
                row = jnp.where(lane_row < LANES - s, row, pltpu.roll(flat[q + 1], LANES - s, 1))
            v_own[FC + r:FC + r + 1, :] = jnp.where(lane_row < CLASSES, row, 0.0)
        v_own[BN:ROWS, :] = jnp.zeros((8, LANES), F32)
        odd = lax.rem(rank, 2) == 1
        rows = [p_bn[pl.ds(128 * k, 128)].reshape(1, LANES) for k in range(3)]
        rows.append(jnp.concatenate([p_bn[pl.ds(384, 64)].reshape(1, 64), jnp.zeros((1, 64), F32)], axis=1))
        for k in range(4):
            before = pltpu.roll(rows[k - 1], 64, 1) if k else jnp.zeros((1, LANES), F32)
            moved = jnp.where(lane_row < 64, before, pltpu.roll(rows[k], 64, 1))
            v_own[BN + k:BN + k + 1, :] = jnp.where(odd, moved, rows[k])
        four = jnp.concatenate([p_bias[...].reshape(1, 4), jnp.zeros((1, LANES - 4), F32)], axis=1)
        v_own[BIAS:BIAS + 1, :] = pltpu.roll(four, 4 * rank, 1)

        for t in range(N_MID):
            even = o_mid[t, pl.ds(mid_off, 9, stride=2), :]
            odds = o_mid[t, pl.ds(mid_off + 1, 9, stride=2), :]
            w_own[mid_row(t):mid_row(t) + 9, :] = jnp.concatenate([even, odds], axis=1)
        for j in range(9):
            other = o_in[2 * j - 1] if j else o_in0[...]
            ot[...] = jnp.concatenate([other, o_in[2 * j]], axis=0).T
            if j == 0:
                w_own[IN0:IN0 + 2, :] = left(ot[pl.ds(4 * rank, 2, stride=2), :], ot[pl.ds(4 * rank + 1, 2, stride=2), :])
            even = ot[pl.ds(col_off, 4, stride=2), :]
            odds = ot[pl.ds(col_off + 1, 4, stride=2), :]
            if j:
                w_own[in_row(2 * j - 1):in_row(2 * j - 1) + 4, :] = left(even, odds)
            w_own[in_row(2 * j):in_row(2 * j) + 4, :] = right(even, odds)
        def own_out(t, carry):
            for p in range(2):
                for h in range(2):
                    w_own[pl.ds(OUT + 4 * t + 2 * p + h, 1), :] = o_out[h, t, pl.ds(out_off + p, 1), :]
            return carry

        lax.fori_loop(0, N_OUT, own_out, 0)
        for p in range(4):
            for h in range(2):
                w_own[SHORT + 2 * p + h:SHORT + 2 * p + h + 1, :] = o_short[h, pl.ds(short_off + p, 1), :]
        ot[0:CLASSES, :] = o_fc[...]
        ot[CLASSES:LANES, :] = jnp.zeros((LANES - CLASSES, LANES), F32)
        ot[...] = ot[...].T
        w_own[FC:FC + 8, :] = ot[pl.ds(col_off, 8), :]
        w_own[BN:ROWS, :] = jnp.zeros((8, LANES), F32)
        bn_at = 7 * (rank // 2) + 3 * lax.rem(rank, 2)
        for k in range(4):
            w_own[BN + k:BN + k + 1, :] = o_bn[pl.ds(bn_at + k, 1), :]
        bias = jnp.concatenate([o_bias[...].reshape(1, CLASSES), jnp.zeros((1, LANES - CLASSES), F32)], axis=1)
        w_own[BIAS:BIAS + 1, :] = jnp.where((lane_row >= 4 * rank) & (lane_row < 4 * rank + 4), bias, 0.0)

    sent = {}

    def start(c, k, src, dst, peer):
        pltpu.make_async_remote_copy(src_ref=src, dst_ref=dst, send_sem=send.at[c * N_SEMS + k],
                                     recv_sem=recv.at[c * N_SEMS + k], device_id=peer, device_id_type=MESH).start()
        sent[c, k] = sent.get((c, k), 0) + (1 if len(src.shape) == 2 else src.size // (src.shape[-1] * src.shape[-2]))

    def wait(c, k, semaphores):
        at, size, _ = CHUNKS[c]
        rows = pl.ds(at, size)
        count = sent[c, k]
        lead = {1: (0, 0, 0), 2: (0, 0), 3: (pl.ds(0, 3), 0, 0), 4: (0,), 8: (pl.ds(0, 2),), 12: (pl.ds(0, 3),), 16: ()}[count]
        block = got_core.at[lead + (slice(None),) * (3 - len(lead)) + (rows,)]
        pltpu.make_async_copy(block, block, semaphores.at[c * N_SEMS + k]).wait()

    def arrived(c, *numbers):
        for k in numbers:
            wait(c, k, recv)

    def tell(k, row, peer):
        pltpu.make_async_remote_copy(src_ref=row, dst_ref=row, send_sem=n_send.at[k], recv_sem=n_recv.at[k],
                                     device_id=peer, device_id_type=MESH).start()

    def told(k, semaphores):
        rows = layer_norms.at[k // 2, pl.ds(0, 3 if k % 2 else 7)]
        pltpu.make_async_copy(rows, rows, semaphores.at[k]).wait()

    def step(c, stage):
        at, size, first = CHUNKS[c]
        rows = pl.ds(at, size)
        x_first, z_first = first[-1] == 'x', first[0] == 'z'
        one_peer, two_peer = (x_peer, y_peer) if x_first else (y_peer, x_peer)

        here = y if x_first else x

        def block(ref, near, *rest):
            first_at = (x if near else 1 - x) if x_first else (y if near else 1 - y)
            return ref.at[(slice(None), slice(None), first_at) + rest] if x_first else (
                ref.at[(slice(None), first_at, slice(None)) + rest])

        def spot(second, near):
            return (second, x if near else 1 - x) if x_first else (y if near else 1 - y, second)

        def both_cores(zz, second, near):
            a, b = spot(second, near)
            return packed[zz, a, b, core, rows, :] + got_core[zz, a, b, rows, :]

        def over_z(body):
            def run(zz, carry):
                body(zz)
                return carry

            lax.fori_loop(0, 4, run, 0)

        if stage == 0:
            pack(at, size)
            if not sent:
                pl.semaphore_wait(barrier, 10)
            for k, near in enumerate((False, True)):
                start(c, S_CORE + k, block(packed, near, 1 - core, rows), block(got_core, near, rows), core_peer)
        elif stage == 1 and z_first:
            arrived(c, S_CORE, S_CORE + 1)
            for d in (2, 3, 1, 0):
                zz = lax.rem(z + d, 4)
                acc[zz, :, :, rows, :] = packed[zz, :, :, core, rows, :] + got_core[zz, :, :, rows, :]
                if d:
                    start(c, S_Z, acc.at[zz, :, :, rows, :], got_line.at[d - 1, :, :, rows, :], line(d))
        elif stage == 1:
            arrived(c, S_CORE)
            for k, second in enumerate((1 - here, here)):
                a, b = spot(second, False)

                def body(zz, a=a, b=b, second=second):
                    acc[zz, a, b, rows, :] = both_cores(zz, second, False)

                over_z(body)
                start(c, S_ONE + k, acc.at[:, a, b, rows, :], got_one.at[:, second, rows, :], one_peer)
        elif stage == 2 and z_first:
            arrived(c, S_Z)
            for near in (False, True):
                for second in range(2):
                    a, b = spot(second, near)
                    total = acc[z, a, b, rows, :] + got_line[0, a, b, rows, :]
                    acc[z, a, b, rows, :] = total + got_line[1, a, b, rows, :] + got_line[2, a, b, rows, :]
                if not near:
                    far = acc.at[z, :, 1 - x, rows, :] if x_first else acc.at[z, 1 - y, :, rows, :]
                    start(c, S_ONE, far, got_one.at[0, :, rows, :], one_peer)
        elif stage == 2:
            arrived(c, S_CORE + 1, S_ONE)
            a, b = spot(1 - here, True)

            def body(zz):
                acc[zz, a, b, rows, :] = both_cores(zz, 1 - here, True) + got_one[zz, 1 - here, rows, :]

            over_z(body)
            for d in (1, 2, 3, 0):
                zz = lax.rem(z + d, 4)
                start(c, S_TWO + (d == 0), acc.at[zz, a, b, rows, :], got_two.at[zz, rows, :], two_peer)
        elif stage == 3 and z_first:
            arrived(c, S_ONE)
            a, b = spot(1 - here, True)
            acc[z, a, b, rows, :] = acc[z, a, b, rows, :] + got_one[0, 1 - here, rows, :]
            start(c, S_TWO, acc.at[z, a, b, rows, :], got_two.at[0, rows, :], two_peer)
        elif stage == 3:
            arrived(c, S_ONE + 1, S_TWO)
            for d in (2, 3, 1):
                zz = lax.rem(z + d, 4)
                acc[zz, y, x, rows, :] = (
                    both_cores(zz, here, True) + got_one[zz, here, rows, :] + got_two[zz, rows, :])
                start(c, S_Z, acc.at[zz, y, x, rows, :], got_z.at[d - 1, rows, :], line(d))
        elif stage == 4:
            if z_first:
                arrived(c, S_TWO)
                mean = acc[z, y, x, rows, :] + got_one[0, here, rows, :] + got_two[0, rows, :]
            else:
                arrived(c, S_TWO + 1, S_Z)
                mean = both_cores(z, here, True) + got_one[z, here, rows, :] + got_two[z, rows, :]
                mean = mean + got_z[0, rows, :] + got_z[1, rows, :] + got_z[2, rows, :]
            mean = mean * (1.0 / N_DEV)
            grad[rows, :] = mean
            own = w_own[rows, :]
            g_sum = jnp.sum(mean * mean, axis=1, keepdims=True)
            w_sum = jnp.sum(own * own, axis=1, keepdims=True)
            row = lax.broadcasted_iota(jnp.int32, (size, LANES), 0) + at
            lane = lax.broadcasted_iota(jnp.int32, (size, LANES), 1)
            tensor = jnp.where(lane < 64, lane, lane - 64)
            member = member_rows(row, tensor)
            part = jnp.where(member, jnp.where(lane < 64, g_sum, w_sum), 0.0)
            here8 = lax.rem(rank, 8)
            layer_norms[c, here8] = jnp.sum(part, axis=0, keepdims=True)
            row8 = layer_norms.at[c, here8]
            for d in range(1, 8):
                tell(2 * c, row8, layer(d))
        elif stage == 5:
            told(2 * c, n_recv)
            norms[c, z] = jnp.sum(layer_norms[c], axis=0)
            for d in range(1, 4):
                tell(2 * c + 1, norms.at[c, z], line(d))
        elif stage == 6:
            told(2 * c + 1, n_recv)
            total = jnp.sum(norms[c], axis=0)
            g_norm = jnp.sqrt(total)
            w_norm = pltpu.roll(g_norm, 64, 1)
            trust = jnp.where((w_norm > 0) & (g_norm > 0), TRUST_COEF * w_norm / (g_norm + DECAY * w_norm), 1.0)
            row = lax.broadcasted_iota(jnp.int32, (size, LANES), 0) + at
            lane = lax.broadcasted_iota(jnp.int32, (size, LANES), 1)
            trust = jnp.where(lane == ID_PLAIN, 1.0, trust)
            member = member_rows(row, lane) & (lane <= ID_PLAIN)
            rate = lr[0] * jnp.sum(jnp.where(member, trust, 0.0), axis=1, keepdims=True)
            decay = jnp.where(row < BN, DECAY, 0.0)
            own = w_own[rows, :]
            moment = MOMENTUM * v_own[rows, :] + rate * (grad[rows, :] + decay * own)
            v_new[rows, :] = moment
            mine = (row != BIAS) | ((lane >= 4 * rank) & (lane < 4 * rank + 4))
            full[z, y, x, core, rows, :] = jnp.where(mine, own - moment, 0.0)
            piece = full.at[z, y, x, core, rows, :]
            if not z_first:
                for d in (2, 3, 1):
                    start(c, A_Z, piece, piece, line(d))
            start(c, A_TWO, piece, piece, two_peer)
        elif stage == 7 and z_first:
            arrived(c, A_TWO)
            pair = full.at[z, :, x, core, rows, :] if x_first else full.at[z, y, :, core, rows, :]
            start(c, A_ONE, pair, pair, one_peer)
        elif stage == 8 and z_first:
            arrived(c, A_ONE)
            plane = full.at[z, :, :, core, rows, :]
            for d in (2, 3, 1):
                start(c, A_Z, plane, plane, line(d))
        elif stage == 9 and z_first:
            arrived(c, A_Z)
            everything = full.at[:, :, :, core, rows, :]
            start(c, A_CORE, everything, everything, core_peer)
        elif stage == 10 and z_first:
            arrived(c, A_CORE)
        elif stage == 7:
            arrived(c, A_Z)
            for d in (1, 2, 3):
                piece = full.at[lax.rem(z + d, 4), y, x, core, rows, :]
                start(c, A_TWO + 1, piece, piece, two_peer)
            column = full.at[:, y, x, core, rows, :]
            start(c, A_ONE, column, column, one_peer)
        elif stage == 8:
            arrived(c, A_TWO, A_TWO + 1)
            a, b = spot(1 - here, True)
            column = full.at[:, a, b, core, rows, :]
            start(c, A_ONE + 1, column, column, one_peer)
            plane = block(full, True, core, rows)
            start(c, A_CORE, plane, plane, core_peer)
        elif stage == 9:
            arrived(c, A_ONE, A_ONE + 1)
            plane = block(full, False, core, rows)
            start(c, A_CORE + 1, plane, plane, core_peer)
        else:
            arrived(c, A_CORE, A_CORE + 1)

    for c, stage in STEPS:
        if stage == 4 and (c, stage) == FIRST_NORMS:
            own_pieces()
        step(c, stage)
    for c, k in sent:
        wait(c, k, send)
    for k in range(2 * len(CHUNKS)):
        told(k, n_send)


def exchange(operands):
    hbm = pl.BlockSpec(memory_space=pltpu.HBM)
    vm = pl.BlockSpec(memory_space=VMEM)
    count = len(CHUNKS)
    bf = jnp.bfloat16
    shapes = [(N_MID, 576, 64), (N_IN, 64, 256), (64, 128), (2, N_OUT, 64, 128), (2, 128, 128), (112, 128)]
    own = [(N_MID, 24, 64), (N_IN, 64, 128), (64, 128), (2, N_OUT, 8, 128), (2, 8, 128), (CLASSES, 128), (112, 128),
           (CLASSES,), (128, 128), (N_MID, 1152), (N_IN, 512), (2, LANES), (N_OUT, 512), (8, LANES), (800,), (448,), (4,)]
    rows = (ROWS, LANES)
    exchanged = [(4, 2, 2) + rows, (4, 2, 2) + rows, (4, 2) + rows, (4,) + rows, (3,) + rows, (3, 2, 2) + rows, rows,
                 (count, 8, 1, LANES), (count, 4, 1, LANES)]
    dma = pltpu.SemaphoreType.DMA
    placed = [pltpu.with_memory_space_constraint(operand, pltpu.HBM) for operand in operands[1:]]
    full, v_new = pl.pallas_call(
        exchange_kernel,
        out_shape=(jax.ShapeDtypeStruct((4, 2, 2, 2) + rows, F32), jax.ShapeDtypeStruct(rows, F32)),
        in_specs=[pl.BlockSpec(memory_space=pltpu.SMEM)] + [hbm] * 24,
        out_specs=(vm, vm),
        scratch_shapes=[VMEM(s, F32) for s in shapes]
        + [VMEM((1024, 256), bf), VMEM((CLASSES, 1024), bf), VMEM((256, 128), F32), VMEM((128, 256), F32)]
        + [VMEM(s, F32) for s in own]
        + [VMEM((4, 2, 2, 2) + rows, F32), VMEM(rows, F32), VMEM(rows, F32)]
        + [VMEM(s, F32) for s in exchanged]
        + [dma((40,)), dma((count * N_SEMS,)), dma((count * N_SEMS,)), dma((2 * count,)), dma((2 * count,))],
        compiler_params=pltpu.CompilerParams(vmem_limit_bytes=EXCHANGE_VMEM, collective_id=0, has_side_effects=True),
    )(operands[0], *placed)
    return full.reshape(N_DEV * ROWS, LANES), v_new


def unpack_kernel(packed, v_own, n_mid, n_in, n_in0, n_out, n_short, n_fc, bn_out, bias_out,
                  b_mid, b_in, b_in0, b_out, b_short, b_fc, *rest):
    v_outs, rest = rest[:8], rest[8:]
    n_bn, n_bias = rest[:2]
    (v_mid, v_in, v_in0, v_out, v_short, v_fc, v_bn, v_bias), rest = rest[2:10], rest[10:]
    (s_mid, s_in, s_out, s_short, s_in0, s_fc, t_mid, t_in, t_out, t_short, t_in0, t_fc, xt, sems) = rest
    bf = jnp.bfloat16
    lane_row = lax.broadcasted_iota(jnp.int32, (1, LANES), 1)

    def put(src, dst, k):
        pltpu.make_async_copy(src, dst, sems.at[k]).start()

    def mid_body(t, carry):
        for a in range(4):
            for k in range(9):
                x = packed[across(a, mid_row(t) + k), :]
                s_mid[t, pl.ds(144 * a + 2 * k, 8, stride=18), :] = x[:, :64]
                s_mid[t, pl.ds(144 * a + 2 * k + 1, 8, stride=18), :] = x[:, 64:]
        put(s_mid.at[t], n_mid.at[t], 0)
        t_mid[t] = s_mid[t].astype(bf)
        put(t_mid.at[t], b_mid.at[t], 1)
        return carry

    lax.fori_loop(0, N_MID, mid_body, 0)

    def in_pair(first, second, row, other):
        for a in range(4):
            for k in range(4):
                x = packed[across(a, row + k), :]
                y = packed[across(a, other + k), :]
                xt[pl.ds(64 * a + 2 * k, 8, stride=8), :] = left(x, y)
                xt[pl.ds(64 * a + 2 * k + 1, 8, stride=8), :] = right(x, y)
        for h in range(2):
            cols = xt[128 * h:128 * h + 128, :].T
            for u, t in enumerate((first, second)):
                s_in[t, :, 128 * h:128 * h + 128] = cols[64 * u:64 * u + 64]
                t_in[t, :, 128 * h:128 * h + 128] = cols[64 * u:64 * u + 64].astype(bf)
        for t in (first, second):
            put(s_in.at[t], n_in.at[t], 2)
            put(t_in.at[t], b_in.at[t], 3)

    def in_body(j, carry):
        in_pair(2 * j + 5, 2 * j + 6, 184 + 8 * j, 188 + 8 * j)
        return carry

    lax.fori_loop(0, 6, in_body, 0)
    in_pair(0, 1, in_row(0), in_row(1))
    in_pair(2, 3, in_row(2), in_row(3))
    for a in range(4):
        for k in range(4):
            x = packed[across(a, in_row(4) + k), :]
            xt[pl.ds(64 * a + 2 * k, 8, stride=8), :] = x
            xt[pl.ds(64 * a + 2 * k + 1, 8, stride=8), :] = right(x, x)
    for h in range(2):
        cols = xt[128 * h:128 * h + 128, :].T
        s_in[4, :, 128 * h:128 * h + 128] = cols[:64]
        t_in[4, :, 128 * h:128 * h + 128] = cols[:64].astype(bf)
    put(s_in.at[4], n_in.at[4], 2)
    put(t_in.at[4], b_in.at[4], 3)
    for a in range(4):
        for k in range(2):
            x = packed[across(a, IN0 + k), :]
            xt[pl.ds(32 * a + 2 * k, 8, stride=4), :] = x
            xt[pl.ds(32 * a + 2 * k + 1, 8, stride=4), :] = right(x, x)
    cols = xt[0:128, :].T
    s_in0[...] = cols[:64]
    t_in0[...] = cols[:64].astype(bf)
    put(s_in0, n_in0, 4)
    put(t_in0, b_in0, 5)

    def out_body(t, carry):
        for a in range(4):
            for p in range(2):
                for h in range(2):
                    s_out[h, t, pl.ds(16 * a + p, 8, stride=2), :] = packed[across(a, OUT + 4 * t + 2 * p + h), :]
        for h in range(2):
            t_out[h, t] = s_out[h, t].astype(bf)
            put(s_out.at[h, t], n_out.at[t, :, pl.ds(128 * h, 128)], 6)
            put(t_out.at[h, t], b_out.at[t, :, pl.ds(128 * h, 128)], 7)
        return carry

    lax.fori_loop(0, N_OUT, out_body, 0)
    for h in range(2):
        for a in range(4):
            for p in range(4):
                s_short[h, pl.ds(32 * a + p, 8, stride=4), :] = packed[across(a, SHORT + 2 * p + h), :]
        t_short[h] = s_short[h].astype(bf)
        put(s_short.at[h], n_short.at[:, pl.ds(128 * h, 128)], 8)
        put(t_short.at[h], b_short.at[:, pl.ds(128 * h, 128)], 9)
    for i in range(N_DEV):
        xt[8 * i:8 * i + 8, :] = packed[i * ROWS + FC:i * ROWS + FC + 8, :]
    for h in range(2):
        cols = xt[128 * h:128 * h + 128, :].T
        s_fc[:, 128 * h:128 * h + 128] = cols[:CLASSES]
        t_fc[:, 128 * h:128 * h + 128] = cols[:CLASSES].astype(bf)
    put(s_fc, n_fc, 10)
    put(t_fc, b_fc, 11)

    lane = lax.broadcasted_iota(jnp.int32, (8, LANES), 1)
    for b in range(2):
        def even(k):
            return packed[pl.ds(16 * b * ROWS + BN + k, 8, stride=2 * ROWS), :]

        def odd(k):
            return packed[pl.ds((16 * b + 1) * ROWS + BN + k, 8, stride=2 * ROWS), :]

        for k in range(3):
            n_bn[pl.ds(56 * b + k, 8, stride=7), :] = even(k)
            n_bn[pl.ds(56 * b + 4 + k, 8, stride=7), :] = odd(1 + k)
        n_bn[pl.ds(56 * b + 3, 8, stride=7), :] = jnp.where(lane < 64, even(3), odd(0))
    total = packed[across(0, BIAS), :]
    for a in range(1, 4):
        total = total + packed[across(a, BIAS), :]
    n_bias[...] = jnp.sum(total, axis=0, keepdims=True)[0, :CLASSES]

    for rows, tile, ref, tensors in momentum_rows(v_mid, v_in, v_out):
        ref[tensors, tile] = v_own[rows, :]
    rank = lax.axis_index('dp')
    v_in0[...] = v_own[IN0:IN0 + 2, :]
    v_short[...] = v_own[SHORT:SHORT + 8, :]
    for q in range(7):
        flat = jnp.zeros((1, LANES), F32)
        for r in range(8):
            d = CLASSES * r - LANES * q
            if -CLASSES < d < LANES:
                row = pltpu.roll(v_own[FC + r:FC + r + 1, :], d % LANES, 1)
                flat = jnp.where((lane_row >= d) & (lane_row < d + CLASSES), row, flat)
        size = min(LANES, 800 - LANES * q)
        v_fc[pl.ds(LANES * q, size)] = flat[0, :size]
    odd = lax.rem(rank, 2) == 1
    for k in range(4):
        here = v_own[BN + k:BN + k + 1, :]
        after = v_own[BN + k + 1:BN + k + 2, :]
        turned = jnp.where(lane_row < 64, pltpu.roll(here, 64, 1), pltpu.roll(after, 64, 1))
        size = min(LANES, 448 - LANES * k)
        v_bn[pl.ds(LANES * k, size)] = jnp.where(odd, turned, here)[0, :size]
    v_bias[...] = pltpu.roll(v_own[BIAS:BIAS + 1, :], lax.rem(N_DEV - rank, N_DEV) * 4, 1)[0, :4]
    momenta = (v_mid, v_in, v_in0, v_out, v_short, v_fc, v_bn, v_bias)
    moved = [pltpu.make_async_copy(src, dst, sems.at[19 + k]) for k, (src, dst) in enumerate(zip(momenta, v_outs))]
    for copy in moved:
        copy.start()
    last = []
    for k, (src, dst) in enumerate(((n_bn, bn_out), (n_bias, bias_out))):
        last.append(pltpu.make_async_copy(src, dst, sems.at[27 + k]))
        last[-1].start()
    for k, (src, dst) in enumerate(((s_mid, n_mid), (t_mid, b_mid), (s_in, n_in), (t_in, b_in), (s_in0, n_in0),
                                    (t_in0, b_in0))):
        pltpu.make_async_copy(src, dst, sems.at[k]).wait()
    for h in range(2):
        half = pl.ds(128 * h, 128)
        for k, (src, dst) in enumerate(((s_out, n_out.at[:, :, half]), (t_out, b_out.at[:, :, half]),
                                        (s_short, n_short.at[:, half]), (t_short, b_short.at[:, half]))):
            pltpu.make_async_copy(src.at[h], dst, sems.at[6 + k]).wait()
    pltpu.make_async_copy(s_fc, n_fc, sems.at[10]).wait()
    pltpu.make_async_copy(t_fc, b_fc, sems.at[11]).wait()
    for copy in moved + last:
        copy.wait()


def unpack_weights(packed, v_own):
    hbm = pl.BlockSpec(memory_space=pltpu.HBM)
    vm = pl.BlockSpec(memory_space=VMEM)
    bf = jnp.bfloat16
    kernels = ((N_MID, 576, 64), (N_IN, 64, 256), (64, 128), (N_OUT, 64, 256), (128, 256), (CLASSES, 256))
    shapes = [(s, F32) for s in kernels] + [((112, 128), F32), ((CLASSES,), F32)] + [(s, bf) for s in kernels]
    shapes += [(s, F32) for s in ((N_MID, 1152), (N_IN, 512), (2, LANES), (N_OUT, 512), (8, LANES), (800,), (448,), (4,))]
    scratch = ((N_MID, 576, 64), (N_IN, 64, 256), (2, N_OUT, 64, 128), (2, 128, 128), (64, 128), (CLASSES, 256))
    return pl.pallas_call(
        unpack_kernel,
        out_shape=[jax.ShapeDtypeStruct(s, d) for s, d in shapes],
        in_specs=[vm, vm],
        out_specs=[hbm] * 22,
        scratch_shapes=[VMEM(s, d) for s, d in shapes[6:8] + shapes[14:]] + [VMEM(s, F32) for s in scratch] + [VMEM(s, bf) for s in scratch]
        + [VMEM((256, 128), F32), pltpu.SemaphoreType.DMA((29,))],
        compiler_params=pltpu.CompilerParams(vmem_limit_bytes=UNPACK_VMEM),
    )(packed, v_own)


def solution(mesh):
    spec_full = P()
    spec_lead = P('dp')
    spec_cols = P(None, 'dp')
    moment_specs = (spec_lead, spec_lead, spec_cols, spec_cols, spec_cols, spec_lead, spec_lead, spec_lead)
    in_specs = (spec_full,) * 8 + (spec_lead,) * 8 + moment_specs + (spec_full,)
    out_specs = (spec_full,) * 14 + moment_specs

    def body(w_in0, w_short, w_in, w_mid, w_out, w_fc, w_bn, w_bias,
             g_in0, g_short, g_in, g_mid, g_out, g_bn, pooled, dlogits,
             v_in0, v_short, v_in, v_mid, v_out, v_fc, v_bn, v_bias, learn_rate):
        gathered, v_next = exchange((
            learn_rate.reshape(1), g_mid.reshape(N_MID, 576, 64), jnp.swapaxes(g_in[0], 1, 2), g_in0[0].T, g_out[0],
            g_short[0], g_bn.reshape(112, LANES), pooled, dlogits.T,
            w_mid.reshape(N_MID, 576, 64), jnp.swapaxes(w_in, 1, 2), w_in0.T, w_out, w_short, w_fc.T,
            w_bn.reshape(112, LANES), w_bias, v_mid, v_in, v_in0.reshape(2, LANES), v_out, v_short.reshape(8, LANES),
            v_fc, v_bn, v_bias))
        (n_mid, n_in, n_in0, n_out, n_short, n_fc, n_bn, n_bias, b_mid, b_in, b_in0, b_out, b_short, b_fc,
         m_mid, m_in, m_in0, m_out, m_short, m_fc, m_bn, m_bias) = unpack_weights(gathered, v_next)
        return (n_in0.T, n_short, jnp.swapaxes(n_in, 1, 2), n_mid.reshape(w_mid.shape), n_out, n_fc.T,
                n_bn.reshape(-1), n_bias,
                b_in0.T, b_short, jnp.swapaxes(b_in, 1, 2), b_mid.reshape(w_mid.shape), b_out, b_fc.T,
                m_in0.reshape(-1), m_short.reshape(-1), m_in, m_mid, m_out, m_fc, m_bn, m_bias)

    return jax.shard_map(body, mesh=mesh, in_specs=in_specs, out_specs=out_specs, check_vma=False)
```

```python
import jax
import jax.numpy as jnp
from jax import lax
from jax.experimental import pallas as pl
from jax.experimental.pallas import tpu as pltpu
from jax.sharding import PartitionSpec as P

MOMENTUM = 0.9
TRUST_COEF = 0.001
DECAY = 0.0001
N_DEV = 32
LANES = 128
IN0, OUT, SHORT, FC, BN, BIAS, ROWS = 178, 232, 304, 312, 320, 324, 328
N_MID, N_IN, N_OUT = 18, 17, 18
CLASSES = 100
ID_IN0, ID_IN, ID_OUT, ID_SHORT, ID_FC, ID_PLAIN = 18, 19, 36, 54, 55, 56
F32 = jnp.float32
VMEM = pltpu.VMEM
MESH = pl.DeviceIdType.MESH
CHUNKS = (
    (0, 40, 'y'), (40, 40, 'x'), (80, 40, 'x'), (120, 40, 'y'), (160, 24, 'zx'),
    (184, 24, 'y'), (208, 24, 'zx'), (232, 24, 'y'), (256, 24, 'y'), (280, 24, 'x'),
    (304, 24, 'x'),
)
STEPS = (
    (7, 0), (1, 0), (4, 0), (7, 1), (3, 0), (1, 1), (4, 1), (3, 1), (9, 0), (6, 0), (5, 0), (8, 0), (9, 1), (0, 0),
    (7, 2), (1, 2), (6, 1), (10, 0), (3, 2), (0, 1), (10, 1), (9, 2), (1, 3), (4, 2), (5, 1), (3, 3), (0, 2), (2, 0),
    (10, 2), (7, 3), (2, 1), (9, 3), (8, 1), (0, 3), (1, 4), (5, 2), (4, 3), (10, 3), (3, 4), (6, 2), (2, 2), (7, 4),
    (8, 2), (9, 4), (4, 4), (1, 5), (5, 3), (6, 3), (3, 5), (2, 3), (10, 4), (0, 4), (7, 5), (8, 3), (4, 5), (9, 5),
    (1, 6), (6, 4), (10, 5), (3, 6), (5, 4), (0, 5), (2, 4), (7, 6), (8, 4), (6, 5), (9, 6), (4, 6), (1, 7), (5, 5),
    (2, 5), (10, 6), (3, 7), (8, 5), (0, 6), (7, 7), (4, 7), (6, 6), (1, 8), (9, 7), (5, 6), (2, 6), (3, 8), (7, 8),
    (8, 6), (6, 7), (4, 8), (0, 7), (1, 9), (10, 7), (3, 9), (5, 7), (2, 7), (8, 7), (9, 8), (6, 8), (7, 9), (0, 8),
    (7, 10), (10, 8), (2, 8), (5, 8), (4, 9), (8, 8), (10, 9), (9, 9), (0, 9), (5, 9), (3, 10), (2, 9), (1, 10),
    (4, 10), (8, 9), (6, 9), (0, 10), (9, 10), (5, 10), (10, 10), (2, 10), (8, 10), (6, 10),
)
FIRST_NORMS = [step for step in STEPS if step[1] == 4][0]
S_CORE, S_ONE, S_TWO, S_Z, A_Z, A_TWO, A_ONE, A_CORE, N_SEMS = 0, 2, 4, 6, 7, 8, 10, 12, 14
EXCHANGE_VMEM, UNPACK_VMEM = 30 * 2**20, 20 * 2**20


def mid_row(t):
    return 40 * (t // 4) + 9 * (t % 4)


def in_row(t):
    return 36 + 40 * t if t < 4 else 164 + 4 * t


def member_rows(row, t):
    first = 9 * t
    for group in (4, 8, 12, 16):
        first = jnp.where(t >= group, first + 4, first)
    size = jnp.where(t < N_MID, 9, jnp.where(t == ID_IN0, 2, jnp.where(t < ID_SHORT, 4, 8)))
    first = jnp.where(t >= ID_IN0, IN0, first)
    first = jnp.where(t >= ID_IN, 36 + 40 * (t - ID_IN), first)
    first = jnp.where(t >= ID_IN + 4, 164 + 4 * (t - ID_IN), first)
    first = jnp.where(t >= ID_OUT, OUT + 4 * (t - ID_OUT), first)
    first = jnp.where(t >= ID_SHORT, SHORT + 8 * (t - ID_SHORT), first)
    return (row >= first) & (row < first + size)


def momentum_rows(mid, inn, out):
    runs = [(mid, mid_row(t), 9, t, min(4, N_MID - t)) for t in range(0, N_MID, 4)]
    runs += [(inn, 36, 40, 0, 4)] + [(inn, 164 + 4 * t, 4, t, min(8, N_IN - t)) for t in (4, 12)]
    runs += [(out, OUT + 4 * t, 4, t, min(8, N_OUT - t)) for t in (0, 8, 16)]
    for ref, base, stride, t, count in runs:
        for m in range(9 if ref is mid else 4):
            yield pl.ds(base + m, count, stride=stride), pl.ds(128 * m, 128), ref, pl.ds(t, count)


def left(a, b):
    return jnp.concatenate([a[:, :64], b[:, :64]], axis=1)


def right(a, b):
    return jnp.concatenate([a[:, 64:], b[:, 64:]], axis=1)


def across(piece8, row):
    return pl.ds(piece8 * 8 * ROWS + row, 8, stride=ROWS)


def exchange_kernel(lr, g_mid, g_in, g_in0, g_out, g_short, g_bn, pooled, dlog_t,
                    w_mid, w_in, w_in0, w_out, w_short, w_fc, w_bn, w_bias,
                    v_mid, v_in, v_in0, v_out, v_short, v_fc, v_bn, v_bias,
                    full, m_mid, m_in, m_in0, m_out, m_short, m_fc, m_bn, m_bias,
                    s_mid, s_in, s_in0, s_out, s_short, s_bn, s_x, s_d, xt, fct,
                    o_mid, o_in, o_in0, o_out, o_short, o_fc, o_bn, o_bias, ot,
                    p_mid, p_in, p_in0, p_out, p_short, p_fc, p_bn, p_bias,
                    packed, w_own, v_own, v_new,
                    got_core, acc, got_one, got_two, got_z, got_line, grad, layer_norms, norms,
                    sems, send, recv, n_send, n_recv):
    rank = lax.axis_index('dp')
    core = lax.rem(rank, 2)
    x = lax.rem(rank // 2, 2)
    y = lax.rem(rank // 4, 2)
    z = rank // 8

    def device(zz, yy, xx, cc):
        return (((zz * 2 + yy) * 2 + xx) * 2 + cc,)

    core_peer = device(z, y, x, 1 - core)
    x_peer = device(z, y, 1 - x, core)
    y_peer = device(z, 1 - y, x, core)

    barrier = pltpu.get_barrier_semaphore()

    def layer(d):
        return (z * 8 + lax.rem(rank + d, 8),)

    def line(d):
        return (lax.rem(rank + 8 * d, N_DEV),)

    for d in range(1, 8):
        pl.semaphore_signal(barrier, inc=1, device_id=layer(d), device_id_type=MESH)
    for d in range(1, 4):
        pl.semaphore_signal(barrier, inc=1, device_id=line(d), device_id_type=MESH)

    waiting = {}
    count = [0]

    def fetch(name, src, dst):
        copy = pltpu.make_async_copy(src, dst, sems.at[count[0]])
        count[0] += 1
        copy.start()
        waiting.setdefault(name, []).append(copy)

    def need(*names):
        for name in names:
            for copy in waiting.pop(name, []):
                copy.wait()

    def halves(name, src, dst):
        for h in range(2):
            fetch(name, src(pl.ds(128 * h, 128)), dst.at[h])

    fetchers = {
        'in': lambda: fetch('in', g_in.at[pl.ds(5, 12)], s_in.at[pl.ds(5, 12)]),
        'in1': lambda: fetch('in1', g_in.at[pl.ds(0, 5)], s_in.at[pl.ds(0, 5)]),
        'in0': lambda: fetch('in0', g_in0, s_in0),
        'out': lambda: halves('out', lambda c: g_out.at[:, :, c], s_out),
        'short': lambda: halves('short', lambda c: g_short.at[:, c], s_short),
        'fc': lambda: (fetch('fc', pooled, s_x), fetch('fc', dlog_t, s_d)),
        'bn': lambda: fetch('bn', g_bn, s_bn),
    }
    for i in range(5):
        part = pl.ds(4 * i, min(4, N_MID - 4 * i))
        fetchers['mid%d' % i] = lambda i=i, part=part: fetch('mid%d' % i, g_mid.at[part], s_mid.at[part])
    units = [(40 * i, 40 * i + 40, ('mid%d' % i, 'in1')) for i in range(4)] + [(160, 184, ('mid4', 'in0', 'in1'))]
    units += [(184 + 8 * j, 192 + 8 * j, ('in',)) for j in range(6)]
    units += [(232 + 8 * j, 240 + 8 * j, ('out',)) for j in range(9)]
    units += [(304, 312, ('short',)), (312, 320, ('fc',)), (320, 328, ('bn', 'fc'))]
    for at, size, _ in CHUNKS:
        for lo, hi, names in units:
            if at <= lo < at + size:
                for name in names:
                    if name in fetchers:
                        fetchers.pop(name)()

    mid_at = pl.multiple_of((18 * rank) // 8 * 8, 8)
    mid_off = lax.rem(18 * rank, 8)
    out_at = pl.multiple_of((2 * rank) // 8 * 8, 8)
    out_off = 2 * lax.rem(rank, 4)
    short_at = pl.multiple_of((4 * rank) // 8 * 8, 8)
    short_off = 4 * lax.rem(rank, 2)
    col_at = pl.multiple_of((rank // 16) * 128, 128)
    col_off = pl.multiple_of(lax.rem(rank, 16) * 8, 8)
    fetch('own', w_mid.at[:, pl.ds(mid_at, 24), :], o_mid)
    fetch('own', w_in.at[:, :, pl.ds(col_at, 128)], o_in)
    fetch('own', w_in0, o_in0)
    halves('own', lambda c: w_out.at[:, pl.ds(out_at, 8), c], o_out)
    halves('own', lambda c: w_short.at[pl.ds(short_at, 8), c], o_short)
    fetch('own', w_fc.at[:, pl.ds(col_at, 128)], o_fc)
    fetch('own', w_bn, o_bn)
    fetch('own', w_bias, o_bias)
    for src, dst in ((v_mid, p_mid), (v_in, p_in), (v_in0, p_in0), (v_out, p_out), (v_short, p_short), (v_fc, p_fc),
                     (v_bn, p_bn), (v_bias, p_bias)):
        fetch('own', src, dst)

    pieces = packed.reshape(N_DEV * ROWS, LANES)

    def pack_mid(base, first, count):
        def body(u, carry):
            t = first + u
            for a in range(4):
                for k in range(9):
                    even = s_mid[t, pl.ds(144 * a + 2 * k, 8, stride=18), :]
                    odd = s_mid[t, pl.ds(144 * a + 2 * k + 1, 8, stride=18), :]
                    pieces[across(a, base + 9 * u + k), :] = jnp.concatenate([even, odd], axis=1)
            return carry

        lax.fori_loop(0, count, body, 0)

    def pack_in_rows(base, pair):
        for a in range(4):
            for k in range(4):
                even = xt[pl.ds(64 * a + 2 * k, 8, stride=8), :]
                odd = xt[pl.ds(64 * a + 2 * k + 1, 8, stride=8), :]
                pieces[across(a, base + k), :] = left(even, odd)
                if pair:
                    pieces[across(a, base + 4 + k), :] = right(even, odd)

    def transpose(a, b):
        both = jnp.concatenate([a, b], axis=0)
        for h in range(2):
            xt[128 * h:128 * h + 128, :] = both[:, 128 * h:128 * h + 128].T

    def pack_in(first, last):
        def body(j, carry):
            transpose(s_in[2 * j + 5], s_in[2 * j + 6])
            pack_in_rows(184 + 8 * j, True)
            return carry

        lax.fori_loop(first, last, body, 0)

    def pack_in_one(t):
        wide = jnp.concatenate([s_in0[...], s_in0[...]], axis=1) if t == 4 else s_in[t]
        transpose(s_in[t], wide)
        pack_in_rows(in_row(t), False)
        if t == 4:
            for a in range(4):
                for k in range(2):
                    even = xt[pl.ds(32 * a + 2 * k, 8, stride=4), :]
                    odd = xt[pl.ds(32 * a + 2 * k + 1, 8, stride=4), :]
                    pieces[across(a, IN0 + k), :] = right(even, odd)

    def pack_out(first, last):
        def body(t, carry):
            for a in range(4):
                for p in range(2):
                    for h in range(2):
                        pieces[across(a, OUT + 4 * t + 2 * p + h), :] = s_out[h, t, pl.ds(16 * a + p, 8, stride=2), :]
            return carry

        lax.fori_loop(first, last, body, 0)

    def pack_short():
        for a in range(4):
            for p in range(4):
                for h in range(2):
                    pieces[across(a, SHORT + 2 * p + h), :] = s_short[h, pl.ds(32 * a + p, 8, stride=4), :]

    scale = 1.0 / pooled.shape[0]

    def pack_fc():
        fct[CLASSES:LANES, :] = jnp.zeros((LANES - CLASSES, 256), F32)
        fct[0:CLASSES, :] = jnp.dot(s_d[...], s_x[...], preferred_element_type=F32) * scale
        for h in range(2):
            cols = fct[:, 128 * h:128 * h + 128].T
            for j in range(16):
                at = (16 * h + j) * ROWS + FC
                pieces[at:at + 8, :] = cols[8 * j:8 * j + 8, :]

    def pack_bn():
        def clear(i, carry):
            pieces[pl.ds(pl.multiple_of(i * ROWS + BN, 8), 8), :] = jnp.zeros((8, LANES), F32)
            return carry

        lax.fori_loop(0, N_DEV, clear, 0)
        for b in range(2):
            for k in range(4):
                for half in range(2):
                    pieces[pl.ds((16 * b + half) * ROWS + BN + k, 8, stride=2 * ROWS), :] = (
                        s_bn[pl.ds(56 * b + 3 * half + k, 8, stride=7), :])
        bias = lax.dot_general(jnp.ones((8, s_d.shape[1]), jnp.bfloat16), s_d[...], (((1,), (1,)), ((), ())),
                               preferred_element_type=F32) * scale
        bias = jnp.concatenate([bias, jnp.zeros((8, LANES - CLASSES), F32)], axis=1)
        for a in range(4):
            pieces[across(a, BIAS), :] = bias

    def pack(at, size):
        end = at + size
        for lo, hi, names in units:
            if at <= lo < end:
                need(*names)
        for i in range(5):
            if at <= 40 * i < end:
                pack_mid(40 * i, 4 * i, min(4, N_MID - 4 * i))
                pack_in_one(i)
        lo, hi = max(at, 184), min(end, 232)
        if lo < hi:
            pack_in((lo - 184) // 8, (hi - 184) // 8)
        lo, hi = max(at, OUT), min(end, SHORT)
        if lo < hi:
            pack_out((lo - OUT) // 4, (hi - OUT) // 4)
        if at <= SHORT < end:
            pack_short()
        if at <= FC < end:
            pack_fc()
        if at <= BN < end:
            pack_bn()

    lane_row = lax.broadcasted_iota(jnp.int32, (1, LANES), 1)

    def own_pieces():
        need('own')
        for rows, tile, ref, tensors in momentum_rows(p_mid, p_in, p_out):
            v_own[rows, :] = ref[tensors, tile]
        v_own[IN0:IN0 + 2, :] = p_in0[...]
        v_own[SHORT:SHORT + 8, :] = p_short[...]
        flat = [p_fc[pl.ds(128 * q, 128)].reshape(1, LANES) for q in range(6)]
        flat.append(jnp.concatenate([p_fc[pl.ds(768, 32)].reshape(1, 32), jnp.zeros((1, 96), F32)], axis=1))
        for r in range(8):
            q, s = divmod(CLASSES * r, LANES)
            row = pltpu.roll(flat[q], (LANES - s) % LANES, 1)
            if s + CLASSES > LANES:
                row = jnp.where(lane_row < LANES - s, row, pltpu.roll(flat[q + 1], LANES - s, 1))
            v_own[FC + r:FC + r + 1, :] = jnp.where(lane_row < CLASSES, row, 0.0)
        v_own[BN:ROWS, :] = jnp.zeros((8, LANES), F32)
        odd = lax.rem(rank, 2) == 1
        rows = [p_bn[pl.ds(128 * k, 128)].reshape(1, LANES) for k in range(3)]
        rows.append(jnp.concatenate([p_bn[pl.ds(384, 64)].reshape(1, 64), jnp.zeros((1, 64), F32)], axis=1))
        for k in range(4):
            before = pltpu.roll(rows[k - 1], 64, 1) if k else jnp.zeros((1, LANES), F32)
            moved = jnp.where(lane_row < 64, before, pltpu.roll(rows[k], 64, 1))
            v_own[BN + k:BN + k + 1, :] = jnp.where(odd, moved, rows[k])
        four = jnp.concatenate([p_bias[...].reshape(1, 4), jnp.zeros((1, LANES - 4), F32)], axis=1)
        v_own[BIAS:BIAS + 1, :] = pltpu.roll(four, 4 * rank, 1)

        for t in range(N_MID):
            even = o_mid[t, pl.ds(mid_off, 9, stride=2), :]
            odds = o_mid[t, pl.ds(mid_off + 1, 9, stride=2), :]
            w_own[mid_row(t):mid_row(t) + 9, :] = jnp.concatenate([even, odds], axis=1)
        for j in range(9):
            other = o_in[2 * j - 1] if j else o_in0[...]
            ot[...] = jnp.concatenate([other, o_in[2 * j]], axis=0).T
            if j == 0:
                w_own[IN0:IN0 + 2, :] = left(ot[pl.ds(4 * rank, 2, stride=2), :], ot[pl.ds(4 * rank + 1, 2, stride=2), :])
            even = ot[pl.ds(col_off, 4, stride=2), :]
            odds = ot[pl.ds(col_off + 1, 4, stride=2), :]
            if j:
                w_own[in_row(2 * j - 1):in_row(2 * j - 1) + 4, :] = left(even, odds)
            w_own[in_row(2 * j):in_row(2 * j) + 4, :] = right(even, odds)
        def own_out(t, carry):
            for p in range(2):
                for h in range(2):
                    w_own[pl.ds(OUT + 4 * t + 2 * p + h, 1), :] = o_out[h, t, pl.ds(out_off + p, 1), :]
            return carry

        lax.fori_loop(0, N_OUT, own_out, 0)
        for p in range(4):
            for h in range(2):
                w_own[SHORT + 2 * p + h:SHORT + 2 * p + h + 1, :] = o_short[h, pl.ds(short_off + p, 1), :]
        ot[0:CLASSES, :] = o_fc[...]
        ot[CLASSES:LANES, :] = jnp.zeros((LANES - CLASSES, LANES), F32)
        ot[...] = ot[...].T
        w_own[FC:FC + 8, :] = ot[pl.ds(col_off, 8), :]
        w_own[BN:ROWS, :] = jnp.zeros((8, LANES), F32)
        bn_at = 7 * (rank // 2) + 3 * lax.rem(rank, 2)
        for k in range(4):
            w_own[BN + k:BN + k + 1, :] = o_bn[pl.ds(bn_at + k, 1), :]
        bias = jnp.concatenate([o_bias[...].reshape(1, CLASSES), jnp.zeros((1, LANES - CLASSES), F32)], axis=1)
        w_own[BIAS:BIAS + 1, :] = jnp.where((lane_row >= 4 * rank) & (lane_row < 4 * rank + 4), bias, 0.0)

    sent = {}

    def start(c, k, src, dst, peer):
        pltpu.make_async_remote_copy(src_ref=src, dst_ref=dst, send_sem=send.at[c * N_SEMS + k],
                                     recv_sem=recv.at[c * N_SEMS + k], device_id=peer, device_id_type=MESH).start()
        sent[c, k] = sent.get((c, k), 0) + (1 if len(src.shape) == 2 else src.size // (src.shape[-1] * src.shape[-2]))

    def wait(c, k, semaphores):
        at, size, _ = CHUNKS[c]
        rows = pl.ds(at, size)
        count = sent[c, k]
        lead = {1: (0, 0, 0), 2: (0, 0), 3: (pl.ds(0, 3), 0, 0), 4: (0,), 8: (pl.ds(0, 2),), 12: (pl.ds(0, 3),), 16: ()}[count]
        block = got_core.at[lead + (slice(None),) * (3 - len(lead)) + (rows,)]
        pltpu.make_async_copy(block, block, semaphores.at[c * N_SEMS + k]).wait()

    def arrived(c, *numbers):
        for k in numbers:
            wait(c, k, recv)

    def store_momentum():
        for rows, tile, ref, tensors in momentum_rows(m_mid, m_in, m_out):
            ref[tensors, tile] = v_new[rows, :]
        m_in0[...] = v_new[IN0:IN0 + 2, :]
        m_short[...] = v_new[SHORT:SHORT + 8, :]
        for q in range(7):
            flat = jnp.zeros((1, LANES), F32)
            for r in range(8):
                d = CLASSES * r - LANES * q
                if -CLASSES < d < LANES:
                    row = pltpu.roll(v_new[FC + r:FC + r + 1, :], d % LANES, 1)
                    flat = jnp.where((lane_row >= d) & (lane_row < d + CLASSES), row, flat)
            size = min(LANES, 800 - LANES * q)
            m_fc[pl.ds(LANES * q, size)] = flat[0, :size]
        odd = lax.rem(rank, 2) == 1
        for k in range(4):
            here = v_new[BN + k:BN + k + 1, :]
            after = v_new[BN + k + 1:BN + k + 2, :]
            turned = jnp.where(lane_row < 64, pltpu.roll(here, 64, 1), pltpu.roll(after, 64, 1))
            size = min(LANES, 448 - LANES * k)
            m_bn[pl.ds(LANES * k, size)] = jnp.where(odd, turned, here)[0, :size]
        m_bias[...] = pltpu.roll(v_new[BIAS:BIAS + 1, :], lax.rem(N_DEV - rank, N_DEV) * 4, 1)[0, :4]

    def tell(k, row, peer):
        pltpu.make_async_remote_copy(src_ref=row, dst_ref=row, send_sem=n_send.at[k], recv_sem=n_recv.at[k],
                                     device_id=peer, device_id_type=MESH).start()

    def told(k, semaphores):
        rows = layer_norms.at[k // 2, pl.ds(0, 3 if k % 2 else 7)]
        pltpu.make_async_copy(rows, rows, semaphores.at[k]).wait()

    def step(c, stage):
        at, size, first = CHUNKS[c]
        rows = pl.ds(at, size)
        x_first, z_first = first[-1] == 'x', first[0] == 'z'
        one_peer, two_peer = (x_peer, y_peer) if x_first else (y_peer, x_peer)

        here = y if x_first else x

        def block(ref, near, *rest):
            first_at = (x if near else 1 - x) if x_first else (y if near else 1 - y)
            return ref.at[(slice(None), slice(None), first_at) + rest] if x_first else (
                ref.at[(slice(None), first_at, slice(None)) + rest])

        def spot(second, near):
            return (second, x if near else 1 - x) if x_first else (y if near else 1 - y, second)

        def both_cores(zz, second, near):
            a, b = spot(second, near)
            return packed[zz, a, b, core, rows, :] + got_core[zz, a, b, rows, :]

        def over_z(body):
            def run(zz, carry):
                body(zz)
                return carry

            lax.fori_loop(0, 4, run, 0)

        if stage == 0:
            pack(at, size)
            if not sent:
                pl.semaphore_wait(barrier, 10)
            for k, near in enumerate((False, True)):
                start(c, S_CORE + k, block(packed, near, 1 - core, rows), block(got_core, near, rows), core_peer)
        elif stage == 1 and z_first:
            arrived(c, S_CORE, S_CORE + 1)
            for d in (2, 3, 1, 0):
                zz = lax.rem(z + d, 4)
                acc[zz, :, :, rows, :] = packed[zz, :, :, core, rows, :] + got_core[zz, :, :, rows, :]
                if d:
                    start(c, S_Z, acc.at[zz, :, :, rows, :], got_line.at[d - 1, :, :, rows, :], line(d))
        elif stage == 1:
            arrived(c, S_CORE)
            for k, second in enumerate((1 - here, here)):
                a, b = spot(second, False)

                def body(zz, a=a, b=b, second=second):
                    acc[zz, a, b, rows, :] = both_cores(zz, second, False)

                over_z(body)
                start(c, S_ONE + k, acc.at[:, a, b, rows, :], got_one.at[:, second, rows, :], one_peer)
        elif stage == 2 and z_first:
            arrived(c, S_Z)
            for near in (False, True):
                for second in range(2):
                    a, b = spot(second, near)
                    total = acc[z, a, b, rows, :] + got_line[0, a, b, rows, :]
                    acc[z, a, b, rows, :] = total + got_line[1, a, b, rows, :] + got_line[2, a, b, rows, :]
                if not near:
                    far = acc.at[z, :, 1 - x, rows, :] if x_first else acc.at[z, 1 - y, :, rows, :]
                    start(c, S_ONE, far, got_one.at[0, :, rows, :], one_peer)
        elif stage == 2:
            arrived(c, S_CORE + 1, S_ONE)
            a, b = spot(1 - here, True)

            def body(zz):
                acc[zz, a, b, rows, :] = both_cores(zz, 1 - here, True) + got_one[zz, 1 - here, rows, :]

            over_z(body)
            for d in (1, 2, 3, 0):
                zz = lax.rem(z + d, 4)
                start(c, S_TWO + (d == 0), acc.at[zz, a, b, rows, :], got_two.at[zz, rows, :], two_peer)
        elif stage == 3 and z_first:
            arrived(c, S_ONE)
            a, b = spot(1 - here, True)
            acc[z, a, b, rows, :] = acc[z, a, b, rows, :] + got_one[0, 1 - here, rows, :]
            start(c, S_TWO, acc.at[z, a, b, rows, :], got_two.at[0, rows, :], two_peer)
        elif stage == 3:
            arrived(c, S_ONE + 1, S_TWO)
            for d in (2, 3, 1):
                zz = lax.rem(z + d, 4)
                acc[zz, y, x, rows, :] = (
                    both_cores(zz, here, True) + got_one[zz, here, rows, :] + got_two[zz, rows, :])
                start(c, S_Z, acc.at[zz, y, x, rows, :], got_z.at[d - 1, rows, :], line(d))
        elif stage == 4:
            if z_first:
                arrived(c, S_TWO)
                mean = acc[z, y, x, rows, :] + got_one[0, here, rows, :] + got_two[0, rows, :]
            else:
                arrived(c, S_TWO + 1, S_Z)
                mean = both_cores(z, here, True) + got_one[z, here, rows, :] + got_two[z, rows, :]
                mean = mean + got_z[0, rows, :] + got_z[1, rows, :] + got_z[2, rows, :]
            mean = mean * (1.0 / N_DEV)
            grad[rows, :] = mean
            own = w_own[rows, :]
            g_sum = jnp.sum(mean * mean, axis=1, keepdims=True)
            w_sum = jnp.sum(own * own, axis=1, keepdims=True)
            row = lax.broadcasted_iota(jnp.int32, (size, LANES), 0) + at
            lane = lax.broadcasted_iota(jnp.int32, (size, LANES), 1)
            tensor = jnp.where(lane < 64, lane, lane - 64)
            member = member_rows(row, tensor)
            part = jnp.where(member, jnp.where(lane < 64, g_sum, w_sum), 0.0)
            here8 = lax.rem(rank, 8)
            layer_norms[c, here8] = jnp.sum(part, axis=0, keepdims=True)
            row8 = layer_norms.at[c, here8]
            for d in range(1, 8):
                tell(2 * c, row8, layer(d))
        elif stage == 5:
            told(2 * c, n_recv)
            norms[c, z] = jnp.sum(layer_norms[c], axis=0)
            for d in range(1, 4):
                tell(2 * c + 1, norms.at[c, z], line(d))
        elif stage == 6:
            told(2 * c + 1, n_recv)
            total = jnp.sum(norms[c], axis=0)
            g_norm = jnp.sqrt(total)
            w_norm = pltpu.roll(g_norm, 64, 1)
            trust = jnp.where((w_norm > 0) & (g_norm > 0), TRUST_COEF * w_norm / (g_norm + DECAY * w_norm), 1.0)
            row = lax.broadcasted_iota(jnp.int32, (size, LANES), 0) + at
            lane = lax.broadcasted_iota(jnp.int32, (size, LANES), 1)
            trust = jnp.where(lane == ID_PLAIN, 1.0, trust)
            member = member_rows(row, lane) & (lane <= ID_PLAIN)
            rate = lr[0] * jnp.sum(jnp.where(member, trust, 0.0), axis=1, keepdims=True)
            decay = jnp.where(row < BN, DECAY, 0.0)
            own = w_own[rows, :]
            moment = MOMENTUM * v_own[rows, :] + rate * (grad[rows, :] + decay * own)
            v_new[rows, :] = moment
            mine = (row != BIAS) | ((lane >= 4 * rank) & (lane < 4 * rank + 4))
            full[z, y, x, core, rows, :] = jnp.where(mine, own - moment, 0.0)
            piece = full.at[z, y, x, core, rows, :]
            if not z_first:
                for d in (2, 3, 1):
                    start(c, A_Z, piece, piece, line(d))
            start(c, A_TWO, piece, piece, two_peer)
        elif stage == 7 and z_first:
            arrived(c, A_TWO)
            pair = full.at[z, :, x, core, rows, :] if x_first else full.at[z, y, :, core, rows, :]
            start(c, A_ONE, pair, pair, one_peer)
        elif stage == 8 and z_first:
            arrived(c, A_ONE)
            plane = full.at[z, :, :, core, rows, :]
            for d in (2, 3, 1):
                start(c, A_Z, plane, plane, line(d))
        elif stage == 9 and z_first:
            arrived(c, A_Z)
            everything = full.at[:, :, :, core, rows, :]
            start(c, A_CORE, everything, everything, core_peer)
        elif stage == 10 and z_first:
            arrived(c, A_CORE)
        elif stage == 7:
            arrived(c, A_Z)
            for d in (1, 2, 3):
                piece = full.at[lax.rem(z + d, 4), y, x, core, rows, :]
                start(c, A_TWO + 1, piece, piece, two_peer)
            column = full.at[:, y, x, core, rows, :]
            start(c, A_ONE, column, column, one_peer)
        elif stage == 8:
            arrived(c, A_TWO, A_TWO + 1)
            a, b = spot(1 - here, True)
            column = full.at[:, a, b, core, rows, :]
            start(c, A_ONE + 1, column, column, one_peer)
            plane = block(full, True, core, rows)
            start(c, A_CORE, plane, plane, core_peer)
        elif stage == 9:
            arrived(c, A_ONE, A_ONE + 1)
            plane = block(full, False, core, rows)
            start(c, A_CORE + 1, plane, plane, core_peer)
        else:
            arrived(c, A_CORE, A_CORE + 1)

    for c, stage in STEPS:
        if stage == 4 and (c, stage) == FIRST_NORMS:
            own_pieces()
        if (c, stage) == STEPS[-3]:
            store_momentum()
        step(c, stage)
    for c, k in sent:
        wait(c, k, send)
    for k in range(2 * len(CHUNKS)):
        told(k, n_send)


def exchange(operands):
    hbm = pl.BlockSpec(memory_space=pltpu.HBM)
    vm = pl.BlockSpec(memory_space=VMEM)
    count = len(CHUNKS)
    bf = jnp.bfloat16
    shapes = [(N_MID, 576, 64), (N_IN, 64, 256), (64, 128), (2, N_OUT, 64, 128), (2, 128, 128), (112, 128)]
    own = [(N_MID, 24, 64), (N_IN, 64, 128), (64, 128), (2, N_OUT, 8, 128), (2, 8, 128), (CLASSES, 128), (112, 128),
           (CLASSES,), (128, 128), (N_MID, 1152), (N_IN, 512), (2, LANES), (N_OUT, 512), (8, LANES), (800,), (448,), (4,)]
    rows = (ROWS, LANES)
    exchanged = [(4, 2, 2) + rows, (4, 2, 2) + rows, (4, 2) + rows, (4,) + rows, (3,) + rows, (3, 2, 2) + rows, rows,
                 (count, 8, 1, LANES), (count, 4, 1, LANES)]
    dma = pltpu.SemaphoreType.DMA
    placed = [pltpu.with_memory_space_constraint(operand, pltpu.HBM) for operand in operands[1:]]
    momenta = own[-8:]
    full, *momenta = pl.pallas_call(
        exchange_kernel,
        out_shape=[jax.ShapeDtypeStruct(s, F32) for s in [(4, 2, 2, 2) + rows] + momenta],
        in_specs=[pl.BlockSpec(memory_space=pltpu.SMEM)] + [hbm] * 24,
        out_specs=[vm] * 9,
        scratch_shapes=[VMEM(s, F32) for s in shapes]
        + [VMEM((1024, 256), bf), VMEM((CLASSES, 1024), bf), VMEM((256, 128), F32), VMEM((128, 256), F32)]
        + [VMEM(s, F32) for s in own]
        + [VMEM((4, 2, 2, 2) + rows, F32), VMEM(rows, F32), VMEM(rows, F32), VMEM(rows, F32)]
        + [VMEM(s, F32) for s in exchanged]
        + [dma((40,)), dma((count * N_SEMS,)), dma((count * N_SEMS,)), dma((2 * count,)), dma((2 * count,))],
        compiler_params=pltpu.CompilerParams(vmem_limit_bytes=EXCHANGE_VMEM, collective_id=0, has_side_effects=True),
    )(operands[0], *placed)
    return full.reshape(N_DEV * ROWS, LANES), momenta


def unpack_kernel(packed, *rest):
    momenta, rest = rest[:8], rest[8:]
    (n_mid, n_in, n_in0, n_out, n_short, n_fc, bn_out, bias_out, b_mid, b_in, b_in0, b_out, b_short, b_fc) = rest[:14]
    v_outs, (n_bn, n_bias), rest = rest[14:22], rest[22:24], rest[24:]
    (s_mid, s_in, s_out, s_short, s_in0, s_fc, t_mid, t_in, t_out, t_short, t_in0, t_fc, xt, sems) = rest
    bf = jnp.bfloat16
    moved = [pltpu.make_async_copy(src, dst, sems.at[19 + k]) for k, (src, dst) in enumerate(zip(momenta, v_outs))]
    for copy in moved:
        copy.start()

    def put(src, dst, k):
        pltpu.make_async_copy(src, dst, sems.at[k]).start()

    def mid_body(t, carry):
        for a in range(4):
            for k in range(9):
                x = packed[across(a, mid_row(t) + k), :]
                s_mid[t, pl.ds(144 * a + 2 * k, 8, stride=18), :] = x[:, :64]
                s_mid[t, pl.ds(144 * a + 2 * k + 1, 8, stride=18), :] = x[:, 64:]
        put(s_mid.at[t], n_mid.at[t], 0)
        t_mid[t] = s_mid[t].astype(bf)
        put(t_mid.at[t], b_mid.at[t], 1)
        return carry

    lax.fori_loop(0, N_MID, mid_body, 0)

    def in_pair(first, second, row, other):
        for a in range(4):
            for k in range(4):
                x = packed[across(a, row + k), :]
                y = packed[across(a, other + k), :]
                xt[pl.ds(64 * a + 2 * k, 8, stride=8), :] = left(x, y)
                xt[pl.ds(64 * a + 2 * k + 1, 8, stride=8), :] = right(x, y)
        for h in range(2):
            cols = xt[128 * h:128 * h + 128, :].T
            for u, t in enumerate((first, second)):
                s_in[t, :, 128 * h:128 * h + 128] = cols[64 * u:64 * u + 64]
                t_in[t, :, 128 * h:128 * h + 128] = cols[64 * u:64 * u + 64].astype(bf)
        for t in (first, second):
            put(s_in.at[t], n_in.at[t], 2)
            put(t_in.at[t], b_in.at[t], 3)

    def in_body(j, carry):
        in_pair(2 * j + 5, 2 * j + 6, 184 + 8 * j, 188 + 8 * j)
        return carry

    lax.fori_loop(0, 6, in_body, 0)
    in_pair(0, 1, in_row(0), in_row(1))
    in_pair(2, 3, in_row(2), in_row(3))
    for a in range(4):
        for k in range(4):
            x = packed[across(a, in_row(4) + k), :]
            xt[pl.ds(64 * a + 2 * k, 8, stride=8), :] = x
            xt[pl.ds(64 * a + 2 * k + 1, 8, stride=8), :] = right(x, x)
    for h in range(2):
        cols = xt[128 * h:128 * h + 128, :].T
        s_in[4, :, 128 * h:128 * h + 128] = cols[:64]
        t_in[4, :, 128 * h:128 * h + 128] = cols[:64].astype(bf)
    put(s_in.at[4], n_in.at[4], 2)
    put(t_in.at[4], b_in.at[4], 3)
    for a in range(4):
        for k in range(2):
            x = packed[across(a, IN0 + k), :]
            xt[pl.ds(32 * a + 2 * k, 8, stride=4), :] = x
            xt[pl.ds(32 * a + 2 * k + 1, 8, stride=4), :] = right(x, x)
    cols = xt[0:128, :].T
    s_in0[...] = cols[:64]
    t_in0[...] = cols[:64].astype(bf)
    put(s_in0, n_in0, 4)
    put(t_in0, b_in0, 5)

    def out_body(t, carry):
        for a in range(4):
            for p in range(2):
                for h in range(2):
                    s_out[h, t, pl.ds(16 * a + p, 8, stride=2), :] = packed[across(a, OUT + 4 * t + 2 * p + h), :]
        for h in range(2):
            t_out[h, t] = s_out[h, t].astype(bf)
            put(s_out.at[h, t], n_out.at[t, :, pl.ds(128 * h, 128)], 6)
            put(t_out.at[h, t], b_out.at[t, :, pl.ds(128 * h, 128)], 7)
        return carry

    lax.fori_loop(0, N_OUT, out_body, 0)
    for h in range(2):
        for a in range(4):
            for p in range(4):
                s_short[h, pl.ds(32 * a + p, 8, stride=4), :] = packed[across(a, SHORT + 2 * p + h), :]
        t_short[h] = s_short[h].astype(bf)
        put(s_short.at[h], n_short.at[:, pl.ds(128 * h, 128)], 8)
        put(t_short.at[h], b_short.at[:, pl.ds(128 * h, 128)], 9)
    for i in range(N_DEV):
        xt[8 * i:8 * i + 8, :] = packed[i * ROWS + FC:i * ROWS + FC + 8, :]
    for h in range(2):
        cols = xt[128 * h:128 * h + 128, :].T
        s_fc[:, 128 * h:128 * h + 128] = cols[:CLASSES]
        t_fc[:, 128 * h:128 * h + 128] = cols[:CLASSES].astype(bf)
    put(s_fc, n_fc, 10)
    put(t_fc, b_fc, 11)

    lane = lax.broadcasted_iota(jnp.int32, (8, LANES), 1)
    for b in range(2):
        def even(k):
            return packed[pl.ds(16 * b * ROWS + BN + k, 8, stride=2 * ROWS), :]

        def odd(k):
            return packed[pl.ds((16 * b + 1) * ROWS + BN + k, 8, stride=2 * ROWS), :]

        for k in range(3):
            n_bn[pl.ds(56 * b + k, 8, stride=7), :] = even(k)
            n_bn[pl.ds(56 * b + 4 + k, 8, stride=7), :] = odd(1 + k)
        n_bn[pl.ds(56 * b + 3, 8, stride=7), :] = jnp.where(lane < 64, even(3), odd(0))
    total = packed[across(0, BIAS), :]
    for a in range(1, 4):
        total = total + packed[across(a, BIAS), :]
    n_bias[...] = jnp.sum(total, axis=0, keepdims=True)[0, :CLASSES]

    last = []
    for k, (src, dst) in enumerate(((n_bn, bn_out), (n_bias, bias_out))):
        last.append(pltpu.make_async_copy(src, dst, sems.at[27 + k]))
        last[-1].start()
    for k, (src, dst) in enumerate(((s_mid, n_mid), (t_mid, b_mid), (s_in, n_in), (t_in, b_in), (s_in0, n_in0),
                                    (t_in0, b_in0))):
        pltpu.make_async_copy(src, dst, sems.at[k]).wait()
    for h in range(2):
        half = pl.ds(128 * h, 128)
        for k, (src, dst) in enumerate(((s_out, n_out.at[:, :, half]), (t_out, b_out.at[:, :, half]),
                                        (s_short, n_short.at[:, half]), (t_short, b_short.at[:, half]))):
            pltpu.make_async_copy(src.at[h], dst, sems.at[6 + k]).wait()
    pltpu.make_async_copy(s_fc, n_fc, sems.at[10]).wait()
    pltpu.make_async_copy(t_fc, b_fc, sems.at[11]).wait()
    for copy in moved + last:
        copy.wait()


def unpack_weights(packed, momenta):
    hbm = pl.BlockSpec(memory_space=pltpu.HBM)
    vm = pl.BlockSpec(memory_space=VMEM)
    bf = jnp.bfloat16
    kernels = ((N_MID, 576, 64), (N_IN, 64, 256), (64, 128), (N_OUT, 64, 256), (128, 256), (CLASSES, 256))
    shapes = [(s, F32) for s in kernels] + [((112, 128), F32), ((CLASSES,), F32)] + [(s, bf) for s in kernels]
    shapes += [(s, F32) for s in ((N_MID, 1152), (N_IN, 512), (2, LANES), (N_OUT, 512), (8, LANES), (800,), (448,), (4,))]
    scratch = ((N_MID, 576, 64), (N_IN, 64, 256), (2, N_OUT, 64, 128), (2, 128, 128), (64, 128), (CLASSES, 256))
    return pl.pallas_call(
        unpack_kernel,
        out_shape=[jax.ShapeDtypeStruct(s, d) for s, d in shapes],
        in_specs=[vm] * 9,
        out_specs=[hbm] * 22,
        scratch_shapes=[VMEM(s, d) for s, d in shapes[6:8]] + [VMEM(s, F32) for s in scratch] + [VMEM(s, bf) for s in scratch]
        + [VMEM((256, 128), F32), pltpu.SemaphoreType.DMA((29,))],
        compiler_params=pltpu.CompilerParams(vmem_limit_bytes=UNPACK_VMEM),
    )(packed, *momenta)


def solution(mesh):
    spec_full = P()
    spec_lead = P('dp')
    spec_cols = P(None, 'dp')
    moment_specs = (spec_lead, spec_lead, spec_cols, spec_cols, spec_cols, spec_lead, spec_lead, spec_lead)
    in_specs = (spec_full,) * 8 + (spec_lead,) * 8 + moment_specs + (spec_full,)
    out_specs = (spec_full,) * 14 + moment_specs

    def body(w_in0, w_short, w_in, w_mid, w_out, w_fc, w_bn, w_bias,
             g_in0, g_short, g_in, g_mid, g_out, g_bn, pooled, dlogits,
             v_in0, v_short, v_in, v_mid, v_out, v_fc, v_bn, v_bias, learn_rate):
        gathered, v_next = exchange((
            learn_rate.reshape(1), g_mid.reshape(N_MID, 576, 64), jnp.swapaxes(g_in[0], 1, 2), g_in0[0].T, g_out[0],
            g_short[0], g_bn.reshape(112, LANES), pooled, dlogits.T,
            w_mid.reshape(N_MID, 576, 64), jnp.swapaxes(w_in, 1, 2), w_in0.T, w_out, w_short, w_fc.T,
            w_bn.reshape(112, LANES), w_bias, v_mid, v_in, v_in0.reshape(2, LANES), v_out, v_short.reshape(8, LANES),
            v_fc, v_bn, v_bias))
        (n_mid, n_in, n_in0, n_out, n_short, n_fc, n_bn, n_bias, b_mid, b_in, b_in0, b_out, b_short, b_fc,
         m_mid, m_in, m_in0, m_out, m_short, m_fc, m_bn, m_bias) = unpack_weights(gathered, v_next)
        return (n_in0.T, n_short, jnp.swapaxes(n_in, 1, 2), n_mid.reshape(w_mid.shape), n_out, n_fc.T,
                n_bn.reshape(-1), n_bias,
                b_in0.T, b_short, jnp.swapaxes(b_in, 1, 2), b_mid.reshape(w_mid.shape), b_out, b_fc.T,
                m_in0.reshape(-1), m_short.reshape(-1), m_in, m_mid, m_out, m_fc, m_bn, m_bias)

    return jax.shard_map(body, mesh=mesh, in_specs=in_specs, out_specs=out_specs, check_vma=False)
```

```python
import jax
import jax.numpy as jnp
from jax import lax
from jax.experimental import pallas as pl
from jax.experimental.pallas import tpu as pltpu
from jax.sharding import PartitionSpec as P

MOMENTUM = 0.9
TRUST_COEF = 0.001
DECAY = 0.0001
N_DEV = 32
LANES = 128
IN0, OUT, SHORT, FC, BN, BIAS, ROWS = 178, 232, 304, 312, 320, 324, 328
N_MID, N_IN, N_OUT = 18, 17, 18
CLASSES = 100
ID_IN0, ID_IN, ID_OUT, ID_SHORT, ID_FC, ID_PLAIN = 18, 19, 36, 54, 55, 56
F32 = jnp.float32
VMEM = pltpu.VMEM
MESH = pl.DeviceIdType.MESH
CHUNKS = (
    (0, 40, 'y'), (40, 40, 'zx'), (80, 40, 'y'), (120, 40, 'x'), (160, 24, 'x'),
    (184, 48, 'y'), (232, 32, 'x'), (264, 24, 'x'), (288, 8, 'zx'), (296, 16, 'x'),
    (312, 16, 'y'),
)
STEPS = (
    (5, 0), (6, 0), (1, 0), (5, 1), (6, 1), (3, 0), (7, 0), (1, 1), (2, 0), (3, 1), (0, 0), (6, 2), (5, 2), (8, 0),
    (7, 1), (0, 1), (10, 0), (3, 2), (6, 3), (2, 1), (5, 3), (0, 2), (4, 0), (4, 1), (3, 3), (6, 4), (0, 3), (7, 2),
    (1, 2), (8, 1), (2, 2), (4, 2), (9, 0), (10, 1), (5, 4), (9, 1), (7, 3), (1, 3), (3, 4), (6, 5), (4, 3), (10, 2),
    (2, 3), (0, 4), (9, 2), (1, 4), (5, 5), (8, 2), (10, 3), (6, 6), (7, 4), (4, 4), (8, 3), (0, 5), (9, 3), (1, 5),
    (3, 5), (5, 6), (2, 4), (8, 4), (10, 4), (4, 5), (7, 5), (0, 6), (9, 4), (6, 7), (2, 5), (3, 6), (1, 6), (5, 7),
    (10, 5), (7, 6), (9, 5), (6, 8), (8, 5), (4, 6), (1, 7), (0, 7), (2, 6), (5, 8), (10, 6), (6, 9), (3, 7), (9, 6),
    (1, 8), (8, 6), (4, 7), (7, 7), (2, 7), (8, 7), (3, 8), (0, 8), (5, 9), (9, 7), (5, 10), (6, 10), (2, 8), (10, 7),
    (8, 8), (7, 8), (4, 8), (9, 8), (0, 9), (10, 8), (1, 9), (7, 9), (0, 10), (3, 9), (2, 9), (4, 9), (8, 9), (10, 9),
    (9, 9), (4, 10), (7, 10), (1, 10), (3, 10), (2, 10), (10, 10), (8, 10), (9, 10),
)
FIRST_NORMS = [step for step in STEPS if step[1] == 4][0]
S_CORE, S_ONE, S_TWO, S_Z, A_Z, A_TWO, A_ONE, A_CORE, N_SEMS = 0, 2, 4, 6, 7, 8, 10, 12, 14
EXCHANGE_VMEM, UNPACK_VMEM = 30 * 2**20, 20 * 2**20


def mid_row(t):
    return 40 * (t // 4) + 9 * (t % 4)


def in_row(t):
    return 36 + 40 * t if t < 4 else 164 + 4 * t


def member_rows(row, t):
    first = 9 * t
    for group in (4, 8, 12, 16):
        first = jnp.where(t >= group, first + 4, first)
    size = jnp.where(t < N_MID, 9, jnp.where(t == ID_IN0, 2, jnp.where(t < ID_SHORT, 4, 8)))
    first = jnp.where(t >= ID_IN0, IN0, first)
    first = jnp.where(t >= ID_IN, 36 + 40 * (t - ID_IN), first)
    first = jnp.where(t >= ID_IN + 4, 164 + 4 * (t - ID_IN), first)
    first = jnp.where(t >= ID_OUT, OUT + 4 * (t - ID_OUT), first)
    first = jnp.where(t >= ID_SHORT, SHORT + 8 * (t - ID_SHORT), first)
    return (row >= first) & (row < first + size)


def momentum_rows(mid, inn, out):
    runs = [(mid, mid_row(t), 9, t, min(4, N_MID - t)) for t in range(0, N_MID, 4)]
    runs += [(inn, 36, 40, 0, 4)] + [(inn, 164 + 4 * t, 4, t, min(8, N_IN - t)) for t in (4, 12)]
    runs += [(out, OUT + 4 * t, 4, t, min(8, N_OUT - t)) for t in (0, 8, 16)]
    for ref, base, stride, t, count in runs:
        for m in range(9 if ref is mid else 4):
            yield pl.ds(base + m, count, stride=stride), pl.ds(128 * m, 128), ref, pl.ds(t, count)


def left(a, b):
    return jnp.concatenate([a[:, :64], b[:, :64]], axis=1)


def right(a, b):
    return jnp.concatenate([a[:, 64:], b[:, 64:]], axis=1)


def across(piece8, row):
    return pl.ds(piece8 * 8 * ROWS + row, 8, stride=ROWS)


def exchange_kernel(lr, g_mid, g_in, g_in0, g_out, g_short, g_bn, pooled, dlog_t,
                    w_mid, w_in, w_in0, w_out, w_short, w_fc, w_bn, w_bias,
                    v_mid, v_in, v_in0, v_out, v_short, v_fc, v_bn, v_bias,
                    full, m_mid, m_in, m_in0, m_out, m_short, m_fc, m_bn, m_bias,
                    s_mid, s_in, s_in0, s_out, s_short, s_bn, s_x, s_d, xt, fct,
                    o_mid, o_in, o_in0, o_out, o_short, o_fc, o_bn, o_bias, ot,
                    p_mid, p_in, p_in0, p_out, p_short, p_fc, p_bn, p_bias,
                    packed, w_own, v_own, v_new,
                    got_core, acc, got_one, got_two, got_z, got_line, grad, layer_norms, norms,
                    sems, send, recv, n_send, n_recv):
    rank = lax.axis_index('dp')
    core = lax.rem(rank, 2)
    x = lax.rem(rank // 2, 2)
    y = lax.rem(rank // 4, 2)
    z = rank // 8

    def device(zz, yy, xx, cc):
        return (((zz * 2 + yy) * 2 + xx) * 2 + cc,)

    core_peer = device(z, y, x, 1 - core)
    x_peer = device(z, y, 1 - x, core)
    y_peer = device(z, 1 - y, x, core)

    barrier = pltpu.get_barrier_semaphore()

    def layer(d):
        return (z * 8 + lax.rem(rank + d, 8),)

    def line(d):
        return (lax.rem(rank + 8 * d, N_DEV),)

    for d in range(1, 8):
        pl.semaphore_signal(barrier, inc=1, device_id=layer(d), device_id_type=MESH)
    for d in range(1, 4):
        pl.semaphore_signal(barrier, inc=1, device_id=line(d), device_id_type=MESH)

    waiting = {}
    count = [0]

    def fetch(name, src, dst):
        copy = pltpu.make_async_copy(src, dst, sems.at[count[0]])
        count[0] += 1
        copy.start()
        waiting.setdefault(name, []).append(copy)

    def need(*names):
        for name in names:
            for copy in waiting.pop(name, []):
                copy.wait()

    def halves(name, src, dst):
        for h in range(2):
            fetch(name, src(pl.ds(128 * h, 128)), dst.at[h])

    fetchers = {
        'in': lambda: fetch('in', g_in.at[pl.ds(5, 12)], s_in.at[pl.ds(5, 12)]),
        'in1': lambda: fetch('in1', g_in.at[pl.ds(0, 5)], s_in.at[pl.ds(0, 5)]),
        'in0': lambda: fetch('in0', g_in0, s_in0),
        'out': lambda: halves('out', lambda c: g_out.at[:, :, c], s_out),
        'short': lambda: halves('short', lambda c: g_short.at[:, c], s_short),
        'fc': lambda: (fetch('fc', pooled, s_x), fetch('fc', dlog_t, s_d)),
        'bn': lambda: fetch('bn', g_bn, s_bn),
    }
    for i in range(5):
        part = pl.ds(4 * i, min(4, N_MID - 4 * i))
        fetchers['mid%d' % i] = lambda i=i, part=part: fetch('mid%d' % i, g_mid.at[part], s_mid.at[part])
    units = [(40 * i, 40 * i + 40, ('mid%d' % i, 'in1')) for i in range(4)] + [(160, 184, ('mid4', 'in0', 'in1'))]
    units += [(184 + 8 * j, 192 + 8 * j, ('in',)) for j in range(6)]
    units += [(232 + 8 * j, 240 + 8 * j, ('out',)) for j in range(9)]
    units += [(304, 312, ('short',)), (312, 320, ('fc',)), (320, 328, ('bn', 'fc'))]
    for at, size, _ in CHUNKS:
        for lo, hi, names in units:
            if at <= lo < at + size:
                for name in names:
                    if name in fetchers:
                        fetchers.pop(name)()

    mid_at = pl.multiple_of((18 * rank) // 8 * 8, 8)
    mid_off = lax.rem(18 * rank, 8)
    out_at = pl.multiple_of((2 * rank) // 8 * 8, 8)
    out_off = 2 * lax.rem(rank, 4)
    short_at = pl.multiple_of((4 * rank) // 8 * 8, 8)
    short_off = 4 * lax.rem(rank, 2)
    col_at = pl.multiple_of((rank // 16) * 128, 128)
    col_off = pl.multiple_of(lax.rem(rank, 16) * 8, 8)
    fetch('own', w_mid.at[:, pl.ds(mid_at, 24), :], o_mid)
    fetch('own', w_in.at[:, :, pl.ds(col_at, 128)], o_in)
    fetch('own', w_in0, o_in0)
    halves('own', lambda c: w_out.at[:, pl.ds(out_at, 8), c], o_out)
    halves('own', lambda c: w_short.at[pl.ds(short_at, 8), c], o_short)
    fetch('own', w_fc.at[:, pl.ds(col_at, 128)], o_fc)
    fetch('own', w_bn, o_bn)
    fetch('own', w_bias, o_bias)
    for src, dst in ((v_mid, p_mid), (v_in, p_in), (v_in0, p_in0), (v_out, p_out), (v_short, p_short), (v_fc, p_fc),
                     (v_bn, p_bn), (v_bias, p_bias)):
        fetch('own', src, dst)

    pieces = packed.reshape(N_DEV * ROWS, LANES)

    def pack_mid(base, first, count):
        def body(u, carry):
            t = first + u
            for a in range(4):
                for k in range(9):
                    even = s_mid[t, pl.ds(144 * a + 2 * k, 8, stride=18), :]
                    odd = s_mid[t, pl.ds(144 * a + 2 * k + 1, 8, stride=18), :]
                    pieces[across(a, base + 9 * u + k), :] = jnp.concatenate([even, odd], axis=1)
            return carry

        lax.fori_loop(0, count, body, 0)

    def pack_in_rows(base, pair):
        for a in range(4):
            for k in range(4):
                even = xt[pl.ds(64 * a + 2 * k, 8, stride=8), :]
                odd = xt[pl.ds(64 * a + 2 * k + 1, 8, stride=8), :]
                pieces[across(a, base + k), :] = left(even, odd)
                if pair:
                    pieces[across(a, base + 4 + k), :] = right(even, odd)

    def transpose(a, b):
        both = jnp.concatenate([a, b], axis=0)
        for h in range(2):
            xt[128 * h:128 * h + 128, :] = both[:, 128 * h:128 * h + 128].T

    def pack_in(first, last):
        def body(j, carry):
            transpose(s_in[2 * j + 5], s_in[2 * j + 6])
            pack_in_rows(184 + 8 * j, True)
            return carry

        lax.fori_loop(first, last, body, 0)

    def pack_in_one(t):
        wide = jnp.concatenate([s_in0[...], s_in0[...]], axis=1) if t == 4 else s_in[t]
        transpose(s_in[t], wide)
        pack_in_rows(in_row(t), False)
        if t == 4:
            for a in range(4):
                for k in range(2):
                    even = xt[pl.ds(32 * a + 2 * k, 8, stride=4), :]
                    odd = xt[pl.ds(32 * a + 2 * k + 1, 8, stride=4), :]
                    pieces[across(a, IN0 + k), :] = right(even, odd)

    def pack_out(first, last):
        def body(t, carry):
            for a in range(4):
                for p in range(2):
                    for h in range(2):
                        pieces[across(a, OUT + 4 * t + 2 * p + h), :] = s_out[h, t, pl.ds(16 * a + p, 8, stride=2), :]
            return carry

        lax.fori_loop(first, last, body, 0)

    def pack_short():
        for a in range(4):
            for p in range(4):
                for h in range(2):
                    pieces[across(a, SHORT + 2 * p + h), :] = s_short[h, pl.ds(32 * a + p, 8, stride=4), :]

    scale = 1.0 / pooled.shape[0]

    def pack_fc():
        fct[CLASSES:LANES, :] = jnp.zeros((LANES - CLASSES, 256), F32)
        fct[0:CLASSES, :] = jnp.dot(s_d[...], s_x[...], preferred_element_type=F32) * scale
        for h in range(2):
            cols = fct[:, 128 * h:128 * h + 128].T
            for j in range(16):
                at = (16 * h + j) * ROWS + FC
                pieces[at:at + 8, :] = cols[8 * j:8 * j + 8, :]

    def pack_bn():
        def clear(i, carry):
            pieces[pl.ds(pl.multiple_of(i * ROWS + BN, 8), 8), :] = jnp.zeros((8, LANES), F32)
            return carry

        lax.fori_loop(0, N_DEV, clear, 0)
        for b in range(2):
            for k in range(4):
                for half in range(2):
                    pieces[pl.ds((16 * b + half) * ROWS + BN + k, 8, stride=2 * ROWS), :] = (
                        s_bn[pl.ds(56 * b + 3 * half + k, 8, stride=7), :])
        bias = lax.dot_general(jnp.ones((8, s_d.shape[1]), jnp.bfloat16), s_d[...], (((1,), (1,)), ((), ())),
                               preferred_element_type=F32) * scale
        bias = jnp.concatenate([bias, jnp.zeros((8, LANES - CLASSES), F32)], axis=1)
        for a in range(4):
            pieces[across(a, BIAS), :] = bias

    def pack(at, size):
        end = at + size
        for lo, hi, names in units:
            if at <= lo < end:
                need(*names)
        for i in range(5):
            if at <= 40 * i < end:
                pack_mid(40 * i, 4 * i, min(4, N_MID - 4 * i))
                pack_in_one(i)
        lo, hi = max(at, 184), min(end, 232)
        if lo < hi:
            pack_in((lo - 184) // 8, (hi - 184) // 8)
        lo, hi = max(at, OUT), min(end, SHORT)
        if lo < hi:
            pack_out((lo - OUT) // 4, (hi - OUT) // 4)
        if at <= SHORT < end:
            pack_short()
        if at <= FC < end:
            pack_fc()
        if at <= BN < end:
            pack_bn()

    lane_row = lax.broadcasted_iota(jnp.int32, (1, LANES), 1)

    def own_pieces():
        need('own')
        for rows, tile, ref, tensors in momentum_rows(p_mid, p_in, p_out):
            v_own[rows, :] = ref[tensors, tile]
        v_own[IN0:IN0 + 2, :] = p_in0[...]
        v_own[SHORT:SHORT + 8, :] = p_short[...]
        flat = [p_fc[pl.ds(128 * q, 128)].reshape(1, LANES) for q in range(6)]
        flat.append(jnp.concatenate([p_fc[pl.ds(768, 32)].reshape(1, 32), jnp.zeros((1, 96), F32)], axis=1))
        for r in range(8):
            q, s = divmod(CLASSES * r, LANES)
            row = pltpu.roll(flat[q], (LANES - s) % LANES, 1)
            if s + CLASSES > LANES:
                row = jnp.where(lane_row < LANES - s, row, pltpu.roll(flat[q + 1], LANES - s, 1))
            v_own[FC + r:FC + r + 1, :] = jnp.where(lane_row < CLASSES, row, 0.0)
        v_own[BN:ROWS, :] = jnp.zeros((8, LANES), F32)
        odd = lax.rem(rank, 2) == 1
        rows = [p_bn[pl.ds(128 * k, 128)].reshape(1, LANES) for k in range(3)]
        rows.append(jnp.concatenate([p_bn[pl.ds(384, 64)].reshape(1, 64), jnp.zeros((1, 64), F32)], axis=1))
        for k in range(4):
            before = pltpu.roll(rows[k - 1], 64, 1) if k else jnp.zeros((1, LANES), F32)
            moved = jnp.where(lane_row < 64, before, pltpu.roll(rows[k], 64, 1))
            v_own[BN + k:BN + k + 1, :] = jnp.where(odd, moved, rows[k])
        four = jnp.concatenate([p_bias[...].reshape(1, 4), jnp.zeros((1, LANES - 4), F32)], axis=1)
        v_own[BIAS:BIAS + 1, :] = pltpu.roll(four, 4 * rank, 1)

        for t in range(N_MID):
            even = o_mid[t, pl.ds(mid_off, 9, stride=2), :]
            odds = o_mid[t, pl.ds(mid_off + 1, 9, stride=2), :]
            w_own[mid_row(t):mid_row(t) + 9, :] = jnp.concatenate([even, odds], axis=1)
        for j in range(9):
            other = o_in[2 * j - 1] if j else o_in0[...]
            ot[...] = jnp.concatenate([other, o_in[2 * j]], axis=0).T
            if j == 0:
                w_own[IN0:IN0 + 2, :] = left(ot[pl.ds(4 * rank, 2, stride=2), :], ot[pl.ds(4 * rank + 1, 2, stride=2), :])
            even = ot[pl.ds(col_off, 4, stride=2), :]
            odds = ot[pl.ds(col_off + 1, 4, stride=2), :]
            if j:
                w_own[in_row(2 * j - 1):in_row(2 * j - 1) + 4, :] = left(even, odds)
            w_own[in_row(2 * j):in_row(2 * j) + 4, :] = right(even, odds)
        def own_out(t, carry):
            for p in range(2):
                for h in range(2):
                    w_own[pl.ds(OUT + 4 * t + 2 * p + h, 1), :] = o_out[h, t, pl.ds(out_off + p, 1), :]
            return carry

        lax.fori_loop(0, N_OUT, own_out, 0)
        for p in range(4):
            for h in range(2):
                w_own[SHORT + 2 * p + h:SHORT + 2 * p + h + 1, :] = o_short[h, pl.ds(short_off + p, 1), :]
        ot[0:CLASSES, :] = o_fc[...]
        ot[CLASSES:LANES, :] = jnp.zeros((LANES - CLASSES, LANES), F32)
        ot[...] = ot[...].T
        w_own[FC:FC + 8, :] = ot[pl.ds(col_off, 8), :]
        w_own[BN:ROWS, :] = jnp.zeros((8, LANES), F32)
        bn_at = 7 * (rank // 2) + 3 * lax.rem(rank, 2)
        for k in range(4):
            w_own[BN + k:BN + k + 1, :] = o_bn[pl.ds(bn_at + k, 1), :]
        bias = jnp.concatenate([o_bias[...].reshape(1, CLASSES), jnp.zeros((1, LANES - CLASSES), F32)], axis=1)
        w_own[BIAS:BIAS + 1, :] = jnp.where((lane_row >= 4 * rank) & (lane_row < 4 * rank + 4), bias, 0.0)

    sent = {}

    def start(c, k, src, dst, peer):
        pltpu.make_async_remote_copy(src_ref=src, dst_ref=dst, send_sem=send.at[c * N_SEMS + k],
                                     recv_sem=recv.at[c * N_SEMS + k], device_id=peer, device_id_type=MESH).start()
        sent[c, k] = sent.get((c, k), 0) + (1 if len(src.shape) == 2 else src.size // (src.shape[-1] * src.shape[-2]))

    def wait(c, k, semaphores):
        at, size, _ = CHUNKS[c]
        rows = pl.ds(at, size)
        count = sent[c, k]
        lead = {1: (0, 0, 0), 2: (0, 0), 3: (pl.ds(0, 3), 0, 0), 4: (0,), 8: (pl.ds(0, 2),), 12: (pl.ds(0, 3),), 16: ()}[count]
        block = got_core.at[lead + (slice(None),) * (3 - len(lead)) + (rows,)]
        pltpu.make_async_copy(block, block, semaphores.at[c * N_SEMS + k]).wait()

    def arrived(c, *numbers):
        for k in numbers:
            wait(c, k, recv)

    def store_momentum():
        for rows, tile, ref, tensors in momentum_rows(m_mid, m_in, m_out):
            ref[tensors, tile] = v_new[rows, :]
        m_in0[...] = v_new[IN0:IN0 + 2, :]
        m_short[...] = v_new[SHORT:SHORT + 8, :]
        for q in range(7):
            flat = jnp.zeros((1, LANES), F32)
            for r in range(8):
                d = CLASSES * r - LANES * q
                if -CLASSES < d < LANES:
                    row = pltpu.roll(v_new[FC + r:FC + r + 1, :], d % LANES, 1)
                    flat = jnp.where((lane_row >= d) & (lane_row < d + CLASSES), row, flat)
            size = min(LANES, 800 - LANES * q)
            m_fc[pl.ds(LANES * q, size)] = flat[0, :size]
        odd = lax.rem(rank, 2) == 1
        for k in range(4):
            here = v_new[BN + k:BN + k + 1, :]
            after = v_new[BN + k + 1:BN + k + 2, :]
            turned = jnp.where(lane_row < 64, pltpu.roll(here, 64, 1), pltpu.roll(after, 64, 1))
            size = min(LANES, 448 - LANES * k)
            m_bn[pl.ds(LANES * k, size)] = jnp.where(odd, turned, here)[0, :size]
        m_bias[...] = pltpu.roll(v_new[BIAS:BIAS + 1, :], lax.rem(N_DEV - rank, N_DEV) * 4, 1)[0, :4]

    def tell(k, row, peer):
        pltpu.make_async_remote_copy(src_ref=row, dst_ref=row, send_sem=n_send.at[k], recv_sem=n_recv.at[k],
                                     device_id=peer, device_id_type=MESH).start()

    def told(k, semaphores):
        rows = layer_norms.at[k // 2, pl.ds(0, 3 if k % 2 else 7)]
        pltpu.make_async_copy(rows, rows, semaphores.at[k]).wait()

    def step(c, stage):
        at, size, first = CHUNKS[c]
        rows = pl.ds(at, size)
        x_first, z_first = first[-1] == 'x', first[0] == 'z'
        one_peer, two_peer = (x_peer, y_peer) if x_first else (y_peer, x_peer)

        here = y if x_first else x

        def block(ref, near, *rest):
            first_at = (x if near else 1 - x) if x_first else (y if near else 1 - y)
            return ref.at[(slice(None), slice(None), first_at) + rest] if x_first else (
                ref.at[(slice(None), first_at, slice(None)) + rest])

        def spot(second, near):
            return (second, x if near else 1 - x) if x_first else (y if near else 1 - y, second)

        def both_cores(zz, second, near):
            a, b = spot(second, near)
            return packed[zz, a, b, core, rows, :] + got_core[zz, a, b, rows, :]

        def over_z(body):
            def run(zz, carry):
                body(zz)
                return carry

            lax.fori_loop(0, 4, run, 0)

        if stage == 0:
            pack(at, size)
            if not sent:
                pl.semaphore_wait(barrier, 10)
            for k, near in enumerate((False, True)):
                start(c, S_CORE + k, block(packed, near, 1 - core, rows), block(got_core, near, rows), core_peer)
        elif stage == 1 and z_first:
            arrived(c, S_CORE, S_CORE + 1)
            for d in (2, 3, 1, 0):
                zz = lax.rem(z + d, 4)
                acc[zz, :, :, rows, :] = packed[zz, :, :, core, rows, :] + got_core[zz, :, :, rows, :]
                if d:
                    start(c, S_Z, acc.at[zz, :, :, rows, :], got_line.at[d - 1, :, :, rows, :], line(d))
        elif stage == 1:
            arrived(c, S_CORE)
            for k, second in enumerate((1 - here, here)):
                a, b = spot(second, False)

                def body(zz, a=a, b=b, second=second):
                    acc[zz, a, b, rows, :] = both_cores(zz, second, False)

                over_z(body)
                start(c, S_ONE + k, acc.at[:, a, b, rows, :], got_one.at[:, second, rows, :], one_peer)
        elif stage == 2 and z_first:
            arrived(c, S_Z)
            for near in (False, True):
                for second in range(2):
                    a, b = spot(second, near)
                    total = acc[z, a, b, rows, :] + got_line[0, a, b, rows, :]
                    acc[z, a, b, rows, :] = total + got_line[1, a, b, rows, :] + got_line[2, a, b, rows, :]
                if not near:
                    far = acc.at[z, :, 1 - x, rows, :] if x_first else acc.at[z, 1 - y, :, rows, :]
                    start(c, S_ONE, far, got_one.at[0, :, rows, :], one_peer)
        elif stage == 2:
            arrived(c, S_CORE + 1, S_ONE)
            a, b = spot(1 - here, True)

            def body(zz):
                acc[zz, a, b, rows, :] = both_cores(zz, 1 - here, True) + got_one[zz, 1 - here, rows, :]

            over_z(body)
            for d in (1, 2, 3, 0):
                zz = lax.rem(z + d, 4)
                start(c, S_TWO + (d == 0), acc.at[zz, a, b, rows, :], got_two.at[zz, rows, :], two_peer)
        elif stage == 3 and z_first:
            arrived(c, S_ONE)
            a, b = spot(1 - here, True)
            acc[z, a, b, rows, :] = acc[z, a, b, rows, :] + got_one[0, 1 - here, rows, :]
            start(c, S_TWO, acc.at[z, a, b, rows, :], got_two.at[0, rows, :], two_peer)
        elif stage == 3:
            arrived(c, S_ONE + 1, S_TWO)
            for d in (2, 3, 1):
                zz = lax.rem(z + d, 4)
                acc[zz, y, x, rows, :] = (
                    both_cores(zz, here, True) + got_one[zz, here, rows, :] + got_two[zz, rows, :])
                start(c, S_Z, acc.at[zz, y, x, rows, :], got_z.at[d - 1, rows, :], line(d))
        elif stage == 4:
            if z_first:
                arrived(c, S_TWO)
                mean = acc[z, y, x, rows, :] + got_one[0, here, rows, :] + got_two[0, rows, :]
            else:
                arrived(c, S_TWO + 1, S_Z)
                mean = both_cores(z, here, True) + got_one[z, here, rows, :] + got_two[z, rows, :]
                mean = mean + got_z[0, rows, :] + got_z[1, rows, :] + got_z[2, rows, :]
            mean = mean * (1.0 / N_DEV)
            grad[rows, :] = mean
            own = w_own[rows, :]
            g_sum = jnp.sum(mean * mean, axis=1, keepdims=True)
            w_sum = jnp.sum(own * own, axis=1, keepdims=True)
            row = lax.broadcasted_iota(jnp.int32, (size, LANES), 0) + at
            lane = lax.broadcasted_iota(jnp.int32, (size, LANES), 1)
            tensor = jnp.where(lane < 64, lane, lane - 64)
            member = member_rows(row, tensor)
            part = jnp.where(member, jnp.where(lane < 64, g_sum, w_sum), 0.0)
            here8 = lax.rem(rank, 8)
            layer_norms[c, here8] = jnp.sum(part, axis=0, keepdims=True)
            row8 = layer_norms.at[c, here8]
            for d in range(1, 8):
                tell(2 * c, row8, layer(d))
        elif stage == 5:
            told(2 * c, n_recv)
            norms[c, z] = jnp.sum(layer_norms[c], axis=0)
            for d in range(1, 4):
                tell(2 * c + 1, norms.at[c, z], line(d))
        elif stage == 6:
            told(2 * c + 1, n_recv)
            total = jnp.sum(norms[c], axis=0)
            g_norm = jnp.sqrt(total)
            w_norm = pltpu.roll(g_norm, 64, 1)
            trust = jnp.where((w_norm > 0) & (g_norm > 0), TRUST_COEF * w_norm / (g_norm + DECAY * w_norm), 1.0)
            row = lax.broadcasted_iota(jnp.int32, (size, LANES), 0) + at
            lane = lax.broadcasted_iota(jnp.int32, (size, LANES), 1)
            trust = jnp.where(lane == ID_PLAIN, 1.0, trust)
            member = member_rows(row, lane) & (lane <= ID_PLAIN)
            rate = lr[0] * jnp.sum(jnp.where(member, trust, 0.0), axis=1, keepdims=True)
            decay = jnp.where(row < BN, DECAY, 0.0)
            own = w_own[rows, :]
            moment = MOMENTUM * v_own[rows, :] + rate * (grad[rows, :] + decay * own)
            v_new[rows, :] = moment
            mine = (row != BIAS) | ((lane >= 4 * rank) & (lane < 4 * rank + 4))
            full[z, y, x, core, rows, :] = jnp.where(mine, own - moment, 0.0)
            piece = full.at[z, y, x, core, rows, :]
            if not z_first:
                for d in (2, 3, 1):
                    start(c, A_Z, piece, piece, line(d))
            start(c, A_TWO, piece, piece, two_peer)
        elif stage == 7 and z_first:
            arrived(c, A_TWO)
            pair = full.at[z, :, x, core, rows, :] if x_first else full.at[z, y, :, core, rows, :]
            start(c, A_ONE, pair, pair, one_peer)
        elif stage == 8 and z_first:
            arrived(c, A_ONE)
            plane = full.at[z, :, :, core, rows, :]
            for d in (2, 3, 1):
                start(c, A_Z, plane, plane, line(d))
        elif stage == 9 and z_first:
            arrived(c, A_Z)
            everything = full.at[:, :, :, core, rows, :]
            start(c, A_CORE, everything, everything, core_peer)
        elif stage == 10 and z_first:
            arrived(c, A_CORE)
        elif stage == 7:
            arrived(c, A_Z)
            for d in (1, 2, 3):
                piece = full.at[lax.rem(z + d, 4), y, x, core, rows, :]
                start(c, A_TWO + 1, piece, piece, two_peer)
            column = full.at[:, y, x, core, rows, :]
            start(c, A_ONE, column, column, one_peer)
        elif stage == 8:
            arrived(c, A_TWO, A_TWO + 1)
            a, b = spot(1 - here, True)
            column = full.at[:, a, b, core, rows, :]
            start(c, A_ONE + 1, column, column, one_peer)
            plane = block(full, True, core, rows)
            start(c, A_CORE, plane, plane, core_peer)
        elif stage == 9:
            arrived(c, A_ONE, A_ONE + 1)
            plane = block(full, False, core, rows)
            start(c, A_CORE + 1, plane, plane, core_peer)
        else:
            arrived(c, A_CORE, A_CORE + 1)

    for c, stage in STEPS:
        if stage == 4 and (c, stage) == FIRST_NORMS:
            own_pieces()
        if (c, stage) == STEPS[-3]:
            store_momentum()
        step(c, stage)
    for c, k in sent:
        wait(c, k, send)
    for k in range(2 * len(CHUNKS)):
        told(k, n_send)


def exchange(operands):
    hbm = pl.BlockSpec(memory_space=pltpu.HBM)
    vm = pl.BlockSpec(memory_space=VMEM)
    count = len(CHUNKS)
    bf = jnp.bfloat16
    shapes = [(N_MID, 576, 64), (N_IN, 64, 256), (64, 128), (2, N_OUT, 64, 128), (2, 128, 128), (112, 128)]
    own = [(N_MID, 24, 64), (N_IN, 64, 128), (64, 128), (2, N_OUT, 8, 128), (2, 8, 128), (CLASSES, 128), (112, 128),
           (CLASSES,), (128, 128), (N_MID, 1152), (N_IN, 512), (2, LANES), (N_OUT, 512), (8, LANES), (800,), (448,), (4,)]
    rows = (ROWS, LANES)
    exchanged = [(4, 2, 2) + rows, (4, 2, 2) + rows, (4, 2) + rows, (4,) + rows, (3,) + rows, (3, 2, 2) + rows, rows,
                 (count, 8, 1, LANES), (count, 4, 1, LANES)]
    dma = pltpu.SemaphoreType.DMA
    placed = [pltpu.with_memory_space_constraint(operand, pltpu.HBM) for operand in operands[1:]]
    momenta = own[-8:]
    full, *momenta = pl.pallas_call(
        exchange_kernel,
        out_shape=[jax.ShapeDtypeStruct(s, F32) for s in [(4, 2, 2, 2) + rows] + momenta],
        in_specs=[pl.BlockSpec(memory_space=pltpu.SMEM)] + [hbm] * 24,
        out_specs=[vm] * 9,
        scratch_shapes=[VMEM(s, F32) for s in shapes]
        + [VMEM((1024, 256), bf), VMEM((CLASSES, 1024), bf), VMEM((256, 128), F32), VMEM((128, 256), F32)]
        + [VMEM(s, F32) for s in own]
        + [VMEM((4, 2, 2, 2) + rows, F32), VMEM(rows, F32), VMEM(rows, F32), VMEM(rows, F32)]
        + [VMEM(s, F32) for s in exchanged]
        + [dma((40,)), dma((count * N_SEMS,)), dma((count * N_SEMS,)), dma((2 * count,)), dma((2 * count,))],
        compiler_params=pltpu.CompilerParams(vmem_limit_bytes=EXCHANGE_VMEM, collective_id=0, has_side_effects=True),
    )(operands[0], *placed)
    return full.reshape(N_DEV * ROWS, LANES), momenta


def unpack_kernel(packed, *rest):
    momenta, rest = rest[:8], rest[8:]
    (n_mid, n_in, n_in0, n_out, n_short, n_fc, bn_out, bias_out, b_mid, b_in, b_in0, b_out, b_short, b_fc) = rest[:14]
    v_outs, (n_bn, n_bias), rest = rest[14:22], rest[22:24], rest[24:]
    (s_mid, s_in, s_out, s_short, s_in0, s_fc, t_mid, t_in, t_out, t_short, t_in0, t_fc, xt, sems) = rest
    bf = jnp.bfloat16
    moved = [pltpu.make_async_copy(src, dst, sems.at[19 + k]) for k, (src, dst) in enumerate(zip(momenta, v_outs))]
    for copy in moved:
        copy.start()

    def put(src, dst, k):
        pltpu.make_async_copy(src, dst, sems.at[k]).start()

    def mid_body(t, carry):
        for a in range(4):
            for k in range(9):
                x = packed[across(a, mid_row(t) + k), :]
                s_mid[t, pl.ds(144 * a + 2 * k, 8, stride=18), :] = x[:, :64]
                s_mid[t, pl.ds(144 * a + 2 * k + 1, 8, stride=18), :] = x[:, 64:]
        put(s_mid.at[t], n_mid.at[t], 0)
        t_mid[t] = s_mid[t].astype(bf)
        put(t_mid.at[t], b_mid.at[t], 1)
        return carry

    lax.fori_loop(0, N_MID, mid_body, 0)

    def in_pair(first, second, row, other):
        for a in range(4):
            for k in range(4):
                x = packed[across(a, row + k), :]
                y = packed[across(a, other + k), :]
                xt[pl.ds(64 * a + 2 * k, 8, stride=8), :] = left(x, y)
                xt[pl.ds(64 * a + 2 * k + 1, 8, stride=8), :] = right(x, y)
        for h in range(2):
            cols = xt[128 * h:128 * h + 128, :].T
            for u, t in enumerate((first, second)):
                s_in[t, :, 128 * h:128 * h + 128] = cols[64 * u:64 * u + 64]
                t_in[t, :, 128 * h:128 * h + 128] = cols[64 * u:64 * u + 64].astype(bf)
        for t in (first, second):
            put(s_in.at[t], n_in.at[t], 2)
            put(t_in.at[t], b_in.at[t], 3)

    def in_body(j, carry):
        in_pair(2 * j + 5, 2 * j + 6, 184 + 8 * j, 188 + 8 * j)
        return carry

    lax.fori_loop(0, 6, in_body, 0)
    in_pair(0, 1, in_row(0), in_row(1))
    in_pair(2, 3, in_row(2), in_row(3))
    for a in range(4):
        for k in range(4):
            x = packed[across(a, in_row(4) + k), :]
            xt[pl.ds(64 * a + 2 * k, 8, stride=8), :] = x
            xt[pl.ds(64 * a + 2 * k + 1, 8, stride=8), :] = right(x, x)
    for h in range(2):
        cols = xt[128 * h:128 * h + 128, :].T
        s_in[4, :, 128 * h:128 * h + 128] = cols[:64]
        t_in[4, :, 128 * h:128 * h + 128] = cols[:64].astype(bf)
    put(s_in.at[4], n_in.at[4], 2)
    put(t_in.at[4], b_in.at[4], 3)
    for a in range(4):
        for k in range(2):
            x = packed[across(a, IN0 + k), :]
            xt[pl.ds(32 * a + 2 * k, 8, stride=4), :] = x
            xt[pl.ds(32 * a + 2 * k + 1, 8, stride=4), :] = right(x, x)
    cols = xt[0:128, :].T
    s_in0[...] = cols[:64]
    t_in0[...] = cols[:64].astype(bf)
    put(s_in0, n_in0, 4)
    put(t_in0, b_in0, 5)

    def out_body(t, carry):
        for a in range(4):
            for p in range(2):
                for h in range(2):
                    s_out[h, t, pl.ds(16 * a + p, 8, stride=2), :] = packed[across(a, OUT + 4 * t + 2 * p + h), :]
        for h in range(2):
            t_out[h, t] = s_out[h, t].astype(bf)
            put(s_out.at[h, t], n_out.at[t, :, pl.ds(128 * h, 128)], 6)
            put(t_out.at[h, t], b_out.at[t, :, pl.ds(128 * h, 128)], 7)
        return carry

    lax.fori_loop(0, N_OUT, out_body, 0)
    for h in range(2):
        for a in range(4):
            for p in range(4):
                s_short[h, pl.ds(32 * a + p, 8, stride=4), :] = packed[across(a, SHORT + 2 * p + h), :]
        t_short[h] = s_short[h].astype(bf)
        put(s_short.at[h], n_short.at[:, pl.ds(128 * h, 128)], 8)
        put(t_short.at[h], b_short.at[:, pl.ds(128 * h, 128)], 9)
    for i in range(N_DEV):
        xt[8 * i:8 * i + 8, :] = packed[i * ROWS + FC:i * ROWS + FC + 8, :]
    for h in range(2):
        cols = xt[128 * h:128 * h + 128, :].T
        s_fc[:, 128 * h:128 * h + 128] = cols[:CLASSES]
        t_fc[:, 128 * h:128 * h + 128] = cols[:CLASSES].astype(bf)
    put(s_fc, n_fc, 10)
    put(t_fc, b_fc, 11)

    lane = lax.broadcasted_iota(jnp.int32, (8, LANES), 1)
    for b in range(2):
        def even(k):
            return packed[pl.ds(16 * b * ROWS + BN + k, 8, stride=2 * ROWS), :]

        def odd(k):
            return packed[pl.ds((16 * b + 1) * ROWS + BN + k, 8, stride=2 * ROWS), :]

        for k in range(3):
            n_bn[pl.ds(56 * b + k, 8, stride=7), :] = even(k)
            n_bn[pl.ds(56 * b + 4 + k, 8, stride=7), :] = odd(1 + k)
        n_bn[pl.ds(56 * b + 3, 8, stride=7), :] = jnp.where(lane < 64, even(3), odd(0))
    total = packed[across(0, BIAS), :]
    for a in range(1, 4):
        total = total + packed[across(a, BIAS), :]
    n_bias[...] = jnp.sum(total, axis=0, keepdims=True)[0, :CLASSES]

    last = []
    for k, (src, dst) in enumerate(((n_bn, bn_out), (n_bias, bias_out))):
        last.append(pltpu.make_async_copy(src, dst, sems.at[27 + k]))
        last[-1].start()
    for k, (src, dst) in enumerate(((s_mid, n_mid), (t_mid, b_mid), (s_in, n_in), (t_in, b_in), (s_in0, n_in0),
                                    (t_in0, b_in0))):
        pltpu.make_async_copy(src, dst, sems.at[k]).wait()
    for h in range(2):
        half = pl.ds(128 * h, 128)
        for k, (src, dst) in enumerate(((s_out, n_out.at[:, :, half]), (t_out, b_out.at[:, :, half]),
                                        (s_short, n_short.at[:, half]), (t_short, b_short.at[:, half]))):
            pltpu.make_async_copy(src.at[h], dst, sems.at[6 + k]).wait()
    pltpu.make_async_copy(s_fc, n_fc, sems.at[10]).wait()
    pltpu.make_async_copy(t_fc, b_fc, sems.at[11]).wait()
    for copy in moved + last:
        copy.wait()


def unpack_weights(packed, momenta):
    hbm = pl.BlockSpec(memory_space=pltpu.HBM)
    vm = pl.BlockSpec(memory_space=VMEM)
    bf = jnp.bfloat16
    kernels = ((N_MID, 576, 64), (N_IN, 64, 256), (64, 128), (N_OUT, 64, 256), (128, 256), (CLASSES, 256))
    shapes = [(s, F32) for s in kernels] + [((112, 128), F32), ((CLASSES,), F32)] + [(s, bf) for s in kernels]
    shapes += [(s, F32) for s in ((N_MID, 1152), (N_IN, 512), (2, LANES), (N_OUT, 512), (8, LANES), (800,), (448,), (4,))]
    scratch = ((N_MID, 576, 64), (N_IN, 64, 256), (2, N_OUT, 64, 128), (2, 128, 128), (64, 128), (CLASSES, 256))
    return pl.pallas_call(
        unpack_kernel,
        out_shape=[jax.ShapeDtypeStruct(s, d) for s, d in shapes],
        in_specs=[vm] * 9,
        out_specs=[hbm] * 22,
        scratch_shapes=[VMEM(s, d) for s, d in shapes[6:8]] + [VMEM(s, F32) for s in scratch] + [VMEM(s, bf) for s in scratch]
        + [VMEM((256, 128), F32), pltpu.SemaphoreType.DMA((29,))],
        compiler_params=pltpu.CompilerParams(vmem_limit_bytes=UNPACK_VMEM),
    )(packed, *momenta)


def solution(mesh):
    spec_full = P()
    spec_lead = P('dp')
    spec_cols = P(None, 'dp')
    moment_specs = (spec_lead, spec_lead, spec_cols, spec_cols, spec_cols, spec_lead, spec_lead, spec_lead)
    in_specs = (spec_full,) * 8 + (spec_lead,) * 8 + moment_specs + (spec_full,)
    out_specs = (spec_full,) * 14 + moment_specs

    def body(w_in0, w_short, w_in, w_mid, w_out, w_fc, w_bn, w_bias,
             g_in0, g_short, g_in, g_mid, g_out, g_bn, pooled, dlogits,
             v_in0, v_short, v_in, v_mid, v_out, v_fc, v_bn, v_bias, learn_rate):
        gathered, v_next = exchange((
            learn_rate.reshape(1), g_mid.reshape(N_MID, 576, 64), jnp.swapaxes(g_in[0], 1, 2), g_in0[0].T, g_out[0],
            g_short[0], g_bn.reshape(112, LANES), pooled, dlogits.T,
            w_mid.reshape(N_MID, 576, 64), jnp.swapaxes(w_in, 1, 2), w_in0.T, w_out, w_short, w_fc.T,
            w_bn.reshape(112, LANES), w_bias, v_mid, v_in, v_in0.reshape(2, LANES), v_out, v_short.reshape(8, LANES),
            v_fc, v_bn, v_bias))
        (n_mid, n_in, n_in0, n_out, n_short, n_fc, n_bn, n_bias, b_mid, b_in, b_in0, b_out, b_short, b_fc,
         m_mid, m_in, m_in0, m_out, m_short, m_fc, m_bn, m_bias) = unpack_weights(gathered, v_next)
        return (n_in0.T, n_short, jnp.swapaxes(n_in, 1, 2), n_mid.reshape(w_mid.shape), n_out, n_fc.T,
                n_bn.reshape(-1), n_bias,
                b_in0.T, b_short, jnp.swapaxes(b_in, 1, 2), b_mid.reshape(w_mid.shape), b_out, b_fc.T,
                m_in0.reshape(-1), m_short.reshape(-1), m_in, m_mid, m_out, m_fc, m_bn, m_bias)

    return jax.shard_map(body, mesh=mesh, in_specs=in_specs, out_specs=out_specs, check_vma=False)
```
